32 devices in a mesh: dp: 16 (over z, y, x), tensor: 2 (over core).
Axes of the slice: x: 2, y: 2, z: 4, core: 2. Of those that a mesh axis runs over, the one named last changes fastest.
Arguments:
- tokens: bfloat16 [16384, 768], P('dp'), may hold values from -6 to 6
- memory: bfloat16 [16384, 768], P('dp'), may hold values from -6 to 6
- segment: int32 [16384], P('dp'), may hold values from 0 to 3, as said below
- cotangent: bfloat16 [16384, 768], P('dp'), may hold values from -6 to 6
- self_query: bfloat16 [768, 768], P(None, 'tensor'), may hold values from -0.21875 to 0.21875
- self_query_bias: bfloat16 [768], P('tensor'), may hold values from -3 to 3
- self_key: bfloat16 [768, 768], P(None, 'tensor'), may hold values from -0.21875 to 0.21875
- self_value: bfloat16 [768, 768], P(None, 'tensor'), may hold values from -0.21875 to 0.21875
- self_value_bias: bfloat16 [768], P('tensor'), may hold values from -3 to 3
- self_output: bfloat16 [768, 768], P('tensor'), may hold values from -0.75 to 0.75
- self_output_bias: bfloat16 [768], replicated, may hold values from -3 to 3
- cross_query: bfloat16 [768, 768], P(None, 'tensor'), may hold values from -0.21875 to 0.21875
- cross_query_bias: bfloat16 [768], P('tensor'), may hold values from -3 to 3
- cross_key: bfloat16 [768, 768], P(None, 'tensor'), may hold values from -0.21875 to 0.21875
- cross_value: bfloat16 [768, 768], P(None, 'tensor'), may hold values from -0.21875 to 0.21875
- cross_value_bias: bfloat16 [768], P('tensor'), may hold values from -3 to 3
- cross_output: bfloat16 [768, 768], P('tensor'), may hold values from -0.75 to 0.75
- cross_output_bias: bfloat16 [768], replicated, may hold values from -3 to 3
- first_gain: bfloat16 [768], replicated, may hold values from 0.5 to 1.5
- first_shift: bfloat16 [768], replicated, may hold values from -3 to 3
- second_gain: bfloat16 [768], replicated, may hold values from 0.5 to 1.5
- second_shift: bfloat16 [768], replicated, may hold values from -3 to 3
- third_gain: bfloat16 [768], replicated, may hold values from 0.5 to 1.5
- third_shift: bfloat16 [768], replicated, may hold values from -3 to 3
- inner_weight: bfloat16 [768, 3072], P(None, 'tensor'), may hold values from -0.21875 to 0.21875
- inner_bias: bfloat16 [3072], P('tensor'), may hold values from -3 to 3
- outer_weight: bfloat16 [3072, 768], P('tensor'), may hold values from -0.21875 to 0.21875
- outer_bias: bfloat16 [768], replicated, may hold values from -3 to 3
Outputs:
- output: bfloat16 [16384, 768], P('dp')
- grad_tokens: float32 [16384, 768], P(('dp', 'tensor'))
- grad_memory: float32 [16384, 768], P(('dp', 'tensor'))
- grad_self_query: float32 [768, 768], P('dp', 'tensor')
- grad_self_query_bias: float32 [768], P('tensor')
- grad_self_key: float32 [768, 768], P('dp', 'tensor')
- grad_self_value: float32 [768, 768], P('dp', 'tensor')
- grad_self_value_bias: float32 [768], P('tensor')
- grad_self_output: float32 [768, 768], P('tensor', 'dp')
- grad_self_output_bias: float32 [768], replicated
- grad_cross_query: float32 [768, 768], P('dp', 'tensor')
- grad_cross_query_bias: float32 [768], P('tensor')
- grad_cross_key: float32 [768, 768], P('dp', 'tensor')
- grad_cross_value: float32 [768, 768], P('dp', 'tensor')
- grad_cross_value_bias: float32 [768], P('tensor')
- grad_cross_output: float32 [768, 768], P('tensor', 'dp')
- grad_cross_output_bias: float32 [768], replicated
- grad_first_gain: float32 [768], replicated
- grad_first_shift: float32 [768], replicated
- grad_second_gain: float32 [768], replicated
- grad_second_shift: float32 [768], replicated
- grad_third_gain: float32 [768], replicated
- grad_third_shift: float32 [768], replicated
- grad_inner_weight: float32 [768, 3072], P('dp', 'tensor')
- grad_inner_bias: float32 [3072], P('tensor')
- grad_outer_weight: float32 [3072, 768], P('tensor', 'dp')
- grad_outer_bias: float32 [768], replicated
The draws below stay inside these ranges and needn't reach their ends.
Inputs may be any that keep to these rules, and one draw needn't show every extreme that they name: Within each block of 1024 consecutive positions the segment is either 0 throughout (one long row) or position // 256 (four rows of 256); half of the blocks are of each kind.
All inputs are finite; a program needn't handle non-finite values.
Results may differ from the reference program's by a relative error of at most 0.028.
Values may be sent and summed in bfloat16 or wider, within the bound.
A program may use at most 256 MiB of HBM per device.

```python
import jax
import jax.numpy as jnp
from jax import lax

D = 768
HEADS = 12
HD = 64
FF = 3072
LONG = 1024
SHORT = 256
TOKENS = 16384


def draw_segment(key, part):
    blocks = TOKENS // LONG
    shuffled = jax.random.permutation(key, jnp.arange(blocks, dtype=jnp.int32))
    block_kind = shuffled % 2
    within = jnp.arange(LONG, dtype=jnp.int32) // SHORT
    table = block_kind[:, None] * within[None, :]
    return table.reshape(TOKENS).astype(jnp.int32)


def level_of(key, shape, pieces, least, top_value):
    def one(position, parts):
        heights = jax.random.uniform(jax.random.fold_in(jax.random.fold_in(key, 6), position), (parts,), jnp.float32, least / len(pieces), top_value / len(pieces))
        return jnp.repeat(jnp.exp(heights), shape[position] // parts).reshape((-1,) + (1,) * (len(shape) - position - 1))

    loudness = one(*pieces[0])
    for cut in pieces[1:]:
        loudness = loudness * one(*cut)
    return loudness


def gaussian(stream_key, extent, scale, limit, shards=(), held_as=jnp.bfloat16):
    values = jax.random.normal(stream_key, extent, jnp.float32) * scale
    if len(shards) > 0:
        values = level_of(stream_key, extent, shards, -0.22, 0.18) * values
    return jnp.clip(values, min=-limit, max=limit).astype(held_as)


def setup_inputs(seed: int = 0) -> dict:
    key_of = jax.random.split(jax.random.key(seed), 29)
    return {
        "tokens": gaussian(key_of[0], (TOKENS, D), 1.0, 6.0, ((0, 16),)),
        "memory": gaussian(key_of[1], (TOKENS, D), 1.0, 6.0, ((0, 16),)),
        "segment": draw_segment(jax.random.fold_in(key_of[28], 71), 0),
        "cotangent": gaussian(key_of[3], (TOKENS, D), 1.0, 6.0, ((0, 16),)),
        "self_query": gaussian(key_of[4], (D, D), D ** -0.5, 0.21875, ((1, 2),)),
        "self_query_bias": gaussian(key_of[5], (D,), 0.5, 3.0, ((0, 2),)),
        "self_key": gaussian(key_of[6], (D, D), D ** -0.5, 0.21875, ((1, 2),)),
        "self_value": gaussian(key_of[7], (D, D), D ** -0.5, 0.21875, ((1, 2),)),
        "self_value_bias": gaussian(key_of[8], (D,), 0.5, 3.0, ((0, 2),)),
        "self_output": gaussian(key_of[9], (D, D), HD ** -0.5, 0.75, ((0, 2),)),
        "self_output_bias": gaussian(key_of[10], (D,), 0.5, 3.0),
        "cross_query": gaussian(key_of[11], (D, D), D ** -0.5, 0.21875, ((1, 2),)),
        "cross_query_bias": gaussian(key_of[12], (D,), 0.5, 3.0, ((0, 2),)),
        "cross_key": gaussian(key_of[13], (D, D), D ** -0.5, 0.21875, ((1, 2),)),
        "cross_value": gaussian(key_of[14], (D, D), D ** -0.5, 0.21875, ((1, 2),)),
        "cross_value_bias": gaussian(key_of[15], (D,), 0.5, 3.0, ((0, 2),)),
        "cross_output": gaussian(key_of[16], (D, D), HD ** -0.5, 0.75, ((0, 2),)),
        "cross_output_bias": gaussian(key_of[17], (D,), 0.5, 3.0),
        "first_gain": jnp.clip(1.0 + 0.1 * jax.random.normal(key_of[18], (D,), jnp.float32), 0.5, 1.5).astype(jnp.bfloat16),
        "first_shift": gaussian(key_of[19], (D,), 0.5, 3.0),
        "second_gain": jnp.clip(1.0 + 0.1 * jax.random.normal(key_of[20], (D,), jnp.float32), 0.5, 1.5).astype(jnp.bfloat16),
        "second_shift": gaussian(key_of[21], (D,), 0.5, 3.0),
        "third_gain": jnp.clip(1.0 + 0.1 * jax.random.normal(key_of[22], (D,), jnp.float32), 0.5, 1.5).astype(jnp.bfloat16),
        "third_shift": gaussian(key_of[23], (D,), 0.5, 3.0),
        "inner_weight": gaussian(key_of[24], (D, FF), D ** -0.5, 0.21875, ((1, 2),)),
        "inner_bias": gaussian(key_of[25], (FF,), 0.5, 3.0, ((0, 2),)),
        "outer_weight": gaussian(key_of[26], (FF, D), (FF // 4) ** -0.5, 0.21875, ((0, 2),)),
        "outer_bias": gaussian(key_of[27], (D,), 0.5, 3.0),
    }


EPSILON = 1e-05
HIGHEST = lax.Precision.HIGHEST

@jax.custom_vjp
def low(v):
    return lax.optimization_barrier(v.astype(jnp.bfloat16)).astype(jnp.float32)

@jax.custom_vjp
def low_back(v):
    return v

def low_keep(v):
    return (low(v), None)

def low_pass(kept, grad):
    return (grad,)

def back_keep(v):
    return (v, None)

def back_low(kept, grad):
    return (low(grad),)
low.defvjp(low_keep, low_pass)
low_back.defvjp(back_keep, back_low)

def rounded_both(value):
    return low(low_back(value))

def product(left, right):
    return jnp.dot(left, right, precision=HIGHEST, preferred_element_type=jnp.float32)

def normalize(hidden, gain, shift):
    center = hidden - lax.optimization_barrier(jnp.mean(hidden, -1, keepdims=True))
    spread = lax.optimization_barrier(jnp.mean(center * center, -1, keepdims=True))
    return center * lax.rsqrt(spread + EPSILON) * gain + shift

def attention(queries, keys, values, segment, causal):
    length = queries.shape[0]
    block_rows = min(512, length)
    count = length // block_rows
    places = jnp.arange(length, dtype=jnp.int32)

    def per_block(inputs):
        query_block, place_block, segment_block = inputs
        scores = low_back(jnp.einsum('qhe,khe->hqk', query_block, keys, precision=HIGHEST))
        allowed = segment_block[:, None] == segment[None, :]
        if causal:
            allowed = allowed & (places[None, :] <= place_block[:, None])
        scores = jnp.where(allowed[None], scores, -1e+30)
        highest = lax.optimization_barrier(jnp.max(scores, -1, keepdims=True))
        powers = jnp.exp(scores - highest)
        weights = powers / lax.optimization_barrier(jnp.sum(powers, -1, keepdims=True))
        return jnp.einsum('hqk,khe->qhe', low(weights), values, precision=HIGHEST)
    result = lax.map(jax.checkpoint(per_block), (queries.reshape(count, block_rows, HEADS, HD), places.reshape(count, block_rows), segment.reshape(count, block_rows)))
    return result.reshape(length, HEADS * HD)

def forward(params, tokens, memory, segment):
    self_query, self_query_bias, self_key, self_value, self_value_bias, self_output, self_output_bias, cross_query, cross_query_bias, cross_key, cross_value, cross_value_bias, cross_output, cross_output_bias, first_gain, first_shift, second_gain, second_shift, third_gain, third_shift, inner_weight, inner_bias, outer_weight, outer_bias = params
    length = tokens.shape[0]
    scale = HD ** (-0.5)
    queries = rounded_both((product(tokens, self_query) + self_query_bias) * scale).reshape(length, HEADS, HD)
    keys = rounded_both(product(tokens, self_key)).reshape(length, HEADS, HD)
    values = rounded_both(product(tokens, self_value) + self_value_bias).reshape(length, HEADS, HD)
    context = rounded_both(attention(queries, keys, values, segment, True))
    branch = low_back(product(context, self_output) + self_output_bias)
    first = normalize(tokens + branch, first_gain, first_shift)
    first_low = low(first)
    cross_queries = rounded_both((product(first_low, cross_query) + cross_query_bias) * scale).reshape(length, HEADS, HD)
    cross_keys = rounded_both(product(memory, cross_key)).reshape(length, HEADS, HD)
    cross_values = rounded_both(product(memory, cross_value) + cross_value_bias).reshape(length, HEADS, HD)
    cross_context = rounded_both(attention(cross_queries, cross_keys, cross_values, segment, False))
    cross_branch = low_back(product(cross_context, cross_output) + cross_output_bias)
    second = normalize(first + cross_branch, second_gain, second_shift)
    inner = low_back(product(low(second), inner_weight) + inner_bias)
    hidden = low(jax.nn.gelu(inner, approximate=False))
    outer = low_back(product(hidden, outer_weight) + outer_bias)
    return normalize(second + outer, third_gain, third_shift)

def reference(tokens, memory, segment, cotangent, self_query, self_query_bias, self_key, self_value, self_value_bias, self_output, self_output_bias, cross_query, cross_query_bias, cross_key, cross_value, cross_value_bias, cross_output, cross_output_bias, first_gain, first_shift, second_gain, second_shift, third_gain, third_shift, inner_weight, inner_bias, outer_weight, outer_bias):
    params = tuple((weight.astype(jnp.float32) for weight in (self_query, self_query_bias, self_key, self_value, self_value_bias, self_output, self_output_bias, cross_query, cross_query_bias, cross_key, cross_value, cross_value_bias, cross_output, cross_output_bias, first_gain, first_shift, second_gain, second_shift, third_gain, third_shift, inner_weight, inner_bias, outer_weight, outer_bias)))
    blocks = TOKENS // LONG

    def advance(totals, portion):
        token_block, memory_block, segment_block, cotangent_block = portion

        def evaluate(params_in, token_in, memory_in):
            return forward(params_in, token_in, memory_in, segment_block)
        result, pullback = jax.vjp(evaluate, params, token_block, memory_block)
        grad_params, grad_token, grad_mem = pullback(cotangent_block)
        totals = jax.tree.map(jnp.add, totals, grad_params)
        return (totals, (result.astype(jnp.bfloat16), grad_token, grad_mem))
    starting = jax.tree.map(jnp.zeros_like, params)
    totals, (results, grad_token_blocks, grad_memory_blocks) = lax.scan(advance, starting, (tokens.astype(jnp.float32).reshape(blocks, LONG, D), memory.astype(jnp.float32).reshape(blocks, LONG, D), segment.reshape(blocks, LONG), cotangent.astype(jnp.float32).reshape(blocks, LONG, D)))
    grad_self_query, grad_self_query_bias, grad_self_key, grad_self_value, grad_self_value_bias, grad_self_output, grad_self_output_bias, grad_cross_query, grad_cross_query_bias, grad_cross_key, grad_cross_value, grad_cross_value_bias, grad_cross_output, grad_cross_output_bias, grad_first_gain, grad_first_shift, grad_second_gain, grad_second_shift, grad_third_gain, grad_third_shift, grad_inner_weight, grad_inner_bias, grad_outer_weight, grad_outer_bias = totals
    return (results.reshape(TOKENS, D), grad_token_blocks.reshape(TOKENS, D), grad_memory_blocks.reshape(TOKENS, D), grad_self_query, grad_self_query_bias, grad_self_key, grad_self_value, grad_self_value_bias, grad_self_output, grad_self_output_bias, grad_cross_query, grad_cross_query_bias, grad_cross_key, grad_cross_value, grad_cross_value_bias, grad_cross_output, grad_cross_output_bias, grad_first_gain, grad_first_shift, grad_second_gain, grad_second_shift, grad_third_gain, grad_third_shift, grad_inner_weight, grad_inner_bias, grad_outer_weight, grad_outer_bias)
```

```python
from functools import partial

import jax
import jax.numpy as jnp
from jax import lax
from jax.sharding import PartitionSpec as P

HD = 64


EPSILON = 1e-05
NEGATIVE = -1e30


def normalize(hidden, gain, shift):
    center = hidden - jnp.mean(hidden, -1, keepdims=True)
    spread = jnp.mean(center * center, -1, keepdims=True)
    return center * lax.rsqrt(spread + EPSILON) * gain + shift


def project(data, weight):
    return jnp.dot(data, weight, preferred_element_type=jnp.float32)


def column_sums(values):
    return jnp.sum(values.astype(jnp.float32), 0)


def heads_of(matrix):
    return matrix.reshape(matrix.shape[0], -1, HD)


def allowed_pairs(query_segment, key_segment, start, causal):
    same = query_segment[:, None] == key_segment[None, :]
    if causal:
        query_place = start + jnp.arange(query_segment.shape[0], dtype=jnp.int32)
        key_place = jnp.arange(key_segment.shape[0], dtype=jnp.int32)
        same = same & (key_place[None, :] <= query_place[:, None])
    return same[None]


def attend_forward(queries, keys, values, segment, causal):
    length = queries.shape[0]
    block_rows = min(512, length)
    contexts = []
    totals = []
    for index in range(length // block_rows):
        start = index * block_rows
        piece = queries[start : start + block_rows]
        scores = jnp.einsum("qhe,khe->hqk", piece, keys, preferred_element_type=jnp.float32)
        scores = jnp.where(
            allowed_pairs(segment[start : start + block_rows], segment, start, causal),
            scores,
            NEGATIVE,
        )
        highest = jnp.max(scores, -1, keepdims=True)
        powers = jnp.exp(scores - highest)
        summed = jnp.sum(powers, -1, keepdims=True)
        weights = (powers / summed).astype(jnp.bfloat16)
        contexts.append(
            jnp.einsum("hqk,khe->qhe", weights, values, preferred_element_type=jnp.float32)
        )
        totals.append(highest + jnp.log(summed))
    return (jnp.concatenate(contexts, 0), jnp.concatenate(totals, 1))


def attend_backward(queries, keys, values, grad_context, totals, segment, causal):
    length = queries.shape[0]
    block_rows = min(512, length)
    grad_queries = []
    grad_keys = jnp.zeros(keys.shape, jnp.float32)
    grad_values = jnp.zeros(values.shape, jnp.float32)
    for index in range(length // block_rows):
        start = index * block_rows
        piece = queries[start : start + block_rows]
        grad_piece = grad_context[start : start + block_rows]
        scores = jnp.einsum("qhe,khe->hqk", piece, keys, preferred_element_type=jnp.float32)
        scores = jnp.where(
            allowed_pairs(segment[start : start + block_rows], segment, start, causal),
            scores,
            NEGATIVE,
        )
        probs = jnp.exp(scores - totals[:, start : start + block_rows])
        grad_probs = jnp.einsum(
            "qhe,khe->hqk", grad_piece, values, preferred_element_type=jnp.float32
        )
        row_inner = jnp.sum(grad_probs * probs, -1, keepdims=True)
        grad_scores = (probs * (grad_probs - row_inner)).astype(jnp.bfloat16)
        grad_queries.append(
            jnp.einsum("hqk,khe->qhe", grad_scores, keys, preferred_element_type=jnp.float32)
        )
        grad_keys = grad_keys + jnp.einsum(
            "hqk,qhe->khe", grad_scores, piece, preferred_element_type=jnp.float32
        )
        grad_values = grad_values + jnp.einsum(
            "hqk,qhe->khe",
            probs.astype(jnp.bfloat16),
            grad_piece,
            preferred_element_type=jnp.float32,
        )
    return (jnp.concatenate(grad_queries, 0), grad_keys, grad_values)


def on_device(
    tokens,
    memory,
    segment,
    cotangent,
    self_query,
    self_query_bias,
    self_key,
    self_value,
    self_value_bias,
    self_output,
    self_output_bias,
    cross_query,
    cross_query_bias,
    cross_key,
    cross_value,
    cross_value_bias,
    cross_output,
    cross_output_bias,
    first_gain,
    first_shift,
    second_gain,
    second_shift,
    third_gain,
    third_shift,
    inner_weight,
    inner_bias,
    outer_weight,
    outer_bias,
):
    scale = HD ** (-0.5)
    length = tokens.shape[0]
    groups = lax.axis_size("tensor")
    member = lax.axis_index("tensor")
    half = length // groups

    def rows_of(values):
        return lax.dynamic_slice_in_dim(values, member * half, half, 0)

    def spread_out(values):
        whole = jnp.zeros((values.shape[0] * groups,), jnp.float32)
        return lax.dynamic_update_slice_in_dim(whole, values, member * values.shape[0], 0)

    def own_share(values, count):
        return lax.dynamic_slice_in_dim(values, member * count, count, 0)

    queries = ((project(tokens, self_query) + self_query_bias.astype(jnp.float32)) * scale).astype(
        jnp.bfloat16
    )
    keys = project(tokens, self_key).astype(jnp.bfloat16)
    values = (project(tokens, self_value) + self_value_bias.astype(jnp.float32)).astype(
        jnp.bfloat16
    )
    self_queries = heads_of(queries)
    self_keys = heads_of(keys)
    self_values = heads_of(values)
    self_context, self_totals = attend_forward(self_queries, self_keys, self_values, segment, True)
    self_context = self_context.reshape(length, -1).astype(jnp.bfloat16)
    attended = lax.psum_scatter(
        project(self_context, self_output), "tensor", scatter_dimension=0, tiled=True
    ) + self_output_bias.astype(jnp.float32)
    first, first_back = jax.vjp(
        normalize,
        rows_of(tokens).astype(jnp.float32) + attended,
        first_gain.astype(jnp.float32),
        first_shift.astype(jnp.float32),
    )
    first_low = lax.all_gather(first.astype(jnp.bfloat16), "tensor", axis=0, tiled=True)
    queries = (
        (project(first_low, cross_query) + cross_query_bias.astype(jnp.float32)) * scale
    ).astype(jnp.bfloat16)
    keys = project(memory, cross_key).astype(jnp.bfloat16)
    values = (project(memory, cross_value) + cross_value_bias.astype(jnp.float32)).astype(
        jnp.bfloat16
    )
    cross_queries = heads_of(queries)
    cross_keys = heads_of(keys)
    cross_values = heads_of(values)
    cross_context, cross_totals = attend_forward(
        cross_queries, cross_keys, cross_values, segment, False
    )
    cross_context = cross_context.reshape(length, -1).astype(jnp.bfloat16)
    crossed = lax.psum_scatter(
        project(cross_context, cross_output).astype(jnp.bfloat16),
        "tensor",
        scatter_dimension=0,
        tiled=True,
    ).astype(jnp.float32) + cross_output_bias.astype(jnp.float32)
    second_part, second_back = jax.vjp(
        normalize,
        first + crossed,
        second_gain.astype(jnp.float32),
        second_shift.astype(jnp.float32),
    )
    second = lax.all_gather(second_part.astype(jnp.bfloat16), "tensor", axis=0, tiled=True).astype(
        second_part.dtype
    )
    second_low = second.astype(jnp.bfloat16)
    inner = project(second_low, inner_weight) + inner_bias.astype(jnp.float32)
    hidden = jax.nn.gelu(inner, approximate=False).astype(jnp.bfloat16)
    outer = lax.psum(project(hidden, outer_weight).astype(jnp.bfloat16), "tensor").astype(
        jnp.float32
    ) + outer_bias.astype(jnp.float32)
    result, third_back = jax.vjp(
        normalize, second + outer, third_gain.astype(jnp.float32), third_shift.astype(jnp.float32)
    )
    output = result.astype(jnp.bfloat16)
    grad_third, grad_third_gain, grad_third_shift = third_back(cotangent.astype(jnp.float32))
    grad_outer = grad_third.astype(jnp.bfloat16)
    grad_outer_bias = column_sums(grad_outer)
    gelu_back = jax.vjp(partial(jax.nn.gelu, approximate=False), inner)[1]
    grad_inner = gelu_back(project(grad_outer, outer_weight.T))[0].astype(jnp.bfloat16)
    grad_inner_weight = project(second_low.T, grad_inner)
    grad_inner_bias = column_sums(grad_inner)
    grad_second = rows_of(grad_third) + lax.psum_scatter(
        project(grad_inner, inner_weight.T).astype(jnp.bfloat16),
        "tensor",
        scatter_dimension=0,
        tiled=True,
    ).astype(jnp.float32)
    grad_second_in, grad_second_gain, grad_second_shift = second_back(grad_second)
    grad_cross_rows = grad_second_in.astype(jnp.bfloat16)
    grad_cross_output_bias = column_sums(grad_cross_rows)
    grad_cross = lax.all_gather(grad_cross_rows, "tensor", axis=0, tiled=True)
    grad_cross_context = heads_of(project(grad_cross, cross_output.T).astype(jnp.bfloat16))
    cross_grad_q, cross_grad_k, cross_grad_v = attend_backward(
        cross_queries, cross_keys, cross_values, grad_cross_context, cross_totals, segment, False
    )
    cross_grad_q = (cross_grad_q.astype(jnp.bfloat16) * scale).reshape(length, -1)
    cross_grad_k = cross_grad_k.astype(jnp.bfloat16).reshape(length, -1)
    cross_grad_v = cross_grad_v.astype(jnp.bfloat16).reshape(length, -1)
    grad_cross_query = project(first_low.T, cross_grad_q)
    grad_cross_query_bias = column_sums(cross_grad_q)
    grad_cross_key = project(memory.T, cross_grad_k)
    grad_cross_value = project(memory.T, cross_grad_v)
    grad_cross_value_bias = column_sums(cross_grad_v)
    memory_term = project(cross_grad_k, cross_key.T) + project(cross_grad_v, cross_value.T)
    grad_first = grad_second_in + lax.psum_scatter(
        project(cross_grad_q, cross_query.T).astype(jnp.bfloat16),
        "tensor",
        scatter_dimension=0,
        tiled=True,
    ).astype(jnp.float32)
    grad_first_in, grad_first_gain, grad_first_shift = first_back(grad_first)
    grad_self_rows = grad_first_in.astype(jnp.bfloat16)
    grad_self_output_bias = column_sums(grad_self_rows)
    grad_self = lax.all_gather(grad_self_rows, "tensor", axis=0, tiled=True)
    grad_self_context = heads_of(project(grad_self, self_output.T).astype(jnp.bfloat16))
    self_grad_q, self_grad_k, self_grad_v = attend_backward(
        self_queries, self_keys, self_values, grad_self_context, self_totals, segment, True
    )
    self_grad_q = (self_grad_q.astype(jnp.bfloat16) * scale).reshape(length, -1)
    self_grad_k = self_grad_k.astype(jnp.bfloat16).reshape(length, -1)
    self_grad_v = self_grad_v.astype(jnp.bfloat16).reshape(length, -1)
    grad_self_query = project(tokens.T, self_grad_q)
    grad_self_query_bias = column_sums(self_grad_q)
    grad_self_key = project(tokens.T, self_grad_k)
    grad_self_value = project(tokens.T, self_grad_v)
    grad_self_value_bias = column_sums(self_grad_v)
    tokens_term = (
        project(self_grad_q, self_query.T)
        + project(self_grad_k, self_key.T)
        + project(self_grad_v, self_value.T)
    )
    tokens_part, memory_part = (
        lax.psum_scatter(
            tokens_term.astype(jnp.bfloat16), "tensor", scatter_dimension=0, tiled=True
        ).astype(jnp.float32),
        lax.psum_scatter(
            memory_term.astype(jnp.bfloat16), "tensor", scatter_dimension=0, tiled=True
        ).astype(jnp.float32),
    )
    grad_tokens = tokens_part + grad_first_in
    grad_self_output_t = project(grad_self.T, self_context)
    grad_cross_output_t = project(grad_cross.T, cross_context)
    grad_outer_weight_t = project(grad_outer.T, hidden)
    gathered = [
        grad_self_query,
        grad_self_key,
        grad_self_value,
        grad_self_output_t,
        grad_cross_query,
        grad_cross_key,
        grad_cross_value,
        grad_cross_output_t,
        grad_inner_weight,
        grad_outer_weight_t,
    ]
    widths = [piece.shape[1] for piece in gathered]
    summed = lax.psum_scatter(
        jnp.concatenate(gathered, 1), "dp", scatter_dimension=0, tiled=True
    )
    everything = []
    offset = 0
    for position, width in enumerate(widths):
        piece = summed[:, offset : offset + width]
        offset += width
        if position in (3, 7, 9):
            piece = piece.T
        everything.append(piece)
    self_sums = everything[0:4]
    cross_sums = everything[4:8]
    ffn_sums = everything[8:10]
    head_columns = grad_self_query_bias.shape[0]
    unit_columns = grad_inner_bias.shape[0]
    smalls = lax.psum(
        (
            spread_out(grad_self_query_bias),
            spread_out(grad_self_value_bias),
            grad_self_output_bias,
            spread_out(grad_cross_query_bias),
            spread_out(grad_cross_value_bias),
            grad_cross_output_bias,
            grad_first_gain,
            grad_first_shift,
            grad_second_gain,
            grad_second_shift,
            grad_third_gain * 0.5,
            grad_third_shift * 0.5,
            spread_out(grad_inner_bias),
            grad_outer_bias * 0.5,
        ),
        ("dp", "tensor"),
    )
    return (
        output,
        grad_tokens,
        memory_part,
        self_sums[0],
        own_share(smalls[0], head_columns),
        self_sums[1],
        self_sums[2],
        own_share(smalls[1], head_columns),
        self_sums[3],
        smalls[2],
        cross_sums[0],
        own_share(smalls[3], head_columns),
        cross_sums[1],
        cross_sums[2],
        own_share(smalls[4], head_columns),
        cross_sums[3],
        smalls[5],
        smalls[6],
        smalls[7],
        smalls[8],
        smalls[9],
        smalls[10],
        smalls[11],
        ffn_sums[0],
        own_share(smalls[12], unit_columns),
        ffn_sums[1],
        smalls[13],
    )


def solution(mesh):
    return jax.shard_map(
        on_device,
        mesh=mesh,
        in_specs=(
            P("dp", None),
            P("dp", None),
            P("dp"),
            P("dp", None),
            P(None, "tensor"),
            P("tensor"),
            P(None, "tensor"),
            P(None, "tensor"),
            P("tensor"),
            P("tensor", None),
            P(),
            P(None, "tensor"),
            P("tensor"),
            P(None, "tensor"),
            P(None, "tensor"),
            P("tensor"),
            P("tensor", None),
            P(),
            P(),
            P(),
            P(),
            P(),
            P(),
            P(),
            P(None, "tensor"),
            P("tensor"),
            P("tensor", None),
            P(),
        ),
        out_specs=(
            P("dp", None),
            P(("dp", "tensor"), None),
            P(("dp", "tensor"), None),
            P("dp", "tensor"),
            P("tensor"),
            P("dp", "tensor"),
            P("dp", "tensor"),
            P("tensor"),
            P("tensor", "dp"),
            P(),
            P("dp", "tensor"),
            P("tensor"),
            P("dp", "tensor"),
            P("dp", "tensor"),
            P("tensor"),
            P("tensor", "dp"),
            P(),
            P(),
            P(),
            P(),
            P(),
            P(),
            P(),
            P("dp", "tensor"),
            P("tensor"),
            P("tensor", "dp"),
            P(),
        ),
        check_vma=False,
    )
```

```python
from functools import partial

import jax
import jax.numpy as jnp
from jax import lax
from jax.sharding import PartitionSpec as P

HD = 64


EPSILON = 1e-05
NEGATIVE = -1e30


def normalize(hidden, gain, shift):
    center = hidden - jnp.mean(hidden, -1, keepdims=True)
    spread = jnp.mean(center * center, -1, keepdims=True)
    return center * lax.rsqrt(spread + EPSILON) * gain + shift


def project(data, weight):
    return jnp.dot(data, weight, preferred_element_type=jnp.float32)


def column_sums(values):
    return jnp.sum(values.astype(jnp.float32), 0)


def heads_of(matrix):
    return matrix.reshape(matrix.shape[0], -1, HD)


def allowed_pairs(query_segment, key_segment, start, causal):
    same = query_segment[:, None] == key_segment[None, :]
    if causal:
        query_place = start + jnp.arange(query_segment.shape[0], dtype=jnp.int32)
        key_place = jnp.arange(key_segment.shape[0], dtype=jnp.int32)
        same = same & (key_place[None, :] <= query_place[:, None])
    return same[None]


def attend_forward(queries, keys, values, segment, causal):
    length = queries.shape[0]
    block_rows = min(512, length)
    contexts = []
    totals = []
    for index in range(length // block_rows):
        start = index * block_rows
        piece = queries[start : start + block_rows]
        scores = jnp.einsum("qhe,khe->hqk", piece, keys, preferred_element_type=jnp.float32)
        scores = jnp.where(
            allowed_pairs(segment[start : start + block_rows], segment, start, causal),
            scores,
            NEGATIVE,
        )
        highest = jnp.max(scores, -1, keepdims=True)
        powers = jnp.exp(scores - highest)
        summed = jnp.sum(powers, -1, keepdims=True)
        weights = (powers / summed).astype(jnp.bfloat16)
        contexts.append(
            jnp.einsum("hqk,khe->qhe", weights, values, preferred_element_type=jnp.float32)
        )
        totals.append(highest + jnp.log(summed))
    return (jnp.concatenate(contexts, 0), jnp.concatenate(totals, 1))


def attend_backward(queries, keys, values, grad_context, totals, segment, causal):
    length = queries.shape[0]
    block_rows = min(512, length)
    grad_queries = []
    grad_keys = jnp.zeros(keys.shape, jnp.float32)
    grad_values = jnp.zeros(values.shape, jnp.float32)
    for index in range(length // block_rows):
        start = index * block_rows
        piece = queries[start : start + block_rows]
        grad_piece = grad_context[start : start + block_rows]
        scores = jnp.einsum("qhe,khe->hqk", piece, keys, preferred_element_type=jnp.float32)
        scores = jnp.where(
            allowed_pairs(segment[start : start + block_rows], segment, start, causal),
            scores,
            NEGATIVE,
        )
        probs = jnp.exp(scores - totals[:, start : start + block_rows])
        grad_probs = jnp.einsum(
            "qhe,khe->hqk", grad_piece, values, preferred_element_type=jnp.float32
        )
        row_inner = jnp.sum(grad_probs * probs, -1, keepdims=True)
        grad_scores = (probs * (grad_probs - row_inner)).astype(jnp.bfloat16)
        grad_queries.append(
            jnp.einsum("hqk,khe->qhe", grad_scores, keys, preferred_element_type=jnp.float32)
        )
        grad_keys = grad_keys + jnp.einsum(
            "hqk,qhe->khe", grad_scores, piece, preferred_element_type=jnp.float32
        )
        grad_values = grad_values + jnp.einsum(
            "hqk,qhe->khe",
            probs.astype(jnp.bfloat16),
            grad_piece,
            preferred_element_type=jnp.float32,
        )
    return (jnp.concatenate(grad_queries, 0), grad_keys, grad_values)


def on_device(
    tokens,
    memory,
    segment,
    cotangent,
    self_query,
    self_query_bias,
    self_key,
    self_value,
    self_value_bias,
    self_output,
    self_output_bias,
    cross_query,
    cross_query_bias,
    cross_key,
    cross_value,
    cross_value_bias,
    cross_output,
    cross_output_bias,
    first_gain,
    first_shift,
    second_gain,
    second_shift,
    third_gain,
    third_shift,
    inner_weight,
    inner_bias,
    outer_weight,
    outer_bias,
):
    scale = HD ** (-0.5)
    length = tokens.shape[0]
    groups = lax.axis_size("tensor")
    member = lax.axis_index("tensor")
    half = length // groups

    def rows_of(values):
        return lax.dynamic_slice_in_dim(values, member * half, half, 0)

    def spread_out(values):
        whole = jnp.zeros((values.shape[0] * groups,), jnp.float32)
        return lax.dynamic_update_slice_in_dim(whole, values, member * values.shape[0], 0)

    def own_share(values, count):
        return lax.dynamic_slice_in_dim(values, member * count, count, 0)

    def swap(values):
        return lax.ppermute(values, "tensor", [(0, 1), (1, 0)])

    def gather_rows(values):
        if groups != 2:
            return lax.all_gather(values, "tensor", axis=0, tiled=True)
        other = swap(values)
        lead = member == 0
        return jnp.concatenate(
            [jnp.where(lead, values, other), jnp.where(lead, other, values)], 0
        )

    def scatter_rows(values):
        if groups != 2:
            return lax.psum_scatter(
                values, "tensor", scatter_dimension=0, tiled=True
            ).astype(jnp.float32)
        top = values[:half]
        bottom = values[half:]
        lead = member == 0
        keep = jnp.where(lead, top, bottom)
        send = jnp.where(lead, bottom, top)
        return keep.astype(jnp.float32) + swap(send).astype(jnp.float32)

    def sum_pair(values):
        if groups != 2:
            return lax.psum(values, "tensor").astype(jnp.float32)
        return values.astype(jnp.float32) + swap(values).astype(jnp.float32)

    queries = ((project(tokens, self_query) + self_query_bias.astype(jnp.float32)) * scale).astype(
        jnp.bfloat16
    )
    keys = project(tokens, self_key).astype(jnp.bfloat16)
    values = (project(tokens, self_value) + self_value_bias.astype(jnp.float32)).astype(
        jnp.bfloat16
    )
    self_queries = heads_of(queries)
    self_keys = heads_of(keys)
    self_values = heads_of(values)
    self_context, self_totals = attend_forward(self_queries, self_keys, self_values, segment, True)
    self_context = self_context.reshape(length, -1).astype(jnp.bfloat16)
    attended = scatter_rows(project(self_context, self_output)) + self_output_bias.astype(
        jnp.float32
    )
    first, first_back = jax.vjp(
        normalize,
        rows_of(tokens).astype(jnp.float32) + attended,
        first_gain.astype(jnp.float32),
        first_shift.astype(jnp.float32),
    )
    first_low = gather_rows(first.astype(jnp.bfloat16))
    queries = (
        (project(first_low, cross_query) + cross_query_bias.astype(jnp.float32)) * scale
    ).astype(jnp.bfloat16)
    keys = project(memory, cross_key).astype(jnp.bfloat16)
    values = (project(memory, cross_value) + cross_value_bias.astype(jnp.float32)).astype(
        jnp.bfloat16
    )
    cross_queries = heads_of(queries)
    cross_keys = heads_of(keys)
    cross_values = heads_of(values)
    cross_context, cross_totals = attend_forward(
        cross_queries, cross_keys, cross_values, segment, False
    )
    cross_context = cross_context.reshape(length, -1).astype(jnp.bfloat16)
    crossed = scatter_rows(
        project(cross_context, cross_output).astype(jnp.bfloat16)
    ) + cross_output_bias.astype(jnp.float32)
    second_part, second_back = jax.vjp(
        normalize,
        first + crossed,
        second_gain.astype(jnp.float32),
        second_shift.astype(jnp.float32),
    )
    second = gather_rows(second_part.astype(jnp.bfloat16)).astype(second_part.dtype)
    second_low = second.astype(jnp.bfloat16)
    inner = project(second_low, inner_weight) + inner_bias.astype(jnp.float32)
    hidden = jax.nn.gelu(inner, approximate=False).astype(jnp.bfloat16)
    outer = sum_pair(project(hidden, outer_weight).astype(jnp.bfloat16)) + outer_bias.astype(
        jnp.float32
    )
    result, third_back = jax.vjp(
        normalize, second + outer, third_gain.astype(jnp.float32), third_shift.astype(jnp.float32)
    )
    output = result.astype(jnp.bfloat16)
    grad_third, grad_third_gain, grad_third_shift = third_back(cotangent.astype(jnp.float32))
    grad_outer = grad_third.astype(jnp.bfloat16)
    grad_outer_bias = column_sums(grad_outer)
    gelu_back = jax.vjp(partial(jax.nn.gelu, approximate=False), inner)[1]
    grad_inner = gelu_back(project(grad_outer, outer_weight.T))[0].astype(jnp.bfloat16)
    grad_inner_weight = project(second_low.T, grad_inner)
    grad_inner_bias = column_sums(grad_inner)
    grad_second = rows_of(grad_third) + scatter_rows(
        project(grad_inner, inner_weight.T).astype(jnp.bfloat16)
    )
    grad_second_in, grad_second_gain, grad_second_shift = second_back(grad_second)
    grad_cross_rows = grad_second_in.astype(jnp.bfloat16)
    grad_cross_output_bias = column_sums(grad_cross_rows)
    grad_cross = gather_rows(grad_cross_rows)
    grad_cross_context = heads_of(project(grad_cross, cross_output.T).astype(jnp.bfloat16))
    cross_grad_q, cross_grad_k, cross_grad_v = attend_backward(
        cross_queries, cross_keys, cross_values, grad_cross_context, cross_totals, segment, False
    )
    cross_grad_q = (cross_grad_q.astype(jnp.bfloat16) * scale).reshape(length, -1)
    cross_grad_k = cross_grad_k.astype(jnp.bfloat16).reshape(length, -1)
    cross_grad_v = cross_grad_v.astype(jnp.bfloat16).reshape(length, -1)
    grad_cross_query = project(first_low.T, cross_grad_q)
    grad_cross_query_bias = column_sums(cross_grad_q)
    grad_cross_key = project(memory.T, cross_grad_k)
    grad_cross_value = project(memory.T, cross_grad_v)
    grad_cross_value_bias = column_sums(cross_grad_v)
    memory_term = project(cross_grad_k, cross_key.T) + project(cross_grad_v, cross_value.T)
    grad_first = grad_second_in + scatter_rows(
        project(cross_grad_q, cross_query.T).astype(jnp.bfloat16)
    )
    grad_first_in, grad_first_gain, grad_first_shift = first_back(grad_first)
    grad_self_rows = grad_first_in.astype(jnp.bfloat16)
    grad_self_output_bias = column_sums(grad_self_rows)
    grad_self = gather_rows(grad_self_rows)
    grad_self_context = heads_of(project(grad_self, self_output.T).astype(jnp.bfloat16))
    self_grad_q, self_grad_k, self_grad_v = attend_backward(
        self_queries, self_keys, self_values, grad_self_context, self_totals, segment, True
    )
    self_grad_q = (self_grad_q.astype(jnp.bfloat16) * scale).reshape(length, -1)
    self_grad_k = self_grad_k.astype(jnp.bfloat16).reshape(length, -1)
    self_grad_v = self_grad_v.astype(jnp.bfloat16).reshape(length, -1)
    grad_self_query = project(tokens.T, self_grad_q)
    grad_self_query_bias = column_sums(self_grad_q)
    grad_self_key = project(tokens.T, self_grad_k)
    grad_self_value = project(tokens.T, self_grad_v)
    grad_self_value_bias = column_sums(self_grad_v)
    tokens_term = (
        project(self_grad_q, self_query.T)
        + project(self_grad_k, self_key.T)
        + project(self_grad_v, self_value.T)
    )
    tokens_part = scatter_rows(tokens_term.astype(jnp.bfloat16))
    memory_part = scatter_rows(memory_term.astype(jnp.bfloat16))
    grad_tokens = tokens_part + grad_first_in
    grad_self_output_t = project(grad_self.T, self_context)
    grad_cross_output_t = project(grad_cross.T, cross_context)
    grad_outer_weight_t = project(grad_outer.T, hidden)
    gathered = [
        grad_self_query,
        grad_self_key,
        grad_self_value,
        grad_self_output_t,
        grad_cross_query,
        grad_cross_key,
        grad_cross_value,
        grad_cross_output_t,
        grad_inner_weight,
        grad_outer_weight_t,
    ]
    widths = [piece.shape[1] for piece in gathered]
    summed = lax.psum_scatter(
        jnp.concatenate(gathered, 1), "dp", scatter_dimension=0, tiled=True
    )
    everything = []
    offset = 0
    for position, width in enumerate(widths):
        piece = summed[:, offset : offset + width]
        offset += width
        if position in (3, 7, 9):
            piece = piece.T
        everything.append(piece)
    self_sums = everything[0:4]
    cross_sums = everything[4:8]
    ffn_sums = everything[8:10]
    head_columns = grad_self_query_bias.shape[0]
    unit_columns = grad_inner_bias.shape[0]
    smalls = lax.psum(
        (
            spread_out(grad_self_query_bias),
            spread_out(grad_self_value_bias),
            grad_self_output_bias,
            spread_out(grad_cross_query_bias),
            spread_out(grad_cross_value_bias),
            grad_cross_output_bias,
            grad_first_gain,
            grad_first_shift,
            grad_second_gain,
            grad_second_shift,
            grad_third_gain * 0.5,
            grad_third_shift * 0.5,
            spread_out(grad_inner_bias),
            grad_outer_bias * 0.5,
        ),
        ("dp", "tensor"),
    )
    return (
        output,
        grad_tokens,
        memory_part,
        self_sums[0],
        own_share(smalls[0], head_columns),
        self_sums[1],
        self_sums[2],
        own_share(smalls[1], head_columns),
        self_sums[3],
        smalls[2],
        cross_sums[0],
        own_share(smalls[3], head_columns),
        cross_sums[1],
        cross_sums[2],
        own_share(smalls[4], head_columns),
        cross_sums[3],
        smalls[5],
        smalls[6],
        smalls[7],
        smalls[8],
        smalls[9],
        smalls[10],
        smalls[11],
        ffn_sums[0],
        own_share(smalls[12], unit_columns),
        ffn_sums[1],
        smalls[13],
    )


def solution(mesh):
    return jax.shard_map(
        on_device,
        mesh=mesh,
        in_specs=(
            P("dp", None),
            P("dp", None),
            P("dp"),
            P("dp", None),
            P(None, "tensor"),
            P("tensor"),
            P(None, "tensor"),
            P(None, "tensor"),
            P("tensor"),
            P("tensor", None),
            P(),
            P(None, "tensor"),
            P("tensor"),
            P(None, "tensor"),
            P(None, "tensor"),
            P("tensor"),
            P("tensor", None),
            P(),
            P(),
            P(),
            P(),
            P(),
            P(),
            P(),
            P(None, "tensor"),
            P("tensor"),
            P("tensor", None),
            P(),
        ),
        out_specs=(
            P("dp", None),
            P(("dp", "tensor"), None),
            P(("dp", "tensor"), None),
            P("dp", "tensor"),
            P("tensor"),
            P("dp", "tensor"),
            P("dp", "tensor"),
            P("tensor"),
            P("tensor", "dp"),
            P(),
            P("dp", "tensor"),
            P("tensor"),
            P("dp", "tensor"),
            P("dp", "tensor"),
            P("tensor"),
            P("tensor", "dp"),
            P(),
            P(),
            P(),
            P(),
            P(),
            P(),
            P(),
            P("dp", "tensor"),
            P("tensor"),
            P("tensor", "dp"),
            P(),
        ),
        check_vma=False,
    )
```

```python
from functools import partial

import jax
import jax.numpy as jnp
from jax import lax
from jax.sharding import PartitionSpec as P

HD = 64


EPSILON = 1e-05
NEGATIVE = -1e30


def normalize(hidden, gain, shift):
    center = hidden - jnp.mean(hidden, -1, keepdims=True)
    spread = jnp.mean(center * center, -1, keepdims=True)
    return center * lax.rsqrt(spread + EPSILON) * gain + shift


def project(data, weight):
    return jnp.dot(data, weight, preferred_element_type=jnp.float32)


def column_sums(values):
    return jnp.sum(values.astype(jnp.float32), 0)


def heads_of(matrix):
    return matrix.reshape(matrix.shape[0], -1, HD)


def allowed_pairs(query_segment, key_segment, start, causal):
    same = query_segment[:, None] == key_segment[None, :]
    if causal:
        query_place = start + jnp.arange(query_segment.shape[0], dtype=jnp.int32)
        key_place = jnp.arange(key_segment.shape[0], dtype=jnp.int32)
        same = same & (key_place[None, :] <= query_place[:, None])
    return same[None]


def attend_forward(queries, keys, values, segment, causal):
    length = queries.shape[0]
    block_rows = min(512, length)
    contexts = []
    totals = []
    for index in range(length // block_rows):
        start = index * block_rows
        piece = queries[start : start + block_rows]
        scores = jnp.einsum("qhe,khe->hqk", piece, keys, preferred_element_type=jnp.float32)
        scores = jnp.where(
            allowed_pairs(segment[start : start + block_rows], segment, start, causal),
            scores,
            NEGATIVE,
        )
        highest = jnp.max(scores, -1, keepdims=True)
        powers = jnp.exp(scores - highest)
        summed = jnp.sum(powers, -1, keepdims=True)
        weights = (powers / summed).astype(jnp.bfloat16)
        contexts.append(
            jnp.einsum("hqk,khe->qhe", weights, values, preferred_element_type=jnp.float32)
        )
        totals.append(highest + jnp.log(summed))
    return (jnp.concatenate(contexts, 0), jnp.concatenate(totals, 1))


def attend_backward(queries, keys, values, grad_context, totals, segment, causal):
    length = queries.shape[0]
    block_rows = min(512, length)
    grad_queries = []
    grad_keys = jnp.zeros(keys.shape, jnp.float32)
    grad_values = jnp.zeros(values.shape, jnp.float32)
    for index in range(length // block_rows):
        start = index * block_rows
        piece = queries[start : start + block_rows]
        grad_piece = grad_context[start : start + block_rows]
        scores = jnp.einsum("qhe,khe->hqk", piece, keys, preferred_element_type=jnp.float32)
        scores = jnp.where(
            allowed_pairs(segment[start : start + block_rows], segment, start, causal),
            scores,
            NEGATIVE,
        )
        probs = jnp.exp(scores - totals[:, start : start + block_rows])
        grad_probs = jnp.einsum(
            "qhe,khe->hqk", grad_piece, values, preferred_element_type=jnp.float32
        )
        row_inner = jnp.sum(grad_probs * probs, -1, keepdims=True)
        grad_scores = (probs * (grad_probs - row_inner)).astype(jnp.bfloat16)
        grad_queries.append(
            jnp.einsum("hqk,khe->qhe", grad_scores, keys, preferred_element_type=jnp.float32)
        )
        grad_keys = grad_keys + jnp.einsum(
            "hqk,qhe->khe", grad_scores, piece, preferred_element_type=jnp.float32
        )
        grad_values = grad_values + jnp.einsum(
            "hqk,qhe->khe",
            probs.astype(jnp.bfloat16),
            grad_piece,
            preferred_element_type=jnp.float32,
        )
    return (jnp.concatenate(grad_queries, 0), grad_keys, grad_values)


def on_device(
    tokens,
    memory,
    segment,
    cotangent,
    self_query,
    self_query_bias,
    self_key,
    self_value,
    self_value_bias,
    self_output,
    self_output_bias,
    cross_query,
    cross_query_bias,
    cross_key,
    cross_value,
    cross_value_bias,
    cross_output,
    cross_output_bias,
    first_gain,
    first_shift,
    second_gain,
    second_shift,
    third_gain,
    third_shift,
    inner_weight,
    inner_bias,
    outer_weight,
    outer_bias,
):
    scale = HD ** (-0.5)
    length = tokens.shape[0]
    groups = lax.axis_size("tensor")
    member = lax.axis_index("tensor")
    half = length // groups

    def rows_of(values):
        return lax.dynamic_slice_in_dim(values, member * half, half, 0)

    def spread_out(values):
        whole = jnp.zeros((values.shape[0] * groups,), jnp.float32)
        return lax.dynamic_update_slice_in_dim(whole, values, member * values.shape[0], 0)

    def own_share(values, count):
        return lax.dynamic_slice_in_dim(values, member * count, count, 0)

    def swap(values):
        return lax.ppermute(values, "tensor", [(0, 1), (1, 0)])

    def gather_rows(values):
        if groups != 2:
            return lax.all_gather(values, "tensor", axis=0, tiled=True)
        other = swap(values)
        lead = member == 0
        return jnp.concatenate(
            [jnp.where(lead, values, other), jnp.where(lead, other, values)], 0
        )

    def scatter_rows(values):
        if groups != 2:
            return lax.psum_scatter(
                values, "tensor", scatter_dimension=0, tiled=True
            ).astype(jnp.float32)
        top = values[:half]
        bottom = values[half:]
        lead = member == 0
        keep = jnp.where(lead, top, bottom)
        send = jnp.where(lead, bottom, top)
        return keep.astype(jnp.float32) + swap(send).astype(jnp.float32)

    def sum_pair(values):
        if groups != 2:
            return lax.psum(values, "tensor").astype(jnp.float32)
        return values.astype(jnp.float32) + swap(values).astype(jnp.float32)

    queries = ((project(tokens, self_query) + self_query_bias.astype(jnp.float32)) * scale).astype(
        jnp.bfloat16
    )
    keys = project(tokens, self_key).astype(jnp.bfloat16)
    values = (project(tokens, self_value) + self_value_bias.astype(jnp.float32)).astype(
        jnp.bfloat16
    )
    self_queries = heads_of(queries)
    self_keys = heads_of(keys)
    self_values = heads_of(values)
    self_context, self_totals = attend_forward(self_queries, self_keys, self_values, segment, True)
    self_context = self_context.reshape(length, -1).astype(jnp.bfloat16)
    attended = scatter_rows(project(self_context, self_output)) + self_output_bias.astype(
        jnp.float32
    )
    first, first_back = jax.vjp(
        normalize,
        rows_of(tokens).astype(jnp.float32) + attended,
        first_gain.astype(jnp.float32),
        first_shift.astype(jnp.float32),
    )
    first_low = gather_rows(first.astype(jnp.bfloat16))
    queries = (
        (project(first_low, cross_query) + cross_query_bias.astype(jnp.float32)) * scale
    ).astype(jnp.bfloat16)
    keys = project(memory, cross_key).astype(jnp.bfloat16)
    values = (project(memory, cross_value) + cross_value_bias.astype(jnp.float32)).astype(
        jnp.bfloat16
    )
    cross_queries = heads_of(queries)
    cross_keys = heads_of(keys)
    cross_values = heads_of(values)
    cross_context, cross_totals = attend_forward(
        cross_queries, cross_keys, cross_values, segment, False
    )
    cross_context = cross_context.reshape(length, -1).astype(jnp.bfloat16)
    crossed = scatter_rows(
        project(cross_context, cross_output).astype(jnp.bfloat16)
    ) + cross_output_bias.astype(jnp.float32)
    second_part, second_back = jax.vjp(
        normalize,
        first + crossed,
        second_gain.astype(jnp.float32),
        second_shift.astype(jnp.float32),
    )
    second = gather_rows(second_part.astype(jnp.bfloat16)).astype(second_part.dtype)
    second_low = second.astype(jnp.bfloat16)
    inner = project(second_low, inner_weight) + inner_bias.astype(jnp.float32)
    hidden = jax.nn.gelu(inner, approximate=False).astype(jnp.bfloat16)
    outer = sum_pair(project(hidden, outer_weight).astype(jnp.bfloat16)) + outer_bias.astype(
        jnp.float32
    )
    result, third_back = jax.vjp(
        normalize, second + outer, third_gain.astype(jnp.float32), third_shift.astype(jnp.float32)
    )
    output = result.astype(jnp.bfloat16)
    grad_third, grad_third_gain, grad_third_shift = third_back(cotangent.astype(jnp.float32))
    grad_outer = grad_third.astype(jnp.bfloat16)
    grad_outer_bias = column_sums(grad_outer)
    gelu_back = jax.vjp(partial(jax.nn.gelu, approximate=False), inner)[1]
    grad_inner = gelu_back(project(grad_outer, outer_weight.T))[0].astype(jnp.bfloat16)
    grad_inner_weight = project(second_low.T, grad_inner)
    grad_inner_bias = column_sums(grad_inner)
    grad_second = rows_of(grad_third) + scatter_rows(
        project(grad_inner, inner_weight.T).astype(jnp.bfloat16)
    )
    grad_second_in, grad_second_gain, grad_second_shift = second_back(grad_second)
    grad_cross_rows = grad_second_in.astype(jnp.bfloat16)
    grad_cross = gather_rows(grad_cross_rows)
    grad_cross_output_bias = column_sums(grad_cross)
    grad_cross_context = heads_of(project(grad_cross, cross_output.T).astype(jnp.bfloat16))
    cross_grad_q, cross_grad_k, cross_grad_v = attend_backward(
        cross_queries, cross_keys, cross_values, grad_cross_context, cross_totals, segment, False
    )
    cross_grad_q = (cross_grad_q.astype(jnp.bfloat16) * scale).reshape(length, -1)
    cross_grad_k = cross_grad_k.astype(jnp.bfloat16).reshape(length, -1)
    cross_grad_v = cross_grad_v.astype(jnp.bfloat16).reshape(length, -1)
    grad_cross_query = project(first_low.T, cross_grad_q)
    grad_cross_query_bias = column_sums(cross_grad_q)
    grad_cross_key = project(memory.T, cross_grad_k)
    grad_cross_value = project(memory.T, cross_grad_v)
    grad_cross_value_bias = column_sums(cross_grad_v)
    memory_term = project(cross_grad_k, cross_key.T) + project(cross_grad_v, cross_value.T)
    grad_first = grad_second_in + scatter_rows(
        project(cross_grad_q, cross_query.T).astype(jnp.bfloat16)
    )
    grad_first_in, grad_first_gain, grad_first_shift = first_back(grad_first)
    grad_self_rows = grad_first_in.astype(jnp.bfloat16)
    grad_self = gather_rows(grad_self_rows)
    grad_self_output_bias = column_sums(grad_self)
    grad_self_context = heads_of(project(grad_self, self_output.T).astype(jnp.bfloat16))
    self_grad_q, self_grad_k, self_grad_v = attend_backward(
        self_queries, self_keys, self_values, grad_self_context, self_totals, segment, True
    )
    self_grad_q = (self_grad_q.astype(jnp.bfloat16) * scale).reshape(length, -1)
    self_grad_k = self_grad_k.astype(jnp.bfloat16).reshape(length, -1)
    self_grad_v = self_grad_v.astype(jnp.bfloat16).reshape(length, -1)
    grad_self_query = project(tokens.T, self_grad_q)
    grad_self_query_bias = column_sums(self_grad_q)
    grad_self_key = project(tokens.T, self_grad_k)
    grad_self_value = project(tokens.T, self_grad_v)
    grad_self_value_bias = column_sums(self_grad_v)
    tokens_term = (
        project(self_grad_q, self_query.T)
        + project(self_grad_k, self_key.T)
        + project(self_grad_v, self_value.T)
    )
    tokens_part = scatter_rows(tokens_term.astype(jnp.bfloat16))
    memory_part = scatter_rows(memory_term.astype(jnp.bfloat16))
    grad_tokens = tokens_part + grad_first_in
    grad_self_output_t = project(grad_self.T, self_context)
    grad_cross_output_t = project(grad_cross.T, cross_context)
    grad_outer_weight_t = project(grad_outer.T, hidden)
    dp_size = lax.axis_size("dp")
    early = [
        grad_cross_query,
        grad_cross_key,
        grad_cross_value,
        grad_cross_output_t,
        grad_inner_weight,
        grad_outer_weight_t,
    ]
    early_widths = [piece.shape[1] for piece in early]
    early_sum = lax.psum_scatter(
        jnp.concatenate(early, 1).astype(jnp.bfloat16), "dp", scatter_dimension=0, tiled=True
    ).astype(jnp.float32)
    early_parts = []
    offset = 0
    for position, width in enumerate(early_widths):
        piece = early_sum[:, offset : offset + width]
        offset += width
        if position in (3, 5):
            piece = piece.T
        early_parts.append(piece)
    cross_sums = early_parts[0:4]
    ffn_sums = early_parts[4:6]
    late = jnp.concatenate(
        [grad_self_query, grad_self_key, grad_self_value, grad_self_output_t], 1
    )
    late_rows = late.shape[0] // dp_size
    late_width = late_rows * late.shape[1]
    norm_pairs = sum_pair(
        jnp.concatenate([grad_first_gain, grad_first_shift, grad_second_gain, grad_second_shift])
    )
    vector = jnp.concatenate(
        [
            grad_self_query_bias,
            grad_self_value_bias,
            grad_self_output_bias,
            grad_cross_query_bias,
            grad_cross_value_bias,
            grad_cross_output_bias,
            norm_pairs,
            grad_third_gain,
            grad_third_shift,
            grad_inner_bias,
            grad_outer_bias,
        ]
    )
    packed = jnp.concatenate(
        [
            late.reshape(dp_size, late_width),
            jnp.broadcast_to(vector[None], (dp_size, vector.shape[0])),
        ],
        1,
    )
    received = lax.all_to_all(packed, "dp", 0, 0, tiled=True)
    total = jnp.sum(received, 0)
    late_sum = total[:late_width].reshape(late_rows, late.shape[1])
    self_sums = []
    offset = 0
    for position in range(4):
        width = (grad_self_query, grad_self_key, grad_self_value, grad_self_output_t)[
            position
        ].shape[1]
        piece = late_sum[:, offset : offset + width]
        offset += width
        if position == 3:
            piece = piece.T
        self_sums.append(piece)
    smalls = []
    offset = late_width
    for piece in (
        grad_self_query_bias,
        grad_self_value_bias,
        grad_self_output_bias,
        grad_cross_query_bias,
        grad_cross_value_bias,
        grad_cross_output_bias,
        grad_first_gain,
        grad_first_shift,
        grad_second_gain,
        grad_second_shift,
        grad_third_gain,
        grad_third_shift,
        grad_inner_bias,
        grad_outer_bias,
    ):
        smalls.append(total[offset : offset + piece.shape[0]])
        offset += piece.shape[0]
    return (
        output,
        grad_tokens,
        memory_part,
        self_sums[0],
        smalls[0],
        self_sums[1],
        self_sums[2],
        smalls[1],
        self_sums[3],
        smalls[2],
        cross_sums[0],
        smalls[3],
        cross_sums[1],
        cross_sums[2],
        smalls[4],
        cross_sums[3],
        smalls[5],
        smalls[6],
        smalls[7],
        smalls[8],
        smalls[9],
        smalls[10],
        smalls[11],
        ffn_sums[0],
        smalls[12],
        ffn_sums[1],
        smalls[13],
    )


def solution(mesh):
    return jax.shard_map(
        on_device,
        mesh=mesh,
        in_specs=(
            P("dp", None),
            P("dp", None),
            P("dp"),
            P("dp", None),
            P(None, "tensor"),
            P("tensor"),
            P(None, "tensor"),
            P(None, "tensor"),
            P("tensor"),
            P("tensor", None),
            P(),
            P(None, "tensor"),
            P("tensor"),
            P(None, "tensor"),
            P(None, "tensor"),
            P("tensor"),
            P("tensor", None),
            P(),
            P(),
            P(),
            P(),
            P(),
            P(),
            P(),
            P(None, "tensor"),
            P("tensor"),
            P("tensor", None),
            P(),
        ),
        out_specs=(
            P("dp", None),
            P(("dp", "tensor"), None),
            P(("dp", "tensor"), None),
            P("dp", "tensor"),
            P("tensor"),
            P("dp", "tensor"),
            P("dp", "tensor"),
            P("tensor"),
            P("tensor", "dp"),
            P(),
            P("dp", "tensor"),
            P("tensor"),
            P("dp", "tensor"),
            P("dp", "tensor"),
            P("tensor"),
            P("tensor", "dp"),
            P(),
            P(),
            P(),
            P(),
            P(),
            P(),
            P(),
            P("dp", "tensor"),
            P("tensor"),
            P("tensor", "dp"),
            P(),
        ),
        check_vma=False,
    )
```

```python
from functools import partial

import jax
import jax.numpy as jnp
from jax import lax
from jax.sharding import PartitionSpec as P

HD = 64


EPSILON = 1e-05
NEGATIVE = -1e30


def normalize(hidden, gain, shift):
    center = hidden - jnp.mean(hidden, -1, keepdims=True)
    spread = jnp.mean(center * center, -1, keepdims=True)
    return center * lax.rsqrt(spread + EPSILON) * gain + shift


def project(data, weight):
    return jnp.dot(data, weight, preferred_element_type=jnp.float32)


def column_sums(values):
    return jnp.sum(values.astype(jnp.float32), 0)


def heads_of(matrix):
    return matrix.reshape(matrix.shape[0], -1, HD)


def allowed_pairs(query_segment, key_segment, start, causal):
    same = query_segment[:, None] == key_segment[None, :]
    if causal:
        query_place = start + jnp.arange(query_segment.shape[0], dtype=jnp.int32)
        key_place = jnp.arange(key_segment.shape[0], dtype=jnp.int32)
        same = same & (key_place[None, :] <= query_place[:, None])
    return same[None]


def attend_forward(queries, keys, values, segment, causal):
    length = queries.shape[0]
    block_rows = min(512, length)
    contexts = []
    totals = []
    for index in range(length // block_rows):
        start = index * block_rows
        piece = queries[start : start + block_rows]
        scores = jnp.einsum("qhe,khe->hqk", piece, keys, preferred_element_type=jnp.float32)
        scores = jnp.where(
            allowed_pairs(segment[start : start + block_rows], segment, start, causal),
            scores,
            NEGATIVE,
        )
        highest = jnp.max(scores, -1, keepdims=True)
        powers = jnp.exp(scores - highest)
        summed = jnp.sum(powers, -1, keepdims=True)
        weights = (powers / summed).astype(jnp.bfloat16)
        contexts.append(
            jnp.einsum("hqk,khe->qhe", weights, values, preferred_element_type=jnp.float32)
        )
        totals.append(highest + jnp.log(summed))
    return (jnp.concatenate(contexts, 0), jnp.concatenate(totals, 1))


def attend_backward(queries, keys, values, grad_context, totals, segment, causal):
    length = queries.shape[0]
    block_rows = min(512, length)
    grad_queries = []
    grad_keys = jnp.zeros(keys.shape, jnp.float32)
    grad_values = jnp.zeros(values.shape, jnp.float32)
    for index in range(length // block_rows):
        start = index * block_rows
        piece = queries[start : start + block_rows]
        grad_piece = grad_context[start : start + block_rows]
        scores = jnp.einsum("qhe,khe->hqk", piece, keys, preferred_element_type=jnp.float32)
        scores = jnp.where(
            allowed_pairs(segment[start : start + block_rows], segment, start, causal),
            scores,
            NEGATIVE,
        )
        probs = jnp.exp(scores - totals[:, start : start + block_rows])
        grad_probs = jnp.einsum(
            "qhe,khe->hqk", grad_piece, values, preferred_element_type=jnp.float32
        )
        row_inner = jnp.sum(grad_probs * probs, -1, keepdims=True)
        grad_scores = (probs * (grad_probs - row_inner)).astype(jnp.bfloat16)
        grad_queries.append(
            jnp.einsum("hqk,khe->qhe", grad_scores, keys, preferred_element_type=jnp.float32)
        )
        grad_keys = grad_keys + jnp.einsum(
            "hqk,qhe->khe", grad_scores, piece, preferred_element_type=jnp.float32
        )
        grad_values = grad_values + jnp.einsum(
            "hqk,qhe->khe",
            probs.astype(jnp.bfloat16),
            grad_piece,
            preferred_element_type=jnp.float32,
        )
    return (jnp.concatenate(grad_queries, 0), grad_keys, grad_values)


def on_device(
    tokens,
    memory,
    segment,
    cotangent,
    self_query,
    self_query_bias,
    self_key,
    self_value,
    self_value_bias,
    self_output,
    self_output_bias,
    cross_query,
    cross_query_bias,
    cross_key,
    cross_value,
    cross_value_bias,
    cross_output,
    cross_output_bias,
    first_gain,
    first_shift,
    second_gain,
    second_shift,
    third_gain,
    third_shift,
    inner_weight,
    inner_bias,
    outer_weight,
    outer_bias,
):
    scale = HD ** (-0.5)
    length = tokens.shape[0]
    groups = lax.axis_size("tensor")
    member = lax.axis_index("tensor")
    half = length // groups

    def rows_of(values):
        return lax.dynamic_slice_in_dim(values, member * half, half, 0)

    def spread_out(values):
        whole = jnp.zeros((values.shape[0] * groups,), jnp.float32)
        return lax.dynamic_update_slice_in_dim(whole, values, member * values.shape[0], 0)

    def own_share(values, count):
        return lax.dynamic_slice_in_dim(values, member * count, count, 0)

    def swap(values):
        return lax.ppermute(values, "tensor", [(0, 1), (1, 0)])

    def gather_rows(values):
        if groups != 2:
            return lax.all_gather(values, "tensor", axis=0, tiled=True)
        other = swap(values)
        lead = member == 0
        return jnp.concatenate(
            [jnp.where(lead, values, other), jnp.where(lead, other, values)], 0
        )

    def scatter_rows(values):
        if groups != 2:
            return lax.psum_scatter(
                values, "tensor", scatter_dimension=0, tiled=True
            ).astype(jnp.float32)
        top = values[:half]
        bottom = values[half:]
        lead = member == 0
        keep = jnp.where(lead, top, bottom)
        send = jnp.where(lead, bottom, top)
        return keep.astype(jnp.float32) + swap(send).astype(jnp.float32)

    def sum_pair(values):
        if groups != 2:
            return lax.psum(values, "tensor").astype(jnp.float32)
        return values.astype(jnp.float32) + swap(values).astype(jnp.float32)

    queries = ((project(tokens, self_query) + self_query_bias.astype(jnp.float32)) * scale).astype(
        jnp.bfloat16
    )
    keys = project(tokens, self_key).astype(jnp.bfloat16)
    values = (project(tokens, self_value) + self_value_bias.astype(jnp.float32)).astype(
        jnp.bfloat16
    )
    self_queries = heads_of(queries)
    self_keys = heads_of(keys)
    self_values = heads_of(values)
    self_context, self_totals = attend_forward(self_queries, self_keys, self_values, segment, True)
    self_context = self_context.reshape(length, -1).astype(jnp.bfloat16)
    attended = scatter_rows(project(self_context, self_output)) + self_output_bias.astype(
        jnp.float32
    )
    first, first_back = jax.vjp(
        normalize,
        rows_of(tokens).astype(jnp.float32) + attended,
        first_gain.astype(jnp.float32),
        first_shift.astype(jnp.float32),
    )
    first_low = gather_rows(first.astype(jnp.bfloat16))
    queries = (
        (project(first_low, cross_query) + cross_query_bias.astype(jnp.float32)) * scale
    ).astype(jnp.bfloat16)
    keys = project(memory, cross_key).astype(jnp.bfloat16)
    values = (project(memory, cross_value) + cross_value_bias.astype(jnp.float32)).astype(
        jnp.bfloat16
    )
    cross_queries = heads_of(queries)
    cross_keys = heads_of(keys)
    cross_values = heads_of(values)
    cross_context, cross_totals = attend_forward(
        cross_queries, cross_keys, cross_values, segment, False
    )
    cross_context = cross_context.reshape(length, -1).astype(jnp.bfloat16)
    crossed = scatter_rows(
        project(cross_context, cross_output).astype(jnp.bfloat16)
    ) + cross_output_bias.astype(jnp.float32)
    second_part, second_back = jax.vjp(
        normalize,
        first + crossed,
        second_gain.astype(jnp.float32),
        second_shift.astype(jnp.float32),
    )
    second = gather_rows(second_part.astype(jnp.bfloat16)).astype(second_part.dtype)
    second_low = second.astype(jnp.bfloat16)
    inner = project(second_low, inner_weight) + inner_bias.astype(jnp.float32)
    hidden = jax.nn.gelu(inner, approximate=False).astype(jnp.bfloat16)
    outer = sum_pair(project(hidden, outer_weight).astype(jnp.bfloat16)) + outer_bias.astype(
        jnp.float32
    )
    result, third_back = jax.vjp(
        normalize, second + outer, third_gain.astype(jnp.float32), third_shift.astype(jnp.float32)
    )
    output = result.astype(jnp.bfloat16)
    grad_third, grad_third_gain, grad_third_shift = third_back(cotangent.astype(jnp.float32))
    grad_outer = grad_third.astype(jnp.bfloat16)
    grad_outer_bias = column_sums(grad_outer)
    gelu_back = jax.vjp(partial(jax.nn.gelu, approximate=False), inner)[1]
    grad_inner = gelu_back(project(grad_outer, outer_weight.T))[0].astype(jnp.bfloat16)
    grad_inner_weight = project(second_low.T, grad_inner)
    grad_inner_bias = column_sums(grad_inner)
    grad_second = rows_of(grad_third) + scatter_rows(
        project(grad_inner, inner_weight.T).astype(jnp.bfloat16)
    )
    grad_second_in, grad_second_gain, grad_second_shift = second_back(grad_second)
    grad_cross_rows = grad_second_in.astype(jnp.bfloat16)
    grad_cross = gather_rows(grad_cross_rows)
    grad_cross_output_bias = column_sums(grad_cross)
    grad_cross_context = heads_of(project(grad_cross, cross_output.T).astype(jnp.bfloat16))
    cross_grad_q, cross_grad_k, cross_grad_v = attend_backward(
        cross_queries, cross_keys, cross_values, grad_cross_context, cross_totals, segment, False
    )
    cross_grad_q = (cross_grad_q.astype(jnp.bfloat16) * scale).reshape(length, -1)
    cross_grad_k = cross_grad_k.astype(jnp.bfloat16).reshape(length, -1)
    cross_grad_v = cross_grad_v.astype(jnp.bfloat16).reshape(length, -1)
    grad_cross_query = project(first_low.T, cross_grad_q)
    grad_cross_query_bias = column_sums(cross_grad_q)
    grad_cross_key = project(memory.T, cross_grad_k)
    grad_cross_value = project(memory.T, cross_grad_v)
    grad_cross_value_bias = column_sums(cross_grad_v)
    memory_term = project(cross_grad_k, cross_key.T) + project(cross_grad_v, cross_value.T)
    grad_first = grad_second_in + scatter_rows(
        project(cross_grad_q, cross_query.T).astype(jnp.bfloat16)
    )
    grad_first_in, grad_first_gain, grad_first_shift = first_back(grad_first)
    grad_self_rows = grad_first_in.astype(jnp.bfloat16)
    grad_self = gather_rows(grad_self_rows)
    grad_self_output_bias = column_sums(grad_self)
    grad_self_context = heads_of(project(grad_self, self_output.T).astype(jnp.bfloat16))
    dp_size = lax.axis_size("dp")
    grad_cross_output_t = project(grad_cross.T, cross_context)
    cross = [grad_cross_query, grad_cross_key, grad_cross_value, grad_cross_output_t]
    cross_joined = jnp.concatenate(cross, 1).astype(jnp.bfloat16)
    cross_joined, grad_self_context = lax.optimization_barrier((cross_joined, grad_self_context))
    self_grad_q, self_grad_k, self_grad_v = attend_backward(
        self_queries, self_keys, self_values, grad_self_context, self_totals, segment, True
    )
    self_grad_q = (self_grad_q.astype(jnp.bfloat16) * scale).reshape(length, -1)
    self_grad_k = self_grad_k.astype(jnp.bfloat16).reshape(length, -1)
    self_grad_v = self_grad_v.astype(jnp.bfloat16).reshape(length, -1)
    grad_self_query = project(tokens.T, self_grad_q)
    grad_self_query_bias = column_sums(self_grad_q)
    grad_self_key = project(tokens.T, self_grad_k)
    grad_self_value = project(tokens.T, self_grad_v)
    grad_self_value_bias = column_sums(self_grad_v)
    tokens_term = (
        project(self_grad_q, self_query.T)
        + project(self_grad_k, self_key.T)
        + project(self_grad_v, self_value.T)
    )
    tokens_part = scatter_rows(tokens_term.astype(jnp.bfloat16))
    memory_part = scatter_rows(memory_term.astype(jnp.bfloat16))
    grad_tokens = tokens_part + grad_first_in
    grad_self_output_t = project(grad_self.T, self_context)
    grad_outer_weight_t = project(grad_outer.T, hidden)

    def split_columns(summed, pieces, flipped):
        parts = []
        offset = 0
        for position, piece in enumerate(pieces):
            width = piece.shape[1]
            part = summed[:, offset : offset + width]
            offset += width
            if position in flipped:
                part = part.T
            parts.append(part)
        return parts

    def exchange_sum(joined, extra=None):
        rows = joined.shape[0] // dp_size
        blocks = joined.reshape(dp_size, rows, joined.shape[1])
        if extra is not None:
            blocks = jnp.concatenate(
                [blocks, jnp.broadcast_to(extra[None], (dp_size,) + extra.shape)], 1
            )
        received = lax.all_to_all(blocks, "dp", 0, 0, tiled=True)
        return jnp.sum(received.astype(jnp.float32), 0)

    ffn = [grad_inner_weight, grad_outer_weight_t]
    ffn_sum = lax.psum_scatter(
        jnp.concatenate(ffn, 1).astype(jnp.bfloat16), "dp", scatter_dimension=0, tiled=True
    ).astype(jnp.float32)
    ffn_sums = split_columns(ffn_sum, ffn, (1,))
    cross_sums = split_columns(exchange_sum(cross_joined), cross, (3,))
    late = [grad_self_query, grad_self_key, grad_self_value, grad_self_output_t]
    late_joined = jnp.concatenate(late, 1).astype(jnp.bfloat16)
    norm_pairs = sum_pair(
        jnp.concatenate([grad_first_gain, grad_first_shift, grad_second_gain, grad_second_shift])
    )
    vector = jnp.concatenate(
        [
            grad_self_query_bias,
            grad_self_value_bias,
            grad_self_output_bias,
            grad_cross_query_bias,
            grad_cross_value_bias,
            grad_cross_output_bias,
            norm_pairs,
            grad_third_gain,
            grad_third_shift,
            grad_inner_bias,
            grad_outer_bias,
        ]
    )
    width = late_joined.shape[1]
    lines = -(-vector.shape[0] // width)
    padded = jnp.pad(vector, (0, lines * width - vector.shape[0])).reshape(lines, width)
    high = padded.astype(jnp.bfloat16)
    low = (padded - high.astype(jnp.float32)).astype(jnp.bfloat16)
    late_rows = late_joined.shape[0] // dp_size
    late_total = exchange_sum(late_joined, jnp.concatenate([high, low], 0))
    self_sums = split_columns(late_total[:late_rows], late, (3,))
    total = (
        late_total[late_rows : late_rows + lines] + late_total[late_rows + lines :]
    ).reshape(-1)
    smalls = []
    offset = 0
    for piece in (
        grad_self_query_bias,
        grad_self_value_bias,
        grad_self_output_bias,
        grad_cross_query_bias,
        grad_cross_value_bias,
        grad_cross_output_bias,
        grad_first_gain,
        grad_first_shift,
        grad_second_gain,
        grad_second_shift,
        grad_third_gain,
        grad_third_shift,
        grad_inner_bias,
        grad_outer_bias,
    ):
        smalls.append(total[offset : offset + piece.shape[0]])
        offset += piece.shape[0]
    return (
        output,
        grad_tokens,
        memory_part,
        self_sums[0],
        smalls[0],
        self_sums[1],
        self_sums[2],
        smalls[1],
        self_sums[3],
        smalls[2],
        cross_sums[0],
        smalls[3],
        cross_sums[1],
        cross_sums[2],
        smalls[4],
        cross_sums[3],
        smalls[5],
        smalls[6],
        smalls[7],
        smalls[8],
        smalls[9],
        smalls[10],
        smalls[11],
        ffn_sums[0],
        smalls[12],
        ffn_sums[1],
        smalls[13],
    )


def solution(mesh):
    return jax.shard_map(
        on_device,
        mesh=mesh,
        in_specs=(
            P("dp", None),
            P("dp", None),
            P("dp"),
            P("dp", None),
            P(None, "tensor"),
            P("tensor"),
            P(None, "tensor"),
            P(None, "tensor"),
            P("tensor"),
            P("tensor", None),
            P(),
            P(None, "tensor"),
            P("tensor"),
            P(None, "tensor"),
            P(None, "tensor"),
            P("tensor"),
            P("tensor", None),
            P(),
            P(),
            P(),
            P(),
            P(),
            P(),
            P(),
            P(None, "tensor"),
            P("tensor"),
            P("tensor", None),
            P(),
        ),
        out_specs=(
            P("dp", None),
            P(("dp", "tensor"), None),
            P(("dp", "tensor"), None),
            P("dp", "tensor"),
            P("tensor"),
            P("dp", "tensor"),
            P("dp", "tensor"),
            P("tensor"),
            P("tensor", "dp"),
            P(),
            P("dp", "tensor"),
            P("tensor"),
            P("dp", "tensor"),
            P("dp", "tensor"),
            P("tensor"),
            P("tensor", "dp"),
            P(),
            P(),
            P(),
            P(),
            P(),
            P(),
            P(),
            P("dp", "tensor"),
            P("tensor"),
            P("tensor", "dp"),
            P(),
        ),
        check_vma=False,
    )
```

```python
from functools import partial

import jax
import jax.numpy as jnp
from jax import lax
from jax.sharding import PartitionSpec as P

HD = 64


EPSILON = 1e-05
NEGATIVE = -1e30


def normalize(hidden, gain, shift):
    center = hidden - jnp.mean(hidden, -1, keepdims=True)
    spread = jnp.mean(center * center, -1, keepdims=True)
    return center * lax.rsqrt(spread + EPSILON) * gain + shift


def project(data, weight):
    return jnp.dot(data, weight, preferred_element_type=jnp.float32)


def column_sums(values):
    return jnp.sum(values.astype(jnp.float32), 0)


def heads_of(matrix):
    return matrix.reshape(matrix.shape[0], -1, HD)


def allowed_pairs(query_segment, key_segment, start, causal):
    same = query_segment[:, None] == key_segment[None, :]
    if causal:
        query_place = start + jnp.arange(query_segment.shape[0], dtype=jnp.int32)
        key_place = jnp.arange(key_segment.shape[0], dtype=jnp.int32)
        same = same & (key_place[None, :] <= query_place[:, None])
    return same[None]


def attend_forward(queries, keys, values, segment, causal):
    length = queries.shape[0]
    block_rows = min(256 if causal else 512, length)
    contexts = []
    totals = []
    for index in range(length // block_rows):
        start = index * block_rows
        end = start + block_rows if causal else length
        piece = queries[start : start + block_rows]
        scores = jnp.einsum(
            "qhe,khe->hqk", piece, keys[:end], preferred_element_type=jnp.float32
        )
        scores = jnp.where(
            allowed_pairs(segment[start : start + block_rows], segment[:end], start, causal),
            scores,
            NEGATIVE,
        )
        highest = jnp.max(scores, -1, keepdims=True)
        powers = jnp.exp(scores - highest)
        summed = jnp.sum(powers, -1, keepdims=True)
        weights = (powers / summed).astype(jnp.bfloat16)
        contexts.append(
            jnp.einsum("hqk,khe->qhe", weights, values[:end], preferred_element_type=jnp.float32)
        )
        totals.append(highest + jnp.log(summed))
    return (jnp.concatenate(contexts, 0), jnp.concatenate(totals, 1))


def attend_backward(queries, keys, values, grad_context, totals, segment, causal):
    length = queries.shape[0]
    block_rows = min(256 if causal else 512, length)
    grad_queries = []
    grad_keys = jnp.zeros(keys.shape, jnp.float32)
    grad_values = jnp.zeros(values.shape, jnp.float32)
    for index in range(length // block_rows):
        start = index * block_rows
        end = start + block_rows if causal else length
        piece = queries[start : start + block_rows]
        grad_piece = grad_context[start : start + block_rows]
        near_keys = keys[:end]
        scores = jnp.einsum("qhe,khe->hqk", piece, near_keys, preferred_element_type=jnp.float32)
        scores = jnp.where(
            allowed_pairs(segment[start : start + block_rows], segment[:end], start, causal),
            scores,
            NEGATIVE,
        )
        probs = jnp.exp(scores - totals[:, start : start + block_rows])
        grad_probs = jnp.einsum(
            "qhe,khe->hqk", grad_piece, values[:end], preferred_element_type=jnp.float32
        )
        row_inner = jnp.sum(grad_probs * probs, -1, keepdims=True)
        grad_scores = (probs * (grad_probs - row_inner)).astype(jnp.bfloat16)
        grad_queries.append(
            jnp.einsum("hqk,khe->qhe", grad_scores, near_keys, preferred_element_type=jnp.float32)
        )
        grad_keys = grad_keys.at[:end].add(
            jnp.einsum("hqk,qhe->khe", grad_scores, piece, preferred_element_type=jnp.float32)
        )
        grad_values = grad_values.at[:end].add(
            jnp.einsum(
                "hqk,qhe->khe",
                probs.astype(jnp.bfloat16),
                grad_piece,
                preferred_element_type=jnp.float32,
            )
        )
    return (jnp.concatenate(grad_queries, 0), grad_keys, grad_values)


def on_device(
    tokens,
    memory,
    segment,
    cotangent,
    self_query,
    self_query_bias,
    self_key,
    self_value,
    self_value_bias,
    self_output,
    self_output_bias,
    cross_query,
    cross_query_bias,
    cross_key,
    cross_value,
    cross_value_bias,
    cross_output,
    cross_output_bias,
    first_gain,
    first_shift,
    second_gain,
    second_shift,
    third_gain,
    third_shift,
    inner_weight,
    inner_bias,
    outer_weight,
    outer_bias,
):
    scale = HD ** (-0.5)
    length = tokens.shape[0]
    groups = lax.axis_size("tensor")
    member = lax.axis_index("tensor")
    half = length // groups

    def rows_of(values):
        return lax.dynamic_slice_in_dim(values, member * half, half, 0)

    def spread_out(values):
        whole = jnp.zeros((values.shape[0] * groups,), jnp.float32)
        return lax.dynamic_update_slice_in_dim(whole, values, member * values.shape[0], 0)

    def own_share(values, count):
        return lax.dynamic_slice_in_dim(values, member * count, count, 0)

    def swap(values):
        return lax.ppermute(values, "tensor", [(0, 1), (1, 0)])

    def gather_rows(values):
        if groups != 2:
            return lax.all_gather(values, "tensor", axis=0, tiled=True)
        other = swap(values)
        lead = member == 0
        return jnp.concatenate(
            [jnp.where(lead, values, other), jnp.where(lead, other, values)], 0
        )

    def scatter_rows(values):
        if groups != 2:
            return lax.psum_scatter(
                values, "tensor", scatter_dimension=0, tiled=True
            ).astype(jnp.float32)
        top = values[:half]
        bottom = values[half:]
        lead = member == 0
        keep = jnp.where(lead, top, bottom)
        send = jnp.where(lead, bottom, top)
        return keep.astype(jnp.float32) + swap(send).astype(jnp.float32)

    def sum_pair(values):
        if groups != 2:
            return lax.psum(values, "tensor").astype(jnp.float32)
        return values.astype(jnp.float32) + swap(values).astype(jnp.float32)

    queries = ((project(tokens, self_query) + self_query_bias.astype(jnp.float32)) * scale).astype(
        jnp.bfloat16
    )
    keys = project(tokens, self_key).astype(jnp.bfloat16)
    values = (project(tokens, self_value) + self_value_bias.astype(jnp.float32)).astype(
        jnp.bfloat16
    )
    self_queries = heads_of(queries)
    self_keys = heads_of(keys)
    self_values = heads_of(values)
    self_context, self_totals = attend_forward(self_queries, self_keys, self_values, segment, True)
    self_context = self_context.reshape(length, -1).astype(jnp.bfloat16)
    attended = scatter_rows(project(self_context, self_output)) + self_output_bias.astype(
        jnp.float32
    )
    first, first_back = jax.vjp(
        normalize,
        rows_of(tokens).astype(jnp.float32) + attended,
        first_gain.astype(jnp.float32),
        first_shift.astype(jnp.float32),
    )
    first_low = gather_rows(first.astype(jnp.bfloat16))
    queries = (
        (project(first_low, cross_query) + cross_query_bias.astype(jnp.float32)) * scale
    ).astype(jnp.bfloat16)
    keys = project(memory, cross_key).astype(jnp.bfloat16)
    values = (project(memory, cross_value) + cross_value_bias.astype(jnp.float32)).astype(
        jnp.bfloat16
    )
    cross_queries = heads_of(queries)
    cross_keys = heads_of(keys)
    cross_values = heads_of(values)
    cross_context, cross_totals = attend_forward(
        cross_queries, cross_keys, cross_values, segment, False
    )
    cross_context = cross_context.reshape(length, -1).astype(jnp.bfloat16)
    crossed = scatter_rows(
        project(cross_context, cross_output).astype(jnp.bfloat16)
    ) + cross_output_bias.astype(jnp.float32)
    second_part, second_back = jax.vjp(
        normalize,
        first + crossed,
        second_gain.astype(jnp.float32),
        second_shift.astype(jnp.float32),
    )
    second = gather_rows(second_part.astype(jnp.bfloat16)).astype(second_part.dtype)
    second_low = second.astype(jnp.bfloat16)
    inner = project(second_low, inner_weight) + inner_bias.astype(jnp.float32)
    hidden = jax.nn.gelu(inner, approximate=False).astype(jnp.bfloat16)
    outer = sum_pair(project(hidden, outer_weight).astype(jnp.bfloat16)) + outer_bias.astype(
        jnp.float32
    )
    result, third_back = jax.vjp(
        normalize, second + outer, third_gain.astype(jnp.float32), third_shift.astype(jnp.float32)
    )
    output = result.astype(jnp.bfloat16)
    grad_third, grad_third_gain, grad_third_shift = third_back(cotangent.astype(jnp.float32))
    grad_outer = grad_third.astype(jnp.bfloat16)
    grad_outer_bias = column_sums(grad_outer)
    gelu_back = jax.vjp(partial(jax.nn.gelu, approximate=False), inner)[1]
    grad_inner = gelu_back(project(grad_outer, outer_weight.T))[0].astype(jnp.bfloat16)
    grad_inner_weight = project(second_low.T, grad_inner)
    grad_inner_bias = column_sums(grad_inner)
    grad_second = rows_of(grad_third) + scatter_rows(
        project(grad_inner, inner_weight.T).astype(jnp.bfloat16)
    )
    grad_second_in, grad_second_gain, grad_second_shift = second_back(grad_second)
    grad_cross_rows = grad_second_in.astype(jnp.bfloat16)
    grad_cross = gather_rows(grad_cross_rows)
    grad_cross_output_bias = column_sums(grad_cross)
    grad_cross_context = heads_of(project(grad_cross, cross_output.T).astype(jnp.bfloat16))
    cross_grad_q, cross_grad_k, cross_grad_v = attend_backward(
        cross_queries, cross_keys, cross_values, grad_cross_context, cross_totals, segment, False
    )
    cross_grad_q = (cross_grad_q.astype(jnp.bfloat16) * scale).reshape(length, -1)
    cross_grad_k = cross_grad_k.astype(jnp.bfloat16).reshape(length, -1)
    cross_grad_v = cross_grad_v.astype(jnp.bfloat16).reshape(length, -1)
    grad_cross_query = project(first_low.T, cross_grad_q)
    grad_cross_query_bias = column_sums(cross_grad_q)
    grad_cross_key = project(memory.T, cross_grad_k)
    grad_cross_value = project(memory.T, cross_grad_v)
    grad_cross_value_bias = column_sums(cross_grad_v)
    memory_term = project(cross_grad_k, cross_key.T) + project(cross_grad_v, cross_value.T)
    grad_first = grad_second_in + scatter_rows(
        project(cross_grad_q, cross_query.T).astype(jnp.bfloat16)
    )
    grad_first_in, grad_first_gain, grad_first_shift = first_back(grad_first)
    grad_self_rows = grad_first_in.astype(jnp.bfloat16)
    grad_self = gather_rows(grad_self_rows)
    grad_self_output_bias = column_sums(grad_self)
    grad_self_context = heads_of(project(grad_self, self_output.T).astype(jnp.bfloat16))
    dp_size = lax.axis_size("dp")
    grad_cross_output_t = project(grad_cross.T, cross_context)
    cross = [grad_cross_query, grad_cross_key, grad_cross_value, grad_cross_output_t]
    cross_joined = jnp.concatenate(cross, 1).astype(jnp.bfloat16)
    cross_joined, grad_self_context = lax.optimization_barrier((cross_joined, grad_self_context))
    self_grad_q, self_grad_k, self_grad_v = attend_backward(
        self_queries, self_keys, self_values, grad_self_context, self_totals, segment, True
    )
    self_grad_q = (self_grad_q.astype(jnp.bfloat16) * scale).reshape(length, -1)
    self_grad_k = self_grad_k.astype(jnp.bfloat16).reshape(length, -1)
    self_grad_v = self_grad_v.astype(jnp.bfloat16).reshape(length, -1)
    grad_self_query = project(tokens.T, self_grad_q)
    grad_self_query_bias = column_sums(self_grad_q)
    grad_self_key = project(tokens.T, self_grad_k)
    grad_self_value = project(tokens.T, self_grad_v)
    grad_self_value_bias = column_sums(self_grad_v)
    tokens_term = (
        project(self_grad_q, self_query.T)
        + project(self_grad_k, self_key.T)
        + project(self_grad_v, self_value.T)
    )
    tokens_part = scatter_rows(tokens_term.astype(jnp.bfloat16))
    memory_part = scatter_rows(memory_term.astype(jnp.bfloat16))
    grad_tokens = tokens_part + grad_first_in
    grad_self_output_t = project(grad_self.T, self_context)
    grad_outer_weight_t = project(grad_outer.T, hidden)

    def split_columns(summed, pieces, flipped):
        parts = []
        offset = 0
        for position, piece in enumerate(pieces):
            width = piece.shape[1]
            part = summed[:, offset : offset + width]
            offset += width
            if position in flipped:
                part = part.T
            parts.append(part)
        return parts

    def exchange_sum(joined, extra=None):
        rows = joined.shape[0] // dp_size
        blocks = joined.reshape(dp_size, rows, joined.shape[1])
        if extra is not None:
            blocks = jnp.concatenate(
                [blocks, jnp.broadcast_to(extra[None], (dp_size,) + extra.shape)], 1
            )
        received = lax.all_to_all(blocks, "dp", 0, 0, tiled=True)
        return jnp.sum(received.astype(jnp.float32), 0)

    ffn = [grad_inner_weight, grad_outer_weight_t]
    ffn_sum = lax.psum_scatter(
        jnp.concatenate(ffn, 1).astype(jnp.bfloat16), "dp", scatter_dimension=0, tiled=True
    ).astype(jnp.float32)
    ffn_sums = split_columns(ffn_sum, ffn, (1,))
    cross_sums = split_columns(exchange_sum(cross_joined), cross, (3,))
    late = [grad_self_query, grad_self_key, grad_self_value, grad_self_output_t]
    late_joined = jnp.concatenate(late, 1).astype(jnp.bfloat16)
    norm_pairs = sum_pair(
        jnp.concatenate([grad_first_gain, grad_first_shift, grad_second_gain, grad_second_shift])
    )
    vector = jnp.concatenate(
        [
            grad_self_query_bias,
            grad_self_value_bias,
            grad_self_output_bias,
            grad_cross_query_bias,
            grad_cross_value_bias,
            grad_cross_output_bias,
            norm_pairs,
            grad_third_gain,
            grad_third_shift,
            grad_inner_bias,
            grad_outer_bias,
        ]
    )
    width = late_joined.shape[1]
    lines = -(-vector.shape[0] // width)
    padded = jnp.pad(vector, (0, lines * width - vector.shape[0])).reshape(lines, width)
    high = padded.astype(jnp.bfloat16)
    low = (padded - high.astype(jnp.float32)).astype(jnp.bfloat16)
    late_rows = late_joined.shape[0] // dp_size
    late_total = exchange_sum(late_joined, jnp.concatenate([high, low], 0))
    self_sums = split_columns(late_total[:late_rows], late, (3,))
    total = (
        late_total[late_rows : late_rows + lines] + late_total[late_rows + lines :]
    ).reshape(-1)
    smalls = []
    offset = 0
    for piece in (
        grad_self_query_bias,
        grad_self_value_bias,
        grad_self_output_bias,
        grad_cross_query_bias,
        grad_cross_value_bias,
        grad_cross_output_bias,
        grad_first_gain,
        grad_first_shift,
        grad_second_gain,
        grad_second_shift,
        grad_third_gain,
        grad_third_shift,
        grad_inner_bias,
        grad_outer_bias,
    ):
        smalls.append(total[offset : offset + piece.shape[0]])
        offset += piece.shape[0]
    return (
        output,
        grad_tokens,
        memory_part,
        self_sums[0],
        smalls[0],
        self_sums[1],
        self_sums[2],
        smalls[1],
        self_sums[3],
        smalls[2],
        cross_sums[0],
        smalls[3],
        cross_sums[1],
        cross_sums[2],
        smalls[4],
        cross_sums[3],
        smalls[5],
        smalls[6],
        smalls[7],
        smalls[8],
        smalls[9],
        smalls[10],
        smalls[11],
        ffn_sums[0],
        smalls[12],
        ffn_sums[1],
        smalls[13],
    )


def solution(mesh):
    return jax.shard_map(
        on_device,
        mesh=mesh,
        in_specs=(
            P("dp", None),
            P("dp", None),
            P("dp"),
            P("dp", None),
            P(None, "tensor"),
            P("tensor"),
            P(None, "tensor"),
            P(None, "tensor"),
            P("tensor"),
            P("tensor", None),
            P(),
            P(None, "tensor"),
            P("tensor"),
            P(None, "tensor"),
            P(None, "tensor"),
            P("tensor"),
            P("tensor", None),
            P(),
            P(),
            P(),
            P(),
            P(),
            P(),
            P(),
            P(None, "tensor"),
            P("tensor"),
            P("tensor", None),
            P(),
        ),
        out_specs=(
            P("dp", None),
            P(("dp", "tensor"), None),
            P(("dp", "tensor"), None),
            P("dp", "tensor"),
            P("tensor"),
            P("dp", "tensor"),
            P("dp", "tensor"),
            P("tensor"),
            P("tensor", "dp"),
            P(),
            P("dp", "tensor"),
            P("tensor"),
            P("dp", "tensor"),
            P("dp", "tensor"),
            P("tensor"),
            P("tensor", "dp"),
            P(),
            P(),
            P(),
            P(),
            P(),
            P(),
            P(),
            P("dp", "tensor"),
            P("tensor"),
            P("tensor", "dp"),
            P(),
        ),
        check_vma=False,
    )
```

```python
from functools import partial

import jax
import jax.numpy as jnp
from jax import lax
from jax.sharding import PartitionSpec as P

HD = 64


EPSILON = 1e-05
NEGATIVE = -1e30


def normalize(hidden, gain, shift):
    center = hidden - jnp.mean(hidden, -1, keepdims=True)
    spread = jnp.mean(center * center, -1, keepdims=True)
    return center * lax.rsqrt(spread + EPSILON) * gain + shift


def project(data, weight):
    return jnp.dot(data, weight, preferred_element_type=jnp.float32)


def column_sums(values):
    return jnp.sum(values.astype(jnp.float32), 0)


def heads_of(matrix):
    return matrix.reshape(matrix.shape[0], -1, HD)


def allowed_pairs(query_segment, key_segment, start, causal):
    same = query_segment[:, None] == key_segment[None, :]
    if causal:
        query_place = start + jnp.arange(query_segment.shape[0], dtype=jnp.int32)
        key_place = jnp.arange(key_segment.shape[0], dtype=jnp.int32)
        same = same & (key_place[None, :] <= query_place[:, None])
    return same[None]


def attend_forward(queries, keys, values, segment, causal):
    length = queries.shape[0]
    block_rows = min(256 if causal else 512, length)
    contexts = []
    totals = []
    for index in range(length // block_rows):
        start = index * block_rows
        end = start + block_rows if causal else length
        piece = queries[start : start + block_rows]
        scores = jnp.einsum(
            "qhe,khe->hqk", piece, keys[:end], preferred_element_type=jnp.float32
        )
        scores = jnp.where(
            allowed_pairs(segment[start : start + block_rows], segment[:end], start, causal),
            scores,
            NEGATIVE,
        )
        highest = jnp.max(scores, -1, keepdims=True)
        powers = jnp.exp(scores - highest)
        summed = jnp.sum(powers, -1, keepdims=True)
        weights = (powers / summed).astype(jnp.bfloat16)
        contexts.append(
            jnp.einsum("hqk,khe->qhe", weights, values[:end], preferred_element_type=jnp.float32)
        )
        totals.append(highest + jnp.log(summed))
    return (jnp.concatenate(contexts, 0), jnp.concatenate(totals, 1))


def attend_backward(queries, keys, values, grad_context, totals, segment, causal):
    length = queries.shape[0]
    block_rows = min(256 if causal else 512, length)
    grad_queries = []
    grad_keys = jnp.zeros(keys.shape, jnp.float32)
    grad_values = jnp.zeros(values.shape, jnp.float32)
    for index in range(length // block_rows):
        start = index * block_rows
        end = start + block_rows if causal else length
        piece = queries[start : start + block_rows]
        grad_piece = grad_context[start : start + block_rows]
        near_keys = keys[:end]
        scores = jnp.einsum("qhe,khe->hqk", piece, near_keys, preferred_element_type=jnp.float32)
        scores = jnp.where(
            allowed_pairs(segment[start : start + block_rows], segment[:end], start, causal),
            scores,
            NEGATIVE,
        )
        probs = jnp.exp(scores - totals[:, start : start + block_rows])
        grad_probs = jnp.einsum(
            "qhe,khe->hqk", grad_piece, values[:end], preferred_element_type=jnp.float32
        )
        row_inner = jnp.sum(grad_probs * probs, -1, keepdims=True)
        grad_scores = (probs * (grad_probs - row_inner)).astype(jnp.bfloat16)
        grad_queries.append(
            jnp.einsum("hqk,khe->qhe", grad_scores, near_keys, preferred_element_type=jnp.float32)
        )
        grad_keys = grad_keys.at[:end].add(
            jnp.einsum("hqk,qhe->khe", grad_scores, piece, preferred_element_type=jnp.float32)
        )
        grad_values = grad_values.at[:end].add(
            jnp.einsum(
                "hqk,qhe->khe",
                probs.astype(jnp.bfloat16),
                grad_piece,
                preferred_element_type=jnp.float32,
            )
        )
    return (jnp.concatenate(grad_queries, 0), grad_keys, grad_values)


def on_device(
    tokens,
    memory,
    segment,
    cotangent,
    self_query,
    self_query_bias,
    self_key,
    self_value,
    self_value_bias,
    self_output,
    self_output_bias,
    cross_query,
    cross_query_bias,
    cross_key,
    cross_value,
    cross_value_bias,
    cross_output,
    cross_output_bias,
    first_gain,
    first_shift,
    second_gain,
    second_shift,
    third_gain,
    third_shift,
    inner_weight,
    inner_bias,
    outer_weight,
    outer_bias,
):
    scale = HD ** (-0.5)
    length = tokens.shape[0]
    groups = lax.axis_size("tensor")
    member = lax.axis_index("tensor")
    half = length // groups

    def rows_of(values):
        return lax.dynamic_slice_in_dim(values, member * half, half, 0)

    def spread_out(values):
        whole = jnp.zeros((values.shape[0] * groups,), jnp.float32)
        return lax.dynamic_update_slice_in_dim(whole, values, member * values.shape[0], 0)

    def own_share(values, count):
        return lax.dynamic_slice_in_dim(values, member * count, count, 0)

    def swap(values):
        return lax.ppermute(values, "tensor", [(0, 1), (1, 0)])

    def gather_rows(values):
        if groups != 2:
            return lax.all_gather(values, "tensor", axis=0, tiled=True)
        other = swap(values)
        lead = member == 0
        return jnp.concatenate(
            [jnp.where(lead, values, other), jnp.where(lead, other, values)], 0
        )

    def scatter_rows(values):
        if groups != 2:
            return lax.psum_scatter(
                values, "tensor", scatter_dimension=0, tiled=True
            ).astype(jnp.float32)
        top = values[:half]
        bottom = values[half:]
        lead = member == 0
        keep = jnp.where(lead, top, bottom)
        send = jnp.where(lead, bottom, top)
        return keep.astype(jnp.float32) + swap(send).astype(jnp.float32)

    def sum_pair(values):
        if groups != 2:
            return lax.psum(values, "tensor").astype(jnp.float32)
        return values.astype(jnp.float32) + swap(values).astype(jnp.float32)

    queries = ((project(tokens, self_query) + self_query_bias.astype(jnp.float32)) * scale).astype(
        jnp.bfloat16
    )
    keys = project(tokens, self_key).astype(jnp.bfloat16)
    values = (project(tokens, self_value) + self_value_bias.astype(jnp.float32)).astype(
        jnp.bfloat16
    )
    self_queries = heads_of(queries)
    self_keys = heads_of(keys)
    self_values = heads_of(values)
    self_context, self_totals = attend_forward(self_queries, self_keys, self_values, segment, True)
    self_context = self_context.reshape(length, -1).astype(jnp.bfloat16)
    attended = scatter_rows(project(self_context, self_output)) + self_output_bias.astype(
        jnp.float32
    )
    first, first_back = jax.vjp(
        normalize,
        rows_of(tokens).astype(jnp.float32) + attended,
        first_gain.astype(jnp.float32),
        first_shift.astype(jnp.float32),
    )
    first_low = gather_rows(first.astype(jnp.bfloat16))
    queries = (
        (project(first_low, cross_query) + cross_query_bias.astype(jnp.float32)) * scale
    ).astype(jnp.bfloat16)
    keys = project(memory, cross_key).astype(jnp.bfloat16)
    values = (project(memory, cross_value) + cross_value_bias.astype(jnp.float32)).astype(
        jnp.bfloat16
    )
    cross_queries = heads_of(queries)
    cross_keys = heads_of(keys)
    cross_values = heads_of(values)
    cross_context, cross_totals = attend_forward(
        cross_queries, cross_keys, cross_values, segment, False
    )
    cross_context = cross_context.reshape(length, -1).astype(jnp.bfloat16)
    crossed = scatter_rows(
        project(cross_context, cross_output).astype(jnp.bfloat16)
    ) + cross_output_bias.astype(jnp.float32)
    second_part, second_back = jax.vjp(
        normalize,
        first + crossed,
        second_gain.astype(jnp.float32),
        second_shift.astype(jnp.float32),
    )
    second = gather_rows(second_part.astype(jnp.bfloat16)).astype(second_part.dtype)
    second_low = second.astype(jnp.bfloat16)
    inner = project(second_low, inner_weight) + inner_bias.astype(jnp.float32)
    hidden = jax.nn.gelu(inner, approximate=False).astype(jnp.bfloat16)
    outer = sum_pair(project(hidden, outer_weight).astype(jnp.bfloat16)) + outer_bias.astype(
        jnp.float32
    )
    result, third_back = jax.vjp(
        normalize, second + outer, third_gain.astype(jnp.float32), third_shift.astype(jnp.float32)
    )
    output = result.astype(jnp.bfloat16)
    grad_third, grad_third_gain, grad_third_shift = third_back(cotangent.astype(jnp.float32))
    grad_outer = grad_third.astype(jnp.bfloat16)
    grad_outer_bias = column_sums(grad_outer)
    gelu_back = jax.vjp(partial(jax.nn.gelu, approximate=False), inner)[1]
    grad_inner = gelu_back(project(grad_outer, outer_weight.T))[0].astype(jnp.bfloat16)
    grad_inner_weight = project(second_low.T, grad_inner)
    grad_inner_bias = column_sums(grad_inner)
    grad_second = rows_of(grad_third) + scatter_rows(
        project(grad_inner, inner_weight.T).astype(jnp.bfloat16)
    )
    grad_second_in, grad_second_gain, grad_second_shift = second_back(grad_second)
    grad_cross_rows = grad_second_in.astype(jnp.bfloat16)
    grad_cross = gather_rows(grad_cross_rows)
    grad_cross_output_bias = column_sums(grad_cross)
    grad_cross_context = heads_of(project(grad_cross, cross_output.T).astype(jnp.bfloat16))
    cross_grad_q, cross_grad_k, cross_grad_v = attend_backward(
        cross_queries, cross_keys, cross_values, grad_cross_context, cross_totals, segment, False
    )
    cross_grad_q = (cross_grad_q.astype(jnp.bfloat16) * scale).reshape(length, -1)
    cross_grad_k = cross_grad_k.astype(jnp.bfloat16).reshape(length, -1)
    cross_grad_v = cross_grad_v.astype(jnp.bfloat16).reshape(length, -1)
    grad_cross_query = project(first_low.T, cross_grad_q)
    grad_cross_query_bias = column_sums(cross_grad_q)
    grad_cross_key = project(memory.T, cross_grad_k)
    grad_cross_value = project(memory.T, cross_grad_v)
    grad_cross_value_bias = column_sums(cross_grad_v)
    memory_term = project(cross_grad_k, cross_key.T) + project(cross_grad_v, cross_value.T)
    grad_first = grad_second_in + scatter_rows(
        project(cross_grad_q, cross_query.T).astype(jnp.bfloat16)
    )
    grad_first_in, grad_first_gain, grad_first_shift = first_back(grad_first)
    grad_self_rows = grad_first_in.astype(jnp.bfloat16)
    grad_self = gather_rows(grad_self_rows)
    grad_self_output_bias = column_sums(grad_self)
    grad_self_context = heads_of(project(grad_self, self_output.T).astype(jnp.bfloat16))
    dp_size = lax.axis_size("dp")

    def pack(joined, vector):
        width = joined.shape[1]
        lines = -(-vector.shape[0] // width)
        padded = jnp.pad(vector, (0, lines * width - vector.shape[0])).reshape(lines, width)
        high = padded.astype(jnp.bfloat16)
        low = (padded - high.astype(jnp.float32)).astype(jnp.bfloat16)
        extra = jnp.concatenate([high, low], 0)
        blocks = joined.reshape(dp_size, joined.shape[0] // dp_size, width)
        return jnp.concatenate(
            [blocks, jnp.broadcast_to(extra[None], (dp_size,) + extra.shape)], 1
        )

    def exchange(blocks, rows, pieces, flipped, count):
        total = jnp.sum(lax.all_to_all(blocks, "dp", 0, 0, tiled=True).astype(jnp.float32), 0)
        lines = (total.shape[0] - rows) // 2
        vector = (total[rows : rows + lines] + total[rows + lines :]).reshape(-1)[:count]
        parts = []
        offset = 0
        for position, piece in enumerate(pieces):
            width = piece.shape[1]
            part = total[:rows, offset : offset + width]
            offset += width
            if position in flipped:
                part = part.T
            parts.append(part)
        return parts, vector

    grad_cross_output_t = project(grad_cross.T, cross_context)
    grad_self_output_t = project(grad_self.T, self_context)
    norm_pairs = sum_pair(
        jnp.concatenate([grad_first_gain, grad_first_shift, grad_second_gain, grad_second_shift])
    )
    early_vector = jnp.concatenate(
        [
            grad_self_output_bias,
            grad_cross_query_bias,
            grad_cross_value_bias,
            grad_cross_output_bias,
            norm_pairs,
            grad_third_gain,
            grad_third_shift,
            grad_inner_bias,
            grad_outer_bias,
        ]
    )
    cross = [
        grad_cross_query,
        grad_cross_key,
        grad_cross_value,
        grad_cross_output_t,
        grad_self_output_t,
    ]
    cross_blocks = pack(jnp.concatenate(cross, 1).astype(jnp.bfloat16), early_vector)
    cross_blocks, grad_self_context = lax.optimization_barrier((cross_blocks, grad_self_context))
    self_grad_q, self_grad_k, self_grad_v = attend_backward(
        self_queries, self_keys, self_values, grad_self_context, self_totals, segment, True
    )
    self_grad_q = (self_grad_q.astype(jnp.bfloat16) * scale).reshape(length, -1)
    self_grad_k = self_grad_k.astype(jnp.bfloat16).reshape(length, -1)
    self_grad_v = self_grad_v.astype(jnp.bfloat16).reshape(length, -1)
    grad_self_query = project(tokens.T, self_grad_q)
    grad_self_query_bias = column_sums(self_grad_q)
    grad_self_key = project(tokens.T, self_grad_k)
    grad_self_value = project(tokens.T, self_grad_v)
    grad_self_value_bias = column_sums(self_grad_v)
    tokens_term = (
        project(self_grad_q, self_query.T)
        + project(self_grad_k, self_key.T)
        + project(self_grad_v, self_value.T)
    )
    tokens_part = scatter_rows(tokens_term.astype(jnp.bfloat16))
    memory_part = scatter_rows(memory_term.astype(jnp.bfloat16))
    grad_tokens = tokens_part + grad_first_in
    grad_outer_weight_t = project(grad_outer.T, hidden)

    rows = grad_inner_weight.shape[0] // dp_size
    ffn = [grad_inner_weight, grad_outer_weight_t]
    ffn_sum = lax.psum_scatter(
        jnp.concatenate(ffn, 1).astype(jnp.bfloat16), "dp", scatter_dimension=0, tiled=True
    ).astype(jnp.float32)
    ffn_sums = [ffn_sum[:, : ffn[0].shape[1]], ffn_sum[:, ffn[0].shape[1] :].T]
    cross_parts, early_total = exchange(
        cross_blocks, rows, cross, (3, 4), early_vector.shape[0]
    )
    cross_sums = cross_parts[0:4]
    late = [grad_self_query, grad_self_key, grad_self_value]
    late_vector = jnp.concatenate([grad_self_query_bias, grad_self_value_bias])
    self_sums, late_total = exchange(
        pack(jnp.concatenate(late, 1).astype(jnp.bfloat16), late_vector),
        rows,
        late,
        (),
        late_vector.shape[0],
    )
    self_sums.append(cross_parts[4])
    total = jnp.concatenate([late_total, early_total])
    smalls = []
    offset = 0
    for piece in (
        grad_self_query_bias,
        grad_self_value_bias,
        grad_self_output_bias,
        grad_cross_query_bias,
        grad_cross_value_bias,
        grad_cross_output_bias,
        grad_first_gain,
        grad_first_shift,
        grad_second_gain,
        grad_second_shift,
        grad_third_gain,
        grad_third_shift,
        grad_inner_bias,
        grad_outer_bias,
    ):
        smalls.append(total[offset : offset + piece.shape[0]])
        offset += piece.shape[0]
    return (
        output,
        grad_tokens,
        memory_part,
        self_sums[0],
        smalls[0],
        self_sums[1],
        self_sums[2],
        smalls[1],
        self_sums[3],
        smalls[2],
        cross_sums[0],
        smalls[3],
        cross_sums[1],
        cross_sums[2],
        smalls[4],
        cross_sums[3],
        smalls[5],
        smalls[6],
        smalls[7],
        smalls[8],
        smalls[9],
        smalls[10],
        smalls[11],
        ffn_sums[0],
        smalls[12],
        ffn_sums[1],
        smalls[13],
    )


def solution(mesh):
    return jax.shard_map(
        on_device,
        mesh=mesh,
        in_specs=(
            P("dp", None),
            P("dp", None),
            P("dp"),
            P("dp", None),
            P(None, "tensor"),
            P("tensor"),
            P(None, "tensor"),
            P(None, "tensor"),
            P("tensor"),
            P("tensor", None),
            P(),
            P(None, "tensor"),
            P("tensor"),
            P(None, "tensor"),
            P(None, "tensor"),
            P("tensor"),
            P("tensor", None),
            P(),
            P(),
            P(),
            P(),
            P(),
            P(),
            P(),
            P(None, "tensor"),
            P("tensor"),
            P("tensor", None),
            P(),
        ),
        out_specs=(
            P("dp", None),
            P(("dp", "tensor"), None),
            P(("dp", "tensor"), None),
            P("dp", "tensor"),
            P("tensor"),
            P("dp", "tensor"),
            P("dp", "tensor"),
            P("tensor"),
            P("tensor", "dp"),
            P(),
            P("dp", "tensor"),
            P("tensor"),
            P("dp", "tensor"),
            P("dp", "tensor"),
            P("tensor"),
            P("tensor", "dp"),
            P(),
            P(),
            P(),
            P(),
            P(),
            P(),
            P(),
            P("dp", "tensor"),
            P("tensor"),
            P("tensor", "dp"),
            P(),
        ),
        check_vma=False,
    )
```

```python
from functools import partial

import jax
import jax.numpy as jnp
from jax import lax
from jax.sharding import PartitionSpec as P

HD = 64


EPSILON = 1e-05
NEGATIVE = -1e30


def normalize(hidden, gain, shift):
    center = hidden - jnp.mean(hidden, -1, keepdims=True)
    spread = jnp.mean(center * center, -1, keepdims=True)
    return center * lax.rsqrt(spread + EPSILON) * gain + shift


def project(data, weight):
    return jnp.dot(data, weight, preferred_element_type=jnp.float32)


def column_sums(values):
    return jnp.sum(values.astype(jnp.float32), 0)


def heads_of(matrix):
    return matrix.reshape(matrix.shape[0], -1, HD)


def allowed_pairs(query_segment, key_segment, start, causal):
    same = query_segment[:, None] == key_segment[None, :]
    if causal:
        query_place = start + jnp.arange(query_segment.shape[0], dtype=jnp.int32)
        key_place = jnp.arange(key_segment.shape[0], dtype=jnp.int32)
        same = same & (key_place[None, :] <= query_place[:, None])
    return same[None]


def attend_forward(queries, keys, values, segment, causal):
    length = queries.shape[0]
    block_rows = min(256 if causal else 512, length)
    contexts = []
    totals = []
    for index in range(length // block_rows):
        start = index * block_rows
        end = start + block_rows if causal else length
        piece = queries[start : start + block_rows]
        scores = jnp.einsum(
            "qhe,khe->hqk", piece, keys[:end], preferred_element_type=jnp.float32
        )
        scores = jnp.where(
            allowed_pairs(segment[start : start + block_rows], segment[:end], start, causal),
            scores,
            NEGATIVE,
        )
        highest = jnp.max(scores, -1, keepdims=True)
        powers = jnp.exp(scores - highest)
        summed = jnp.sum(powers, -1, keepdims=True)
        weights = (powers / summed).astype(jnp.bfloat16)
        contexts.append(
            jnp.einsum("hqk,khe->qhe", weights, values[:end], preferred_element_type=jnp.float32)
        )
        totals.append(highest + jnp.log(summed))
    return (jnp.concatenate(contexts, 0), jnp.concatenate(totals, 1))


def attend_backward(queries, keys, values, grad_context, totals, segment, causal):
    length = queries.shape[0]
    block_rows = min(256 if causal else 512, length)
    grad_queries = []
    grad_keys = jnp.zeros(keys.shape, jnp.float32)
    grad_values = jnp.zeros(values.shape, jnp.float32)
    for index in range(length // block_rows):
        start = index * block_rows
        end = start + block_rows if causal else length
        piece = queries[start : start + block_rows]
        grad_piece = grad_context[start : start + block_rows]
        near_keys = keys[:end]
        scores = jnp.einsum("qhe,khe->hqk", piece, near_keys, preferred_element_type=jnp.float32)
        scores = jnp.where(
            allowed_pairs(segment[start : start + block_rows], segment[:end], start, causal),
            scores,
            NEGATIVE,
        )
        probs = jnp.exp(scores - totals[:, start : start + block_rows])
        grad_probs = jnp.einsum(
            "qhe,khe->hqk", grad_piece, values[:end], preferred_element_type=jnp.float32
        )
        row_inner = jnp.sum(grad_probs * probs, -1, keepdims=True)
        grad_scores = (probs * (grad_probs - row_inner)).astype(jnp.bfloat16)
        grad_queries.append(
            jnp.einsum("hqk,khe->qhe", grad_scores, near_keys, preferred_element_type=jnp.float32)
        )
        grad_keys = grad_keys.at[:end].add(
            jnp.einsum("hqk,qhe->khe", grad_scores, piece, preferred_element_type=jnp.float32)
        )
        grad_values = grad_values.at[:end].add(
            jnp.einsum(
                "hqk,qhe->khe",
                probs.astype(jnp.bfloat16),
                grad_piece,
                preferred_element_type=jnp.float32,
            )
        )
    return (jnp.concatenate(grad_queries, 0), grad_keys, grad_values)


def on_device(
    tokens,
    memory,
    segment,
    cotangent,
    self_query,
    self_query_bias,
    self_key,
    self_value,
    self_value_bias,
    self_output,
    self_output_bias,
    cross_query,
    cross_query_bias,
    cross_key,
    cross_value,
    cross_value_bias,
    cross_output,
    cross_output_bias,
    first_gain,
    first_shift,
    second_gain,
    second_shift,
    third_gain,
    third_shift,
    inner_weight,
    inner_bias,
    outer_weight,
    outer_bias,
):
    scale = HD ** (-0.5)
    length = tokens.shape[0]
    groups = lax.axis_size("tensor")
    member = lax.axis_index("tensor")
    half = length // groups

    def rows_of(values):
        return lax.dynamic_slice_in_dim(values, member * half, half, 0)

    def spread_out(values):
        whole = jnp.zeros((values.shape[0] * groups,), jnp.float32)
        return lax.dynamic_update_slice_in_dim(whole, values, member * values.shape[0], 0)

    def own_share(values, count):
        return lax.dynamic_slice_in_dim(values, member * count, count, 0)

    def swap(values):
        return lax.ppermute(values, "tensor", [(0, 1), (1, 0)])

    def gather_rows(values):
        if groups != 2:
            return lax.all_gather(values, "tensor", axis=0, tiled=True)
        other = swap(values)
        lead = member == 0
        return jnp.concatenate(
            [jnp.where(lead, values, other), jnp.where(lead, other, values)], 0
        )

    def scatter_rows(values):
        if groups != 2:
            return lax.psum_scatter(
                values, "tensor", scatter_dimension=0, tiled=True
            ).astype(jnp.float32)
        top = values[:half]
        bottom = values[half:]
        lead = member == 0
        keep = jnp.where(lead, top, bottom)
        send = jnp.where(lead, bottom, top)
        return keep.astype(jnp.float32) + swap(send).astype(jnp.float32)

    def sum_pair(values):
        if groups != 2:
            return lax.psum(values, "tensor").astype(jnp.float32)
        return values.astype(jnp.float32) + swap(values).astype(jnp.float32)

    queries = ((project(tokens, self_query) + self_query_bias.astype(jnp.float32)) * scale).astype(
        jnp.bfloat16
    )
    keys = project(tokens, self_key).astype(jnp.bfloat16)
    values = (project(tokens, self_value) + self_value_bias.astype(jnp.float32)).astype(
        jnp.bfloat16
    )
    self_queries = heads_of(queries)
    self_keys = heads_of(keys)
    self_values = heads_of(values)
    self_context, self_totals = attend_forward(self_queries, self_keys, self_values, segment, True)
    self_context = self_context.reshape(length, -1).astype(jnp.bfloat16)
    attended = scatter_rows(project(self_context, self_output)) + self_output_bias.astype(
        jnp.float32
    )
    first, first_back = jax.vjp(
        normalize,
        rows_of(tokens).astype(jnp.float32) + attended,
        first_gain.astype(jnp.float32),
        first_shift.astype(jnp.float32),
    )
    first_low = gather_rows(first.astype(jnp.bfloat16))
    queries = (
        (project(first_low, cross_query) + cross_query_bias.astype(jnp.float32)) * scale
    ).astype(jnp.bfloat16)
    keys = project(memory, cross_key).astype(jnp.bfloat16)
    values = (project(memory, cross_value) + cross_value_bias.astype(jnp.float32)).astype(
        jnp.bfloat16
    )
    cross_queries = heads_of(queries)
    cross_keys = heads_of(keys)
    cross_values = heads_of(values)
    cross_context, cross_totals = attend_forward(
        cross_queries, cross_keys, cross_values, segment, False
    )
    cross_context = cross_context.reshape(length, -1).astype(jnp.bfloat16)
    crossed = scatter_rows(
        project(cross_context, cross_output).astype(jnp.bfloat16)
    ) + cross_output_bias.astype(jnp.float32)
    second_part, second_back = jax.vjp(
        normalize,
        first + crossed,
        second_gain.astype(jnp.float32),
        second_shift.astype(jnp.float32),
    )
    second = gather_rows(second_part.astype(jnp.bfloat16)).astype(second_part.dtype)
    second_low = second.astype(jnp.bfloat16)
    inner = project(second_low, inner_weight) + inner_bias.astype(jnp.float32)
    hidden = jax.nn.gelu(inner, approximate=False).astype(jnp.bfloat16)
    outer = sum_pair(project(hidden, outer_weight).astype(jnp.bfloat16)) + outer_bias.astype(
        jnp.float32
    )
    result, third_back = jax.vjp(
        normalize, second + outer, third_gain.astype(jnp.float32), third_shift.astype(jnp.float32)
    )
    output = result.astype(jnp.bfloat16)
    grad_third, grad_third_gain, grad_third_shift = third_back(cotangent.astype(jnp.float32))
    grad_outer = grad_third.astype(jnp.bfloat16)
    grad_outer_bias = column_sums(grad_outer)
    gelu_back = jax.vjp(partial(jax.nn.gelu, approximate=False), inner)[1]
    grad_inner = gelu_back(project(grad_outer, outer_weight.T))[0].astype(jnp.bfloat16)
    grad_inner_weight = project(second_low.T, grad_inner)
    grad_inner_bias = column_sums(grad_inner)
    grad_second = rows_of(grad_third) + scatter_rows(
        project(grad_inner, inner_weight.T).astype(jnp.bfloat16)
    )
    grad_second_in, grad_second_gain, grad_second_shift = second_back(grad_second)
    grad_cross_rows = grad_second_in.astype(jnp.bfloat16)
    grad_cross = gather_rows(grad_cross_rows)
    grad_cross_output_bias = column_sums(grad_cross)
    grad_cross_context = heads_of(project(grad_cross, cross_output.T).astype(jnp.bfloat16))
    cross_grad_q, cross_grad_k, cross_grad_v = attend_backward(
        cross_queries, cross_keys, cross_values, grad_cross_context, cross_totals, segment, False
    )
    cross_grad_q = (cross_grad_q.astype(jnp.bfloat16) * scale).reshape(length, -1)
    cross_grad_k = cross_grad_k.astype(jnp.bfloat16).reshape(length, -1)
    cross_grad_v = cross_grad_v.astype(jnp.bfloat16).reshape(length, -1)
    grad_cross_query = project(first_low.T, cross_grad_q)
    grad_cross_query_bias = column_sums(cross_grad_q)
    grad_cross_key = project(memory.T, cross_grad_k)
    grad_cross_value = project(memory.T, cross_grad_v)
    grad_cross_value_bias = column_sums(cross_grad_v)
    memory_term = project(cross_grad_k, cross_key.T) + project(cross_grad_v, cross_value.T)
    grad_first = grad_second_in + scatter_rows(
        project(cross_grad_q, cross_query.T).astype(jnp.bfloat16)
    )
    grad_first_in, grad_first_gain, grad_first_shift = first_back(grad_first)
    grad_self_rows = grad_first_in.astype(jnp.bfloat16)
    grad_self = gather_rows(grad_self_rows)
    grad_self_output_bias = column_sums(grad_self)
    grad_self_context = heads_of(project(grad_self, self_output.T).astype(jnp.bfloat16))
    dp_size = lax.axis_size("dp")
    grad_cross_output_t = project(grad_cross.T, cross_context)
    cross = [grad_cross_query, grad_cross_key, grad_cross_value, grad_cross_output_t]
    cross_joined = jnp.concatenate(cross, 1).astype(jnp.bfloat16)
    cross_joined, grad_self_context = lax.optimization_barrier((cross_joined, grad_self_context))
    self_grad_q, self_grad_k, self_grad_v = attend_backward(
        self_queries, self_keys, self_values, grad_self_context, self_totals, segment, True
    )
    self_grad_q = (self_grad_q.astype(jnp.bfloat16) * scale).reshape(length, -1)
    self_grad_k = self_grad_k.astype(jnp.bfloat16).reshape(length, -1)
    self_grad_v = self_grad_v.astype(jnp.bfloat16).reshape(length, -1)
    grad_self_query = project(tokens.T, self_grad_q)
    grad_self_query_bias = column_sums(self_grad_q)
    grad_self_key = project(tokens.T, self_grad_k)
    grad_self_value = project(tokens.T, self_grad_v)
    grad_self_value_bias = column_sums(self_grad_v)
    tokens_term = (
        project(self_grad_q, self_query.T)
        + project(self_grad_k, self_key.T)
        + project(self_grad_v, self_value.T)
    )
    tokens_part = scatter_rows(tokens_term.astype(jnp.bfloat16))
    memory_part = scatter_rows(memory_term.astype(jnp.bfloat16))
    grad_tokens = tokens_part + grad_first_in
    grad_self_output_t = project(grad_self.T, self_context)
    grad_outer_weight_t = project(grad_outer.T, hidden)

    def split_columns(summed, pieces, flipped):
        parts = []
        offset = 0
        for position, piece in enumerate(pieces):
            width = piece.shape[1]
            part = summed[:, offset : offset + width]
            offset += width
            if position in flipped:
                part = part.T
            parts.append(part)
        return parts

    def exchange_sum(joined, extra=None):
        rows = joined.shape[0] // dp_size
        blocks = joined.reshape(dp_size, rows, joined.shape[1])
        if extra is not None:
            blocks = jnp.concatenate(
                [blocks, jnp.broadcast_to(extra[None], (dp_size,) + extra.shape)], 1
            )
        received = lax.all_to_all(blocks, "dp", 0, 0, tiled=True)
        return jnp.sum(received.astype(jnp.float32), 0)

    ffn = [grad_inner_weight, grad_outer_weight_t]
    ffn_sum = lax.psum_scatter(
        jnp.concatenate(ffn, 1).astype(jnp.bfloat16), "dp", scatter_dimension=0, tiled=True
    ).astype(jnp.float32)
    ffn_sums = split_columns(ffn_sum, ffn, (1,))
    cross_sums = split_columns(exchange_sum(cross_joined), cross, (3,))
    late = [grad_self_query, grad_self_key, grad_self_value, grad_self_output_t]
    late_joined = jnp.concatenate(late, 1).astype(jnp.bfloat16)
    norm_pairs = sum_pair(
        jnp.concatenate([grad_first_gain, grad_first_shift, grad_second_gain, grad_second_shift])
    )
    width = late_joined.shape[1]
    sections = norm_pairs.shape[0] // 4
    biases = [
        grad_self_query_bias,
        grad_self_value_bias,
        grad_self_output_bias,
        grad_cross_query_bias,
        grad_cross_value_bias,
        grad_cross_output_bias,
        norm_pairs[:sections],
        norm_pairs[sections : 2 * sections],
        norm_pairs[2 * sections : 3 * sections],
        norm_pairs[3 * sections :],
        grad_third_gain,
        grad_third_shift,
        grad_inner_bias,
        grad_outer_bias,
    ]
    lines = []
    current = []
    used = 0
    places = []
    for bias in biases:
        chunks = []
        for begin in range(0, bias.shape[0], width):
            chunk = bias[begin : begin + width]
            if used + chunk.shape[0] > width:
                if used < width:
                    current.append(jnp.zeros((width - used,), jnp.float32))
                lines.append(jnp.concatenate(current))
                current = []
                used = 0
            chunks.append((len(lines), used, chunk.shape[0]))
            current.append(chunk)
            used += chunk.shape[0]
        places.append(chunks)
    if used < width:
        current.append(jnp.zeros((width - used,), jnp.float32))
    lines.append(jnp.concatenate(current))
    padded = jnp.stack(lines)
    count = padded.shape[0]
    high = padded.astype(jnp.bfloat16)
    low = (padded - high.astype(jnp.float32)).astype(jnp.bfloat16)
    late_rows = late_joined.shape[0] // dp_size
    late_total = exchange_sum(late_joined, jnp.concatenate([high, low], 0))
    self_sums = split_columns(late_total[:late_rows], late, (3,))
    summed_lines = late_total[late_rows : late_rows + count] + late_total[late_rows + count :]
    smalls = []
    for chunks in places:
        smalls.append(
            jnp.concatenate(
                [summed_lines[line, begin : begin + size] for line, begin, size in chunks]
            )
        )
    return (
        output,
        grad_tokens,
        memory_part,
        self_sums[0],
        smalls[0],
        self_sums[1],
        self_sums[2],
        smalls[1],
        self_sums[3],
        smalls[2],
        cross_sums[0],
        smalls[3],
        cross_sums[1],
        cross_sums[2],
        smalls[4],
        cross_sums[3],
        smalls[5],
        smalls[6],
        smalls[7],
        smalls[8],
        smalls[9],
        smalls[10],
        smalls[11],
        ffn_sums[0],
        smalls[12],
        ffn_sums[1],
        smalls[13],
    )


def solution(mesh):
    return jax.shard_map(
        on_device,
        mesh=mesh,
        in_specs=(
            P("dp", None),
            P("dp", None),
            P("dp"),
            P("dp", None),
            P(None, "tensor"),
            P("tensor"),
            P(None, "tensor"),
            P(None, "tensor"),
            P("tensor"),
            P("tensor", None),
            P(),
            P(None, "tensor"),
            P("tensor"),
            P(None, "tensor"),
            P(None, "tensor"),
            P("tensor"),
            P("tensor", None),
            P(),
            P(),
            P(),
            P(),
            P(),
            P(),
            P(),
            P(None, "tensor"),
            P("tensor"),
            P("tensor", None),
            P(),
        ),
        out_specs=(
            P("dp", None),
            P(("dp", "tensor"), None),
            P(("dp", "tensor"), None),
            P("dp", "tensor"),
            P("tensor"),
            P("dp", "tensor"),
            P("dp", "tensor"),
            P("tensor"),
            P("tensor", "dp"),
            P(),
            P("dp", "tensor"),
            P("tensor"),
            P("dp", "tensor"),
            P("dp", "tensor"),
            P("tensor"),
            P("tensor", "dp"),
            P(),
            P(),
            P(),
            P(),
            P(),
            P(),
            P(),
            P("dp", "tensor"),
            P("tensor"),
            P("tensor", "dp"),
            P(),
        ),
        check_vma=False,
    )
```

```python
from functools import partial

import jax
import jax.numpy as jnp
from jax import lax
from jax.sharding import PartitionSpec as P

HD = 64


EPSILON = 1e-05
NEGATIVE = -1e30


def normalize(hidden, gain, shift):
    center = hidden - jnp.mean(hidden, -1, keepdims=True)
    spread = jnp.mean(center * center, -1, keepdims=True)
    return center * lax.rsqrt(spread + EPSILON) * gain + shift


def project(data, weight):
    return jnp.dot(data, weight, preferred_element_type=jnp.float32)


def column_sums(values):
    return jnp.sum(values.astype(jnp.float32), 0)


def heads_of(matrix):
    return matrix.reshape(matrix.shape[0], -1, HD)


def allowed_pairs(query_segment, key_segment, start, causal):
    same = query_segment[:, None] == key_segment[None, :]
    if causal:
        query_place = start + jnp.arange(query_segment.shape[0], dtype=jnp.int32)
        key_place = jnp.arange(key_segment.shape[0], dtype=jnp.int32)
        same = same & (key_place[None, :] <= query_place[:, None])
    return same[None]


def attend_forward(queries, keys, values, segment, causal):
    length = queries.shape[0]
    block_rows = min(256 if causal else 512, length)
    contexts = []
    totals = []
    for index in range(length // block_rows):
        start = index * block_rows
        end = start + block_rows if causal else length
        piece = queries[start : start + block_rows]
        scores = jnp.einsum(
            "qhe,khe->hqk", piece, keys[:end], preferred_element_type=jnp.float32
        )
        scores = jnp.where(
            allowed_pairs(segment[start : start + block_rows], segment[:end], start, causal),
            scores,
            NEGATIVE,
        )
        highest = jnp.max(scores, -1, keepdims=True)
        powers = jnp.exp(scores - highest)
        summed = jnp.sum(powers, -1, keepdims=True)
        weights = (powers / summed).astype(jnp.bfloat16)
        contexts.append(
            jnp.einsum("hqk,khe->qhe", weights, values[:end], preferred_element_type=jnp.float32)
        )
        totals.append(highest + jnp.log(summed))
    return (jnp.concatenate(contexts, 0), jnp.concatenate(totals, 1))


def attend_backward(queries, keys, values, grad_context, totals, segment, causal):
    length = queries.shape[0]
    block_rows = min(256 if causal else 512, length)
    grad_queries = []
    grad_keys = jnp.zeros(keys.shape, jnp.float32)
    grad_values = jnp.zeros(values.shape, jnp.float32)
    for index in range(length // block_rows):
        start = index * block_rows
        end = start + block_rows if causal else length
        piece = queries[start : start + block_rows]
        grad_piece = grad_context[start : start + block_rows]
        near_keys = keys[:end]
        scores = jnp.einsum("qhe,khe->hqk", piece, near_keys, preferred_element_type=jnp.float32)
        scores = jnp.where(
            allowed_pairs(segment[start : start + block_rows], segment[:end], start, causal),
            scores,
            NEGATIVE,
        )
        probs = jnp.exp(scores - totals[:, start : start + block_rows])
        grad_probs = jnp.einsum(
            "qhe,khe->hqk", grad_piece, values[:end], preferred_element_type=jnp.float32
        )
        row_inner = jnp.sum(grad_probs * probs, -1, keepdims=True)
        grad_scores = (probs * (grad_probs - row_inner)).astype(jnp.bfloat16)
        grad_queries.append(
            jnp.einsum("hqk,khe->qhe", grad_scores, near_keys, preferred_element_type=jnp.float32)
        )
        grad_keys = grad_keys.at[:end].add(
            jnp.einsum("hqk,qhe->khe", grad_scores, piece, preferred_element_type=jnp.float32)
        )
        grad_values = grad_values.at[:end].add(
            jnp.einsum(
                "hqk,qhe->khe",
                probs.astype(jnp.bfloat16),
                grad_piece,
                preferred_element_type=jnp.float32,
            )
        )
    return (jnp.concatenate(grad_queries, 0), grad_keys, grad_values)


def on_device(
    tokens,
    memory,
    segment,
    cotangent,
    self_query,
    self_query_bias,
    self_key,
    self_value,
    self_value_bias,
    self_output,
    self_output_bias,
    cross_query,
    cross_query_bias,
    cross_key,
    cross_value,
    cross_value_bias,
    cross_output,
    cross_output_bias,
    first_gain,
    first_shift,
    second_gain,
    second_shift,
    third_gain,
    third_shift,
    inner_weight,
    inner_bias,
    outer_weight,
    outer_bias,
):
    scale = HD ** (-0.5)
    length = tokens.shape[0]
    groups = lax.axis_size("tensor")
    member = lax.axis_index("tensor")
    half = length // groups

    def rows_of(values):
        return lax.dynamic_slice_in_dim(values, member * half, half, 0)

    def spread_out(values):
        whole = jnp.zeros((values.shape[0] * groups,), jnp.float32)
        return lax.dynamic_update_slice_in_dim(whole, values, member * values.shape[0], 0)

    def own_share(values, count):
        return lax.dynamic_slice_in_dim(values, member * count, count, 0)

    def swap(values):
        return lax.ppermute(values, "tensor", [(0, 1), (1, 0)])

    def gather_rows(values):
        if groups != 2:
            return lax.all_gather(values, "tensor", axis=0, tiled=True)
        other = swap(values)
        lead = member == 0
        return jnp.concatenate(
            [jnp.where(lead, values, other), jnp.where(lead, other, values)], 0
        )

    def scatter_rows(values):
        if groups != 2:
            return lax.psum_scatter(
                values, "tensor", scatter_dimension=0, tiled=True
            ).astype(jnp.float32)
        top = values[:half]
        bottom = values[half:]
        lead = member == 0
        keep = jnp.where(lead, top, bottom)
        send = jnp.where(lead, bottom, top)
        return keep.astype(jnp.float32) + swap(send).astype(jnp.float32)

    def sum_pair(values):
        if groups != 2:
            return lax.psum(values, "tensor").astype(jnp.float32)
        return values.astype(jnp.float32) + swap(values).astype(jnp.float32)

    queries = ((project(tokens, self_query) + self_query_bias.astype(jnp.float32)) * scale).astype(
        jnp.bfloat16
    )
    keys = project(tokens, self_key).astype(jnp.bfloat16)
    values = (project(tokens, self_value) + self_value_bias.astype(jnp.float32)).astype(
        jnp.bfloat16
    )
    self_queries = heads_of(queries)
    self_keys = heads_of(keys)
    self_values = heads_of(values)
    self_context, self_totals = attend_forward(self_queries, self_keys, self_values, segment, True)
    self_context = self_context.reshape(length, -1).astype(jnp.bfloat16)
    attended = scatter_rows(project(self_context, self_output)) + self_output_bias.astype(
        jnp.float32
    )
    first, first_back = jax.vjp(
        normalize,
        rows_of(tokens).astype(jnp.float32) + attended,
        first_gain.astype(jnp.float32),
        first_shift.astype(jnp.float32),
    )
    first_low = gather_rows(first.astype(jnp.bfloat16))
    queries = (
        (project(first_low, cross_query) + cross_query_bias.astype(jnp.float32)) * scale
    ).astype(jnp.bfloat16)
    keys = project(memory, cross_key).astype(jnp.bfloat16)
    values = (project(memory, cross_value) + cross_value_bias.astype(jnp.float32)).astype(
        jnp.bfloat16
    )
    cross_queries = heads_of(queries)
    cross_keys = heads_of(keys)
    cross_values = heads_of(values)
    cross_context, cross_totals = attend_forward(
        cross_queries, cross_keys, cross_values, segment, False
    )
    cross_context = cross_context.reshape(length, -1).astype(jnp.bfloat16)
    crossed = scatter_rows(
        project(cross_context, cross_output).astype(jnp.bfloat16)
    ) + cross_output_bias.astype(jnp.float32)
    second_part, second_back = jax.vjp(
        normalize,
        first + crossed,
        second_gain.astype(jnp.float32),
        second_shift.astype(jnp.float32),
    )
    second = gather_rows(second_part.astype(jnp.bfloat16)).astype(second_part.dtype)
    second_low = second.astype(jnp.bfloat16)
    inner = project(second_low, inner_weight) + inner_bias.astype(jnp.float32)
    hidden = jax.nn.gelu(inner, approximate=False).astype(jnp.bfloat16)
    outer = sum_pair(project(hidden, outer_weight).astype(jnp.bfloat16)) + outer_bias.astype(
        jnp.float32
    )
    result, third_back = jax.vjp(
        normalize, second + outer, third_gain.astype(jnp.float32), third_shift.astype(jnp.float32)
    )
    output = result.astype(jnp.bfloat16)
    grad_third, grad_third_gain, grad_third_shift = third_back(cotangent.astype(jnp.float32))
    grad_outer = grad_third.astype(jnp.bfloat16)
    grad_outer_bias = column_sums(grad_outer)
    gelu_back = jax.vjp(partial(jax.nn.gelu, approximate=False), inner)[1]
    grad_inner = gelu_back(project(grad_outer, outer_weight.T))[0].astype(jnp.bfloat16)
    grad_inner_weight = project(second_low.T, grad_inner)
    grad_inner_bias = column_sums(grad_inner)
    grad_second = rows_of(grad_third) + scatter_rows(
        project(grad_inner, inner_weight.T).astype(jnp.bfloat16)
    )
    grad_second_in, grad_second_gain, grad_second_shift = second_back(grad_second)
    grad_cross_rows = grad_second_in.astype(jnp.bfloat16)
    grad_cross = gather_rows(grad_cross_rows)
    grad_cross_output_bias = column_sums(grad_cross)
    grad_cross_context = heads_of(project(grad_cross, cross_output.T).astype(jnp.bfloat16))
    cross_grad_q, cross_grad_k, cross_grad_v = attend_backward(
        cross_queries, cross_keys, cross_values, grad_cross_context, cross_totals, segment, False
    )
    cross_grad_q = (cross_grad_q.astype(jnp.bfloat16) * scale).reshape(length, -1)
    cross_grad_k = cross_grad_k.astype(jnp.bfloat16).reshape(length, -1)
    cross_grad_v = cross_grad_v.astype(jnp.bfloat16).reshape(length, -1)
    grad_cross_query = project(first_low.T, cross_grad_q)
    grad_cross_query_bias = column_sums(cross_grad_q)
    grad_cross_key = project(memory.T, cross_grad_k)
    grad_cross_value = project(memory.T, cross_grad_v)
    grad_cross_value_bias = column_sums(cross_grad_v)
    memory_term = project(cross_grad_k, cross_key.T) + project(cross_grad_v, cross_value.T)
    grad_first = grad_second_in + scatter_rows(
        project(cross_grad_q, cross_query.T).astype(jnp.bfloat16)
    )
    grad_cross_output_t = project(grad_cross.T, cross_context)
    cross = [grad_cross_query, grad_cross_key, grad_cross_value, grad_cross_output_t]
    cross_joined = jnp.concatenate(cross, 1).astype(jnp.bfloat16)
    cross_joined, grad_first = lax.optimization_barrier((cross_joined, grad_first))
    grad_first_in, grad_first_gain, grad_first_shift = first_back(grad_first)
    grad_self_rows = grad_first_in.astype(jnp.bfloat16)
    grad_self = gather_rows(grad_self_rows)
    grad_self_output_bias = column_sums(grad_self)
    grad_self_context = heads_of(project(grad_self, self_output.T).astype(jnp.bfloat16))
    dp_size = lax.axis_size("dp")
    self_grad_q, self_grad_k, self_grad_v = attend_backward(
        self_queries, self_keys, self_values, grad_self_context, self_totals, segment, True
    )
    self_grad_q = (self_grad_q.astype(jnp.bfloat16) * scale).reshape(length, -1)
    self_grad_k = self_grad_k.astype(jnp.bfloat16).reshape(length, -1)
    self_grad_v = self_grad_v.astype(jnp.bfloat16).reshape(length, -1)
    grad_self_query = project(tokens.T, self_grad_q)
    grad_self_query_bias = column_sums(self_grad_q)
    grad_self_key = project(tokens.T, self_grad_k)
    grad_self_value = project(tokens.T, self_grad_v)
    grad_self_value_bias = column_sums(self_grad_v)
    tokens_term = (
        project(self_grad_q, self_query.T)
        + project(self_grad_k, self_key.T)
        + project(self_grad_v, self_value.T)
    )
    tokens_part = scatter_rows(tokens_term.astype(jnp.bfloat16))
    memory_part = scatter_rows(memory_term.astype(jnp.bfloat16))
    grad_tokens = tokens_part + grad_first_in
    grad_self_output_t = project(grad_self.T, self_context)
    grad_outer_weight_t = project(grad_outer.T, hidden)

    def split_columns(summed, pieces, flipped):
        parts = []
        offset = 0
        for position, piece in enumerate(pieces):
            width = piece.shape[1]
            part = summed[:, offset : offset + width]
            offset += width
            if position in flipped:
                part = part.T
            parts.append(part)
        return parts

    def exchange_sum(joined, extra=None):
        rows = joined.shape[0] // dp_size
        blocks = joined.reshape(dp_size, rows, joined.shape[1])
        if extra is not None:
            blocks = jnp.concatenate(
                [blocks, jnp.broadcast_to(extra[None], (dp_size,) + extra.shape)], 1
            )
        received = lax.all_to_all(blocks, "dp", 0, 0, tiled=True)
        return jnp.sum(received.astype(jnp.float32), 0)

    ffn = [grad_inner_weight, grad_outer_weight_t]
    ffn_sum = lax.psum_scatter(
        jnp.concatenate(ffn, 1).astype(jnp.bfloat16), "dp", scatter_dimension=0, tiled=True
    ).astype(jnp.float32)
    ffn_sums = split_columns(ffn_sum, ffn, (1,))
    cross_sums = split_columns(exchange_sum(cross_joined), cross, (3,))
    late = [grad_self_query, grad_self_key, grad_self_value, grad_self_output_t]
    late_joined = jnp.concatenate(late, 1).astype(jnp.bfloat16)
    norm_pairs = sum_pair(
        jnp.concatenate([grad_first_gain, grad_first_shift, grad_second_gain, grad_second_shift])
    )
    width = late_joined.shape[1]
    sections = norm_pairs.shape[0] // 4
    biases = [
        grad_self_query_bias,
        grad_self_value_bias,
        grad_self_output_bias,
        grad_cross_query_bias,
        grad_cross_value_bias,
        grad_cross_output_bias,
        norm_pairs[:sections],
        norm_pairs[sections : 2 * sections],
        norm_pairs[2 * sections : 3 * sections],
        norm_pairs[3 * sections :],
        grad_third_gain,
        grad_third_shift,
        grad_inner_bias,
        grad_outer_bias,
    ]
    lines = []
    current = []
    used = 0
    places = []
    for bias in biases:
        chunks = []
        for begin in range(0, bias.shape[0], width):
            chunk = bias[begin : begin + width]
            if used + chunk.shape[0] > width:
                if used < width:
                    current.append(jnp.zeros((width - used,), jnp.float32))
                lines.append(jnp.concatenate(current))
                current = []
                used = 0
            chunks.append((len(lines), used, chunk.shape[0]))
            current.append(chunk)
            used += chunk.shape[0]
        places.append(chunks)
    if used < width:
        current.append(jnp.zeros((width - used,), jnp.float32))
    lines.append(jnp.concatenate(current))
    padded = jnp.stack(lines)
    count = padded.shape[0]
    high = padded.astype(jnp.bfloat16)
    low = (padded - high.astype(jnp.float32)).astype(jnp.bfloat16)
    late_rows = late_joined.shape[0] // dp_size
    late_total = exchange_sum(late_joined, jnp.concatenate([high, low], 0))
    self_sums = split_columns(late_total[:late_rows], late, (3,))
    summed_lines = late_total[late_rows : late_rows + count] + late_total[late_rows + count :]
    smalls = []
    for chunks in places:
        smalls.append(
            jnp.concatenate(
                [summed_lines[line, begin : begin + size] for line, begin, size in chunks]
            )
        )
    return (
        output,
        grad_tokens,
        memory_part,
        self_sums[0],
        smalls[0],
        self_sums[1],
        self_sums[2],
        smalls[1],
        self_sums[3],
        smalls[2],
        cross_sums[0],
        smalls[3],
        cross_sums[1],
        cross_sums[2],
        smalls[4],
        cross_sums[3],
        smalls[5],
        smalls[6],
        smalls[7],
        smalls[8],
        smalls[9],
        smalls[10],
        smalls[11],
        ffn_sums[0],
        smalls[12],
        ffn_sums[1],
        smalls[13],
    )


def solution(mesh):
    return jax.shard_map(
        on_device,
        mesh=mesh,
        in_specs=(
            P("dp", None),
            P("dp", None),
            P("dp"),
            P("dp", None),
            P(None, "tensor"),
            P("tensor"),
            P(None, "tensor"),
            P(None, "tensor"),
            P("tensor"),
            P("tensor", None),
            P(),
            P(None, "tensor"),
            P("tensor"),
            P(None, "tensor"),
            P(None, "tensor"),
            P("tensor"),
            P("tensor", None),
            P(),
            P(),
            P(),
            P(),
            P(),
            P(),
            P(),
            P(None, "tensor"),
            P("tensor"),
            P("tensor", None),
            P(),
        ),
        out_specs=(
            P("dp", None),
            P(("dp", "tensor"), None),
            P(("dp", "tensor"), None),
            P("dp", "tensor"),
            P("tensor"),
            P("dp", "tensor"),
            P("dp", "tensor"),
            P("tensor"),
            P("tensor", "dp"),
            P(),
            P("dp", "tensor"),
            P("tensor"),
            P("dp", "tensor"),
            P("dp", "tensor"),
            P("tensor"),
            P("tensor", "dp"),
            P(),
            P(),
            P(),
            P(),
            P(),
            P(),
            P(),
            P("dp", "tensor"),
            P("tensor"),
            P("tensor", "dp"),
            P(),
        ),
        check_vma=False,
    )
```

```python
from functools import partial

import jax
import jax.numpy as jnp
from jax import lax
from jax.sharding import PartitionSpec as P

HD = 64


EPSILON = 1e-05
NEGATIVE = -1e30


def normalize(hidden, gain, shift):
    center = hidden - jnp.mean(hidden, -1, keepdims=True)
    spread = jnp.mean(center * center, -1, keepdims=True)
    return center * lax.rsqrt(spread + EPSILON) * gain + shift


def project(data, weight):
    return jnp.dot(data, weight, preferred_element_type=jnp.float32)


def column_sums(values):
    return jnp.sum(values.astype(jnp.float32), 0)


def heads_of(matrix):
    return matrix.reshape(matrix.shape[0], -1, HD)


def allowed_pairs(query_segment, key_segment, start, causal):
    same = query_segment[:, None] == key_segment[None, :]
    if causal:
        query_place = start + jnp.arange(query_segment.shape[0], dtype=jnp.int32)
        key_place = jnp.arange(key_segment.shape[0], dtype=jnp.int32)
        same = same & (key_place[None, :] <= query_place[:, None])
    return same[None]


def attend_forward(queries, keys, values, segment, causal):
    length = queries.shape[0]
    block_rows = min(256 if causal else 512, length)
    contexts = []
    totals = []
    for index in range(length // block_rows):
        start = index * block_rows
        end = start + block_rows if causal else length
        piece = queries[start : start + block_rows]
        scores = jnp.einsum(
            "qhe,khe->hqk", piece, keys[:end], preferred_element_type=jnp.float32
        )
        scores = jnp.where(
            allowed_pairs(segment[start : start + block_rows], segment[:end], start, causal),
            scores,
            NEGATIVE,
        )
        highest = jnp.max(scores, -1, keepdims=True)
        powers = jnp.exp(scores - highest)
        summed = jnp.sum(powers, -1, keepdims=True)
        weights = (powers / summed).astype(jnp.bfloat16)
        contexts.append(
            jnp.einsum("hqk,khe->qhe", weights, values[:end], preferred_element_type=jnp.float32)
        )
        totals.append(highest + jnp.log(summed))
    return (jnp.concatenate(contexts, 0), jnp.concatenate(totals, 1))


def attend_backward(queries, keys, values, grad_context, totals, segment, causal, exact_context):
    length = queries.shape[0]
    block_rows = min(256 if causal else 512, length)
    inner = jnp.einsum(
        "qhe,qhe->hq", grad_context.astype(jnp.float32), exact_context
    )[..., None]
    grad_queries = []
    grad_keys = jnp.zeros(keys.shape, jnp.float32)
    grad_values = jnp.zeros(values.shape, jnp.float32)
    for index in range(length // block_rows):
        start = index * block_rows
        end = start + block_rows if causal else length
        piece = queries[start : start + block_rows]
        grad_piece = grad_context[start : start + block_rows]
        near_keys = keys[:end]
        scores = jnp.einsum("qhe,khe->hqk", piece, near_keys, preferred_element_type=jnp.float32)
        scores = jnp.where(
            allowed_pairs(segment[start : start + block_rows], segment[:end], start, causal),
            scores,
            NEGATIVE,
        )
        probs = jnp.exp(scores - totals[:, start : start + block_rows])
        grad_probs = jnp.einsum(
            "qhe,khe->hqk", grad_piece, values[:end], preferred_element_type=jnp.float32
        )
        row_inner = inner[:, start : start + block_rows]
        grad_scores = (probs * (grad_probs - row_inner)).astype(jnp.bfloat16)
        grad_queries.append(
            jnp.einsum("hqk,khe->qhe", grad_scores, near_keys, preferred_element_type=jnp.float32)
        )
        grad_keys = grad_keys.at[:end].add(
            jnp.einsum("hqk,qhe->khe", grad_scores, piece, preferred_element_type=jnp.float32)
        )
        grad_values = grad_values.at[:end].add(
            jnp.einsum(
                "hqk,qhe->khe",
                probs.astype(jnp.bfloat16),
                grad_piece,
                preferred_element_type=jnp.float32,
            )
        )
    return (jnp.concatenate(grad_queries, 0), grad_keys, grad_values)


def on_device(
    tokens,
    memory,
    segment,
    cotangent,
    self_query,
    self_query_bias,
    self_key,
    self_value,
    self_value_bias,
    self_output,
    self_output_bias,
    cross_query,
    cross_query_bias,
    cross_key,
    cross_value,
    cross_value_bias,
    cross_output,
    cross_output_bias,
    first_gain,
    first_shift,
    second_gain,
    second_shift,
    third_gain,
    third_shift,
    inner_weight,
    inner_bias,
    outer_weight,
    outer_bias,
):
    scale = HD ** (-0.5)
    length = tokens.shape[0]
    groups = lax.axis_size("tensor")
    member = lax.axis_index("tensor")
    half = length // groups

    def rows_of(values):
        return lax.dynamic_slice_in_dim(values, member * half, half, 0)

    def spread_out(values):
        whole = jnp.zeros((values.shape[0] * groups,), jnp.float32)
        return lax.dynamic_update_slice_in_dim(whole, values, member * values.shape[0], 0)

    def own_share(values, count):
        return lax.dynamic_slice_in_dim(values, member * count, count, 0)

    def swap(values):
        return lax.ppermute(values, "tensor", [(0, 1), (1, 0)])

    def gather_rows(values):
        if groups != 2:
            return lax.all_gather(values, "tensor", axis=0, tiled=True)
        other = swap(values)
        lead = member == 0
        return jnp.concatenate(
            [jnp.where(lead, values, other), jnp.where(lead, other, values)], 0
        )

    def scatter_rows(values):
        if groups != 2:
            return lax.psum_scatter(
                values, "tensor", scatter_dimension=0, tiled=True
            ).astype(jnp.float32)
        top = values[:half]
        bottom = values[half:]
        lead = member == 0
        keep = jnp.where(lead, top, bottom)
        send = jnp.where(lead, bottom, top)
        return keep.astype(jnp.float32) + swap(send).astype(jnp.float32)

    def sum_pair(values):
        if groups != 2:
            return lax.psum(values, "tensor").astype(jnp.float32)
        return values.astype(jnp.float32) + swap(values).astype(jnp.float32)

    queries = ((project(tokens, self_query) + self_query_bias.astype(jnp.float32)) * scale).astype(
        jnp.bfloat16
    )
    keys = project(tokens, self_key).astype(jnp.bfloat16)
    values = (project(tokens, self_value) + self_value_bias.astype(jnp.float32)).astype(
        jnp.bfloat16
    )
    self_queries = heads_of(queries)
    self_keys = heads_of(keys)
    self_values = heads_of(values)
    self_context, self_totals = attend_forward(self_queries, self_keys, self_values, segment, True)
    self_exact = self_context
    self_context = self_context.reshape(length, -1).astype(jnp.bfloat16)
    attended = scatter_rows(project(self_context, self_output)) + self_output_bias.astype(
        jnp.float32
    )
    first, first_back = jax.vjp(
        normalize,
        rows_of(tokens).astype(jnp.float32) + attended,
        first_gain.astype(jnp.float32),
        first_shift.astype(jnp.float32),
    )
    first_low = gather_rows(first.astype(jnp.bfloat16))
    queries = (
        (project(first_low, cross_query) + cross_query_bias.astype(jnp.float32)) * scale
    ).astype(jnp.bfloat16)
    keys = project(memory, cross_key).astype(jnp.bfloat16)
    values = (project(memory, cross_value) + cross_value_bias.astype(jnp.float32)).astype(
        jnp.bfloat16
    )
    cross_queries = heads_of(queries)
    cross_keys = heads_of(keys)
    cross_values = heads_of(values)
    cross_context, cross_totals = attend_forward(
        cross_queries, cross_keys, cross_values, segment, False
    )
    cross_exact = cross_context
    cross_context = cross_context.reshape(length, -1).astype(jnp.bfloat16)
    crossed = scatter_rows(
        project(cross_context, cross_output).astype(jnp.bfloat16)
    ) + cross_output_bias.astype(jnp.float32)
    second_part, second_back = jax.vjp(
        normalize,
        first + crossed,
        second_gain.astype(jnp.float32),
        second_shift.astype(jnp.float32),
    )
    second = gather_rows(second_part.astype(jnp.bfloat16)).astype(second_part.dtype)
    second_low = second.astype(jnp.bfloat16)
    inner = project(second_low, inner_weight) + inner_bias.astype(jnp.float32)
    hidden = jax.nn.gelu(inner, approximate=False).astype(jnp.bfloat16)
    outer = sum_pair(project(hidden, outer_weight).astype(jnp.bfloat16)) + outer_bias.astype(
        jnp.float32
    )
    result, third_back = jax.vjp(
        normalize, second + outer, third_gain.astype(jnp.float32), third_shift.astype(jnp.float32)
    )
    output = result.astype(jnp.bfloat16)
    grad_third, grad_third_gain, grad_third_shift = third_back(cotangent.astype(jnp.float32))
    grad_outer = grad_third.astype(jnp.bfloat16)
    grad_outer_bias = column_sums(grad_outer)
    gelu_back = jax.vjp(partial(jax.nn.gelu, approximate=False), inner)[1]
    grad_inner = gelu_back(project(grad_outer, outer_weight.T))[0].astype(jnp.bfloat16)
    grad_inner_weight = project(second_low.T, grad_inner)
    grad_inner_bias = column_sums(grad_inner)
    grad_second = rows_of(grad_third) + scatter_rows(
        project(grad_inner, inner_weight.T).astype(jnp.bfloat16)
    )
    grad_second_in, grad_second_gain, grad_second_shift = second_back(grad_second)
    grad_cross_rows = grad_second_in.astype(jnp.bfloat16)
    grad_cross = gather_rows(grad_cross_rows)
    grad_cross_output_bias = column_sums(grad_cross)
    grad_cross_context = heads_of(project(grad_cross, cross_output.T).astype(jnp.bfloat16))
    cross_grad_q, cross_grad_k, cross_grad_v = attend_backward(
        cross_queries,
        cross_keys,
        cross_values,
        grad_cross_context,
        cross_totals,
        segment,
        False,
        cross_exact,
    )
    cross_grad_q = (cross_grad_q.astype(jnp.bfloat16) * scale).reshape(length, -1)
    cross_grad_k = cross_grad_k.astype(jnp.bfloat16).reshape(length, -1)
    cross_grad_v = cross_grad_v.astype(jnp.bfloat16).reshape(length, -1)
    grad_cross_query = project(first_low.T, cross_grad_q)
    grad_cross_query_bias = column_sums(cross_grad_q)
    grad_cross_key = project(memory.T, cross_grad_k)
    grad_cross_value = project(memory.T, cross_grad_v)
    grad_cross_value_bias = column_sums(cross_grad_v)
    memory_term = project(cross_grad_k, cross_key.T) + project(cross_grad_v, cross_value.T)
    grad_first = grad_second_in + scatter_rows(
        project(cross_grad_q, cross_query.T).astype(jnp.bfloat16)
    )
    grad_cross_output_t = project(grad_cross.T, cross_context)
    cross = [grad_cross_query, grad_cross_key, grad_cross_value, grad_cross_output_t]
    cross_joined = jnp.concatenate(cross, 1).astype(jnp.bfloat16)
    cross_joined, grad_first = lax.optimization_barrier((cross_joined, grad_first))
    grad_first_in, grad_first_gain, grad_first_shift = first_back(grad_first)
    grad_self_rows = grad_first_in.astype(jnp.bfloat16)
    grad_self = gather_rows(grad_self_rows)
    grad_self_output_bias = column_sums(grad_self)
    grad_self_context = heads_of(project(grad_self, self_output.T).astype(jnp.bfloat16))
    dp_size = lax.axis_size("dp")
    self_grad_q, self_grad_k, self_grad_v = attend_backward(
        self_queries,
        self_keys,
        self_values,
        grad_self_context,
        self_totals,
        segment,
        True,
        self_exact,
    )
    self_grad_q = (self_grad_q.astype(jnp.bfloat16) * scale).reshape(length, -1)
    self_grad_k = self_grad_k.astype(jnp.bfloat16).reshape(length, -1)
    self_grad_v = self_grad_v.astype(jnp.bfloat16).reshape(length, -1)
    grad_self_query = project(tokens.T, self_grad_q)
    grad_self_query_bias = column_sums(self_grad_q)
    grad_self_key = project(tokens.T, self_grad_k)
    grad_self_value = project(tokens.T, self_grad_v)
    grad_self_value_bias = column_sums(self_grad_v)
    tokens_term = (
        project(self_grad_q, self_query.T)
        + project(self_grad_k, self_key.T)
        + project(self_grad_v, self_value.T)
    )
    tokens_part = scatter_rows(tokens_term.astype(jnp.bfloat16))
    memory_part = scatter_rows(memory_term.astype(jnp.bfloat16))
    grad_tokens = tokens_part + grad_first_in
    grad_self_output_t = project(grad_self.T, self_context)
    grad_outer_weight_t = project(grad_outer.T, hidden)

    def split_columns(summed, pieces, flipped):
        parts = []
        offset = 0
        for position, piece in enumerate(pieces):
            width = piece.shape[1]
            part = summed[:, offset : offset + width]
            offset += width
            if position in flipped:
                part = part.T
            parts.append(part)
        return parts

    def exchange_sum(joined, extra=None):
        rows = joined.shape[0] // dp_size
        blocks = joined.reshape(dp_size, rows, joined.shape[1])
        if extra is not None:
            blocks = jnp.concatenate(
                [blocks, jnp.broadcast_to(extra[None], (dp_size,) + extra.shape)], 1
            )
        received = lax.all_to_all(blocks, "dp", 0, 0, tiled=True)
        return jnp.sum(received.astype(jnp.float32), 0)

    ffn = [grad_inner_weight, grad_outer_weight_t]
    ffn_sum = lax.psum_scatter(
        jnp.concatenate(ffn, 1).astype(jnp.bfloat16), "dp", scatter_dimension=0, tiled=True
    ).astype(jnp.float32)
    ffn_sums = split_columns(ffn_sum, ffn, (1,))
    cross_sums = split_columns(exchange_sum(cross_joined), cross, (3,))
    late = [grad_self_query, grad_self_key, grad_self_value, grad_self_output_t]
    late_joined = jnp.concatenate(late, 1).astype(jnp.bfloat16)
    norm_pairs = sum_pair(
        jnp.concatenate([grad_first_gain, grad_first_shift, grad_second_gain, grad_second_shift])
    )
    width = late_joined.shape[1]
    sections = norm_pairs.shape[0] // 4
    biases = [
        grad_self_query_bias,
        grad_self_value_bias,
        grad_self_output_bias,
        grad_cross_query_bias,
        grad_cross_value_bias,
        grad_cross_output_bias,
        norm_pairs[:sections],
        norm_pairs[sections : 2 * sections],
        norm_pairs[2 * sections : 3 * sections],
        norm_pairs[3 * sections :],
        grad_third_gain,
        grad_third_shift,
        grad_inner_bias,
        grad_outer_bias,
    ]
    lines = []
    current = []
    used = 0
    places = []
    for bias in biases:
        chunks = []
        for begin in range(0, bias.shape[0], width):
            chunk = bias[begin : begin + width]
            if used + chunk.shape[0] > width:
                if used < width:
                    current.append(jnp.zeros((width - used,), jnp.float32))
                lines.append(jnp.concatenate(current))
                current = []
                used = 0
            chunks.append((len(lines), used, chunk.shape[0]))
            current.append(chunk)
            used += chunk.shape[0]
        places.append(chunks)
    if used < width:
        current.append(jnp.zeros((width - used,), jnp.float32))
    lines.append(jnp.concatenate(current))
    padded = jnp.stack(lines)
    count = padded.shape[0]
    high = padded.astype(jnp.bfloat16)
    low = (padded - high.astype(jnp.float32)).astype(jnp.bfloat16)
    late_rows = late_joined.shape[0] // dp_size
    late_total = exchange_sum(late_joined, jnp.concatenate([high, low], 0))
    self_sums = split_columns(late_total[:late_rows], late, (3,))
    summed_lines = late_total[late_rows : late_rows + count] + late_total[late_rows + count :]
    smalls = []
    for chunks in places:
        smalls.append(
            jnp.concatenate(
                [summed_lines[line, begin : begin + size] for line, begin, size in chunks]
            )
        )
    return (
        output,
        grad_tokens,
        memory_part,
        self_sums[0],
        smalls[0],
        self_sums[1],
        self_sums[2],
        smalls[1],
        self_sums[3],
        smalls[2],
        cross_sums[0],
        smalls[3],
        cross_sums[1],
        cross_sums[2],
        smalls[4],
        cross_sums[3],
        smalls[5],
        smalls[6],
        smalls[7],
        smalls[8],
        smalls[9],
        smalls[10],
        smalls[11],
        ffn_sums[0],
        smalls[12],
        ffn_sums[1],
        smalls[13],
    )


def solution(mesh):
    return jax.shard_map(
        on_device,
        mesh=mesh,
        in_specs=(
            P("dp", None),
            P("dp", None),
            P("dp"),
            P("dp", None),
            P(None, "tensor"),
            P("tensor"),
            P(None, "tensor"),
            P(None, "tensor"),
            P("tensor"),
            P("tensor", None),
            P(),
            P(None, "tensor"),
            P("tensor"),
            P(None, "tensor"),
            P(None, "tensor"),
            P("tensor"),
            P("tensor", None),
            P(),
            P(),
            P(),
            P(),
            P(),
            P(),
            P(),
            P(None, "tensor"),
            P("tensor"),
            P("tensor", None),
            P(),
        ),
        out_specs=(
            P("dp", None),
            P(("dp", "tensor"), None),
            P(("dp", "tensor"), None),
            P("dp", "tensor"),
            P("tensor"),
            P("dp", "tensor"),
            P("dp", "tensor"),
            P("tensor"),
            P("tensor", "dp"),
            P(),
            P("dp", "tensor"),
            P("tensor"),
            P("dp", "tensor"),
            P("dp", "tensor"),
            P("tensor"),
            P("tensor", "dp"),
            P(),
            P(),
            P(),
            P(),
            P(),
            P(),
            P(),
            P("dp", "tensor"),
            P("tensor"),
            P("tensor", "dp"),
            P(),
        ),
        check_vma=False,
    )
```

```python
from functools import partial

import jax
import jax.numpy as jnp
from jax import lax
from jax.sharding import Mesh, PartitionSpec as P
import numpy as np

DP = ("outer", "inner")

HD = 64


EPSILON = 1e-05
NEGATIVE = -1e30


def normalize(hidden, gain, shift):
    center = hidden - jnp.mean(hidden, -1, keepdims=True)
    spread = jnp.mean(center * center, -1, keepdims=True)
    return center * lax.rsqrt(spread + EPSILON) * gain + shift


def project(data, weight):
    return jnp.dot(data, weight, preferred_element_type=jnp.float32)


def column_sums(values):
    return jnp.sum(values.astype(jnp.float32), 0)


def heads_of(matrix):
    return matrix.reshape(matrix.shape[0], -1, HD)


def allowed_pairs(query_segment, key_segment, start, causal):
    same = query_segment[:, None] == key_segment[None, :]
    if causal:
        query_place = start + jnp.arange(query_segment.shape[0], dtype=jnp.int32)
        key_place = jnp.arange(key_segment.shape[0], dtype=jnp.int32)
        same = same & (key_place[None, :] <= query_place[:, None])
    return same[None]


def attend_forward(queries, keys, values, segment, causal):
    length = queries.shape[0]
    block_rows = min(256 if causal else 512, length)
    contexts = []
    totals = []
    for index in range(length // block_rows):
        start = index * block_rows
        end = start + block_rows if causal else length
        piece = queries[start : start + block_rows]
        scores = jnp.einsum(
            "qhe,khe->hqk", piece, keys[:end], preferred_element_type=jnp.float32
        )
        scores = jnp.where(
            allowed_pairs(segment[start : start + block_rows], segment[:end], start, causal),
            scores,
            NEGATIVE,
        )
        highest = jnp.max(scores, -1, keepdims=True)
        powers = jnp.exp(scores - highest)
        summed = jnp.sum(powers, -1, keepdims=True)
        weights = (powers / summed).astype(jnp.bfloat16)
        contexts.append(
            jnp.einsum("hqk,khe->qhe", weights, values[:end], preferred_element_type=jnp.float32)
        )
        totals.append(highest + jnp.log(summed))
    return (jnp.concatenate(contexts, 0), jnp.concatenate(totals, 1))


def attend_backward(queries, keys, values, grad_context, totals, segment, causal, exact_context):
    length = queries.shape[0]
    block_rows = min(256 if causal else 512, length)
    inner = jnp.einsum(
        "qhe,qhe->hq", grad_context.astype(jnp.float32), exact_context
    )[..., None]
    grad_queries = []
    grad_keys = jnp.zeros(keys.shape, jnp.float32)
    grad_values = jnp.zeros(values.shape, jnp.float32)
    for index in range(length // block_rows):
        start = index * block_rows
        end = start + block_rows if causal else length
        piece = queries[start : start + block_rows]
        grad_piece = grad_context[start : start + block_rows]
        near_keys = keys[:end]
        scores = jnp.einsum("qhe,khe->hqk", piece, near_keys, preferred_element_type=jnp.float32)
        scores = jnp.where(
            allowed_pairs(segment[start : start + block_rows], segment[:end], start, causal),
            scores,
            NEGATIVE,
        )
        probs = jnp.exp(scores - totals[:, start : start + block_rows])
        grad_probs = jnp.einsum(
            "qhe,khe->hqk", grad_piece, values[:end], preferred_element_type=jnp.float32
        )
        row_inner = inner[:, start : start + block_rows]
        grad_scores = (probs * (grad_probs - row_inner)).astype(jnp.bfloat16)
        grad_queries.append(
            jnp.einsum("hqk,khe->qhe", grad_scores, near_keys, preferred_element_type=jnp.float32)
        )
        grad_keys = grad_keys.at[:end].add(
            jnp.einsum("hqk,qhe->khe", grad_scores, piece, preferred_element_type=jnp.float32)
        )
        grad_values = grad_values.at[:end].add(
            jnp.einsum(
                "hqk,qhe->khe",
                probs.astype(jnp.bfloat16),
                grad_piece,
                preferred_element_type=jnp.float32,
            )
        )
    return (jnp.concatenate(grad_queries, 0), grad_keys, grad_values)


def on_device(
    tokens,
    memory,
    segment,
    cotangent,
    self_query,
    self_query_bias,
    self_key,
    self_value,
    self_value_bias,
    self_output,
    self_output_bias,
    cross_query,
    cross_query_bias,
    cross_key,
    cross_value,
    cross_value_bias,
    cross_output,
    cross_output_bias,
    first_gain,
    first_shift,
    second_gain,
    second_shift,
    third_gain,
    third_shift,
    inner_weight,
    inner_bias,
    outer_weight,
    outer_bias,
):
    scale = HD ** (-0.5)
    length = tokens.shape[0]
    groups = lax.axis_size("tensor")
    member = lax.axis_index("tensor")
    half = length // groups

    def rows_of(values):
        return lax.dynamic_slice_in_dim(values, member * half, half, 0)

    def spread_out(values):
        whole = jnp.zeros((values.shape[0] * groups,), jnp.float32)
        return lax.dynamic_update_slice_in_dim(whole, values, member * values.shape[0], 0)

    def own_share(values, count):
        return lax.dynamic_slice_in_dim(values, member * count, count, 0)

    def swap(values):
        return lax.ppermute(values, "tensor", [(0, 1), (1, 0)])

    def gather_rows(values):
        if groups != 2:
            return lax.all_gather(values, "tensor", axis=0, tiled=True)
        other = swap(values)
        lead = member == 0
        return jnp.concatenate(
            [jnp.where(lead, values, other), jnp.where(lead, other, values)], 0
        )

    def scatter_rows(values):
        if groups != 2:
            return lax.psum_scatter(
                values, "tensor", scatter_dimension=0, tiled=True
            ).astype(jnp.float32)
        top = values[:half]
        bottom = values[half:]
        lead = member == 0
        keep = jnp.where(lead, top, bottom)
        send = jnp.where(lead, bottom, top)
        return keep.astype(jnp.float32) + swap(send).astype(jnp.float32)

    def sum_pair(values):
        if groups != 2:
            return lax.psum(values, "tensor").astype(jnp.float32)
        return values.astype(jnp.float32) + swap(values).astype(jnp.float32)

    queries = ((project(tokens, self_query) + self_query_bias.astype(jnp.float32)) * scale).astype(
        jnp.bfloat16
    )
    keys = project(tokens, self_key).astype(jnp.bfloat16)
    values = (project(tokens, self_value) + self_value_bias.astype(jnp.float32)).astype(
        jnp.bfloat16
    )
    self_queries = heads_of(queries)
    self_keys = heads_of(keys)
    self_values = heads_of(values)
    self_context, self_totals = attend_forward(self_queries, self_keys, self_values, segment, True)
    self_exact = self_context
    self_context = self_context.reshape(length, -1).astype(jnp.bfloat16)
    attended = scatter_rows(project(self_context, self_output)) + self_output_bias.astype(
        jnp.float32
    )
    first, first_back = jax.vjp(
        normalize,
        rows_of(tokens).astype(jnp.float32) + attended,
        first_gain.astype(jnp.float32),
        first_shift.astype(jnp.float32),
    )
    first_low = gather_rows(first.astype(jnp.bfloat16))
    queries = (
        (project(first_low, cross_query) + cross_query_bias.astype(jnp.float32)) * scale
    ).astype(jnp.bfloat16)
    keys = project(memory, cross_key).astype(jnp.bfloat16)
    values = (project(memory, cross_value) + cross_value_bias.astype(jnp.float32)).astype(
        jnp.bfloat16
    )
    cross_queries = heads_of(queries)
    cross_keys = heads_of(keys)
    cross_values = heads_of(values)
    cross_context, cross_totals = attend_forward(
        cross_queries, cross_keys, cross_values, segment, False
    )
    cross_exact = cross_context
    cross_context = cross_context.reshape(length, -1).astype(jnp.bfloat16)
    crossed = scatter_rows(
        project(cross_context, cross_output).astype(jnp.bfloat16)
    ) + cross_output_bias.astype(jnp.float32)
    second_part, second_back = jax.vjp(
        normalize,
        first + crossed,
        second_gain.astype(jnp.float32),
        second_shift.astype(jnp.float32),
    )
    second = gather_rows(second_part.astype(jnp.bfloat16)).astype(second_part.dtype)
    second_low = second.astype(jnp.bfloat16)
    inner = project(second_low, inner_weight) + inner_bias.astype(jnp.float32)
    hidden = jax.nn.gelu(inner, approximate=False).astype(jnp.bfloat16)
    outer = sum_pair(project(hidden, outer_weight).astype(jnp.bfloat16)) + outer_bias.astype(
        jnp.float32
    )
    result, third_back = jax.vjp(
        normalize, second + outer, third_gain.astype(jnp.float32), third_shift.astype(jnp.float32)
    )
    output = result.astype(jnp.bfloat16)
    grad_third, grad_third_gain, grad_third_shift = third_back(cotangent.astype(jnp.float32))
    grad_outer = grad_third.astype(jnp.bfloat16)
    grad_outer_bias = column_sums(grad_outer)
    gelu_back = jax.vjp(partial(jax.nn.gelu, approximate=False), inner)[1]
    grad_inner = gelu_back(project(grad_outer, outer_weight.T))[0].astype(jnp.bfloat16)
    grad_inner_weight = project(second_low.T, grad_inner)
    grad_inner_bias = column_sums(grad_inner)
    grad_second = rows_of(grad_third) + scatter_rows(
        project(grad_inner, inner_weight.T).astype(jnp.bfloat16)
    )
    grad_second_in, grad_second_gain, grad_second_shift = second_back(grad_second)
    grad_cross_rows = grad_second_in.astype(jnp.bfloat16)
    grad_cross = gather_rows(grad_cross_rows)
    grad_cross_output_bias = column_sums(grad_cross)
    grad_cross_context = heads_of(project(grad_cross, cross_output.T).astype(jnp.bfloat16))
    cross_grad_q, cross_grad_k, cross_grad_v = attend_backward(
        cross_queries,
        cross_keys,
        cross_values,
        grad_cross_context,
        cross_totals,
        segment,
        False,
        cross_exact,
    )
    cross_grad_q = (cross_grad_q.astype(jnp.bfloat16) * scale).reshape(length, -1)
    cross_grad_k = cross_grad_k.astype(jnp.bfloat16).reshape(length, -1)
    cross_grad_v = cross_grad_v.astype(jnp.bfloat16).reshape(length, -1)
    grad_cross_query = project(first_low.T, cross_grad_q)
    grad_cross_query_bias = column_sums(cross_grad_q)
    grad_cross_key = project(memory.T, cross_grad_k)
    grad_cross_value = project(memory.T, cross_grad_v)
    grad_cross_value_bias = column_sums(cross_grad_v)
    memory_term = project(cross_grad_k, cross_key.T) + project(cross_grad_v, cross_value.T)
    grad_first = grad_second_in + scatter_rows(
        project(cross_grad_q, cross_query.T).astype(jnp.bfloat16)
    )
    grad_cross_output_t = project(grad_cross.T, cross_context)
    cross = [grad_cross_query, grad_cross_key, grad_cross_value, grad_cross_output_t]
    cross_joined = jnp.concatenate(cross, 1).astype(jnp.bfloat16)
    cross_joined, grad_first = lax.optimization_barrier((cross_joined, grad_first))
    grad_first_in, grad_first_gain, grad_first_shift = first_back(grad_first)
    grad_self_rows = grad_first_in.astype(jnp.bfloat16)
    grad_self = gather_rows(grad_self_rows)
    grad_self_output_bias = column_sums(grad_self)
    grad_self_context = heads_of(project(grad_self, self_output.T).astype(jnp.bfloat16))
    outer_size = lax.axis_size("outer")
    inner_size = lax.axis_size("inner")
    dp_size = outer_size * inner_size
    self_grad_q, self_grad_k, self_grad_v = attend_backward(
        self_queries,
        self_keys,
        self_values,
        grad_self_context,
        self_totals,
        segment,
        True,
        self_exact,
    )
    self_grad_q = (self_grad_q.astype(jnp.bfloat16) * scale).reshape(length, -1)
    self_grad_k = self_grad_k.astype(jnp.bfloat16).reshape(length, -1)
    self_grad_v = self_grad_v.astype(jnp.bfloat16).reshape(length, -1)
    grad_self_query = project(tokens.T, self_grad_q)
    grad_self_query_bias = column_sums(self_grad_q)
    grad_self_key = project(tokens.T, self_grad_k)
    grad_self_value = project(tokens.T, self_grad_v)
    grad_self_value_bias = column_sums(self_grad_v)
    tokens_term = (
        project(self_grad_q, self_query.T)
        + project(self_grad_k, self_key.T)
        + project(self_grad_v, self_value.T)
    )
    tokens_part = scatter_rows(tokens_term.astype(jnp.bfloat16))
    memory_part = scatter_rows(memory_term.astype(jnp.bfloat16))
    grad_tokens = tokens_part + grad_first_in
    grad_self_output_t = project(grad_self.T, self_context)
    grad_outer_weight_t = project(grad_outer.T, hidden)

    def split_columns(summed, pieces, flipped):
        parts = []
        offset = 0
        for position, piece in enumerate(pieces):
            width = piece.shape[1]
            part = summed[:, offset : offset + width]
            offset += width
            if position in flipped:
                part = part.T
            parts.append(part)
        return parts

    def exchange_sum(joined, extra=None):
        rows = joined.shape[0] // dp_size
        blocks = joined.reshape(dp_size, rows, joined.shape[1])
        if extra is not None:
            blocks = jnp.concatenate(
                [blocks, jnp.broadcast_to(extra[None], (dp_size,) + extra.shape)], 1
            )
        if inner_size == 1 or outer_size == 1:
            received = lax.all_to_all(blocks, DP, 0, 0, tiled=True)
            return jnp.sum(received.astype(jnp.float32), 0)
        staged = blocks.reshape((outer_size, inner_size) + blocks.shape[1:])
        first = lax.all_to_all(staged, "inner", 1, 1, tiled=True)
        partial = jnp.sum(first.astype(jnp.float32), 1)
        middle = partial.astype(jnp.bfloat16)
        if extra is not None:
            lines = extra.shape[0] // 2
            merged = partial[:, rows : rows + lines] + partial[:, rows + lines :]
            high = merged.astype(jnp.bfloat16)
            low = (merged - high.astype(jnp.float32)).astype(jnp.bfloat16)
            middle = jnp.concatenate([middle[:, :rows], high, low], 1)
        second = lax.all_to_all(middle, "outer", 0, 0, tiled=True)
        return jnp.sum(second.astype(jnp.float32), 0)

    ffn = [grad_inner_weight, grad_outer_weight_t]
    ffn_sum = lax.psum_scatter(
        jnp.concatenate(ffn, 1).astype(jnp.bfloat16), DP, scatter_dimension=0, tiled=True
    ).astype(jnp.float32)
    ffn_sums = split_columns(ffn_sum, ffn, (1,))
    cross_sums = split_columns(exchange_sum(cross_joined), cross, (3,))
    late = [grad_self_query, grad_self_key, grad_self_value, grad_self_output_t]
    late_joined = jnp.concatenate(late, 1).astype(jnp.bfloat16)
    norm_pairs = sum_pair(
        jnp.concatenate([grad_first_gain, grad_first_shift, grad_second_gain, grad_second_shift])
    )
    width = late_joined.shape[1]
    sections = norm_pairs.shape[0] // 4
    biases = [
        grad_self_query_bias,
        grad_self_value_bias,
        grad_self_output_bias,
        grad_cross_query_bias,
        grad_cross_value_bias,
        grad_cross_output_bias,
        norm_pairs[:sections],
        norm_pairs[sections : 2 * sections],
        norm_pairs[2 * sections : 3 * sections],
        norm_pairs[3 * sections :],
        grad_third_gain,
        grad_third_shift,
        grad_inner_bias,
        grad_outer_bias,
    ]
    lines = []
    current = []
    used = 0
    places = []
    for bias in biases:
        chunks = []
        for begin in range(0, bias.shape[0], width):
            chunk = bias[begin : begin + width]
            if used + chunk.shape[0] > width:
                if used < width:
                    current.append(jnp.zeros((width - used,), jnp.float32))
                lines.append(jnp.concatenate(current))
                current = []
                used = 0
            chunks.append((len(lines), used, chunk.shape[0]))
            current.append(chunk)
            used += chunk.shape[0]
        places.append(chunks)
    if used < width:
        current.append(jnp.zeros((width - used,), jnp.float32))
    lines.append(jnp.concatenate(current))
    padded = jnp.stack(lines)
    count = padded.shape[0]
    high = padded.astype(jnp.bfloat16)
    low = (padded - high.astype(jnp.float32)).astype(jnp.bfloat16)
    late_rows = late_joined.shape[0] // dp_size
    late_total = exchange_sum(late_joined, jnp.concatenate([high, low], 0))
    self_sums = split_columns(late_total[:late_rows], late, (3,))
    summed_lines = late_total[late_rows : late_rows + count] + late_total[late_rows + count :]
    smalls = []
    for chunks in places:
        smalls.append(
            jnp.concatenate(
                [summed_lines[line, begin : begin + size] for line, begin, size in chunks]
            )
        )
    return (
        output,
        grad_tokens,
        memory_part,
        self_sums[0],
        smalls[0],
        self_sums[1],
        self_sums[2],
        smalls[1],
        self_sums[3],
        smalls[2],
        cross_sums[0],
        smalls[3],
        cross_sums[1],
        cross_sums[2],
        smalls[4],
        cross_sums[3],
        smalls[5],
        smalls[6],
        smalls[7],
        smalls[8],
        smalls[9],
        smalls[10],
        smalls[11],
        ffn_sums[0],
        smalls[12],
        ffn_sums[1],
        smalls[13],
    )


def solution(mesh):
    dp_size = mesh.shape["dp"]
    inner = 4 if dp_size % 4 == 0 and dp_size > 4 else 1
    devices = np.asarray(mesh.devices).reshape(dp_size // inner, inner, mesh.shape["tensor"])
    staged = Mesh(devices, ("outer", "inner", "tensor"))
    return jax.shard_map(
        on_device,
        mesh=staged,
        in_specs=(
            P(DP, None),
            P(DP, None),
            P(DP),
            P(DP, None),
            P(None, "tensor"),
            P("tensor"),
            P(None, "tensor"),
            P(None, "tensor"),
            P("tensor"),
            P("tensor", None),
            P(),
            P(None, "tensor"),
            P("tensor"),
            P(None, "tensor"),
            P(None, "tensor"),
            P("tensor"),
            P("tensor", None),
            P(),
            P(),
            P(),
            P(),
            P(),
            P(),
            P(),
            P(None, "tensor"),
            P("tensor"),
            P("tensor", None),
            P(),
        ),
        out_specs=(
            P(DP, None),
            P(("outer", "inner", "tensor"), None),
            P(("outer", "inner", "tensor"), None),
            P(DP, "tensor"),
            P("tensor"),
            P(DP, "tensor"),
            P(DP, "tensor"),
            P("tensor"),
            P("tensor", DP),
            P(),
            P(DP, "tensor"),
            P("tensor"),
            P(DP, "tensor"),
            P(DP, "tensor"),
            P("tensor"),
            P("tensor", DP),
            P(),
            P(),
            P(),
            P(),
            P(),
            P(),
            P(),
            P(DP, "tensor"),
            P("tensor"),
            P("tensor", DP),
            P(),
        ),
        check_vma=False,
    )
```

```python
from functools import partial

import jax
import jax.numpy as jnp
from jax import lax
from jax.sharding import Mesh, PartitionSpec as P
import numpy as np

DP = ("outer", "inner")

HD = 64


EPSILON = 1e-05
NEGATIVE = -1e30


def normalize(hidden, gain, shift):
    center = hidden - jnp.mean(hidden, -1, keepdims=True)
    spread = jnp.mean(center * center, -1, keepdims=True)
    return center * lax.rsqrt(spread + EPSILON) * gain + shift


def project(data, weight):
    return jnp.dot(data, weight, preferred_element_type=jnp.float32)


def column_sums(values):
    return jnp.sum(values.astype(jnp.float32), 0)


def heads_of(matrix):
    return matrix.reshape(matrix.shape[0], -1, HD)


def allowed_pairs(query_segment, key_segment, start, causal):
    same = query_segment[:, None] == key_segment[None, :]
    if causal:
        query_place = start + jnp.arange(query_segment.shape[0], dtype=jnp.int32)
        key_place = jnp.arange(key_segment.shape[0], dtype=jnp.int32)
        same = same & (key_place[None, :] <= query_place[:, None])
    return same[None]


def attend_forward(queries, keys, values, segment, causal):
    length = queries.shape[0]
    block_rows = min(256 if causal else 512, length)
    contexts = []
    totals = []
    for index in range(length // block_rows):
        start = index * block_rows
        end = start + block_rows if causal else length
        piece = queries[start : start + block_rows]
        scores = jnp.einsum(
            "qhe,khe->hqk", piece, keys[:end], preferred_element_type=jnp.float32
        )
        scores = jnp.where(
            allowed_pairs(segment[start : start + block_rows], segment[:end], start, causal),
            scores,
            NEGATIVE,
        )
        highest = jnp.max(scores, -1, keepdims=True)
        powers = jnp.exp(scores - highest)
        summed = jnp.sum(powers, -1, keepdims=True)
        weights = (powers / summed).astype(jnp.bfloat16)
        contexts.append(
            jnp.einsum("hqk,khe->qhe", weights, values[:end], preferred_element_type=jnp.float32)
        )
        totals.append(highest + jnp.log(summed))
    return (jnp.concatenate(contexts, 0), jnp.concatenate(totals, 1))


def attend_backward(queries, keys, values, grad_context, totals, segment, causal, exact_context):
    length = queries.shape[0]
    block_rows = min(256 if causal else 512, length)
    inner = jnp.einsum(
        "qhe,qhe->hq", grad_context.astype(jnp.float32), exact_context
    )[..., None]
    grad_queries = []
    grad_keys = jnp.zeros(keys.shape, jnp.float32)
    grad_values = jnp.zeros(values.shape, jnp.float32)
    for index in range(length // block_rows):
        start = index * block_rows
        end = start + block_rows if causal else length
        piece = queries[start : start + block_rows]
        grad_piece = grad_context[start : start + block_rows]
        near_keys = keys[:end]
        scores = jnp.einsum("qhe,khe->hqk", piece, near_keys, preferred_element_type=jnp.float32)
        scores = jnp.where(
            allowed_pairs(segment[start : start + block_rows], segment[:end], start, causal),
            scores,
            NEGATIVE,
        )
        probs = jnp.exp(scores - totals[:, start : start + block_rows])
        grad_probs = jnp.einsum(
            "qhe,khe->hqk", grad_piece, values[:end], preferred_element_type=jnp.float32
        )
        row_inner = inner[:, start : start + block_rows]
        grad_scores = (probs * (grad_probs - row_inner)).astype(jnp.bfloat16)
        grad_queries.append(
            jnp.einsum("hqk,khe->qhe", grad_scores, near_keys, preferred_element_type=jnp.float32)
        )
        grad_keys = grad_keys.at[:end].add(
            jnp.einsum("hqk,qhe->khe", grad_scores, piece, preferred_element_type=jnp.float32)
        )
        grad_values = grad_values.at[:end].add(
            jnp.einsum(
                "hqk,qhe->khe",
                probs.astype(jnp.bfloat16),
                grad_piece,
                preferred_element_type=jnp.float32,
            )
        )
    return (jnp.concatenate(grad_queries, 0), grad_keys, grad_values)


def on_device(
    tokens,
    memory,
    segment,
    cotangent,
    self_query,
    self_query_bias,
    self_key,
    self_value,
    self_value_bias,
    self_output,
    self_output_bias,
    cross_query,
    cross_query_bias,
    cross_key,
    cross_value,
    cross_value_bias,
    cross_output,
    cross_output_bias,
    first_gain,
    first_shift,
    second_gain,
    second_shift,
    third_gain,
    third_shift,
    inner_weight,
    inner_bias,
    outer_weight,
    outer_bias,
):
    scale = HD ** (-0.5)
    length = tokens.shape[0]
    groups = lax.axis_size("tensor")
    member = lax.axis_index("tensor")
    half = length // groups

    def rows_of(values):
        return lax.dynamic_slice_in_dim(values, member * half, half, 0)

    def spread_out(values):
        whole = jnp.zeros((values.shape[0] * groups,), jnp.float32)
        return lax.dynamic_update_slice_in_dim(whole, values, member * values.shape[0], 0)

    def own_share(values, count):
        return lax.dynamic_slice_in_dim(values, member * count, count, 0)

    def swap(values):
        return lax.ppermute(values, "tensor", [(0, 1), (1, 0)])

    def gather_rows(values):
        if groups != 2:
            return lax.all_gather(values, "tensor", axis=0, tiled=True)
        other = swap(values)
        lead = member == 0
        return jnp.concatenate(
            [jnp.where(lead, values, other), jnp.where(lead, other, values)], 0
        )

    def scatter_rows(values):
        if groups != 2:
            return lax.psum_scatter(
                values, "tensor", scatter_dimension=0, tiled=True
            ).astype(jnp.float32)
        top = values[:half]
        bottom = values[half:]
        lead = member == 0
        keep = jnp.where(lead, top, bottom)
        send = jnp.where(lead, bottom, top)
        return keep.astype(jnp.float32) + swap(send).astype(jnp.float32)

    def sum_pair(values):
        if groups != 2:
            return lax.psum(values, "tensor").astype(jnp.float32)
        return values.astype(jnp.float32) + swap(values).astype(jnp.float32)

    queries = ((project(tokens, self_query) + self_query_bias.astype(jnp.float32)) * scale).astype(
        jnp.bfloat16
    )
    keys = project(tokens, self_key).astype(jnp.bfloat16)
    values = (project(tokens, self_value) + self_value_bias.astype(jnp.float32)).astype(
        jnp.bfloat16
    )
    self_queries = heads_of(queries)
    self_keys = heads_of(keys)
    self_values = heads_of(values)
    self_context, self_totals = attend_forward(self_queries, self_keys, self_values, segment, True)
    self_exact = self_context
    self_context = self_context.reshape(length, -1).astype(jnp.bfloat16)
    attended = scatter_rows(project(self_context, self_output)) + self_output_bias.astype(
        jnp.float32
    )
    first, first_back = jax.vjp(
        normalize,
        rows_of(tokens).astype(jnp.float32) + attended,
        first_gain.astype(jnp.float32),
        first_shift.astype(jnp.float32),
    )
    first_low = gather_rows(first.astype(jnp.bfloat16))
    queries = (
        (project(first_low, cross_query) + cross_query_bias.astype(jnp.float32)) * scale
    ).astype(jnp.bfloat16)
    keys = project(memory, cross_key).astype(jnp.bfloat16)
    values = (project(memory, cross_value) + cross_value_bias.astype(jnp.float32)).astype(
        jnp.bfloat16
    )
    cross_queries = heads_of(queries)
    cross_keys = heads_of(keys)
    cross_values = heads_of(values)
    cross_context, cross_totals = attend_forward(
        cross_queries, cross_keys, cross_values, segment, False
    )
    cross_exact = cross_context
    cross_context = cross_context.reshape(length, -1).astype(jnp.bfloat16)
    crossed = scatter_rows(
        project(cross_context, cross_output).astype(jnp.bfloat16)
    ) + cross_output_bias.astype(jnp.float32)
    second_part, second_back = jax.vjp(
        normalize,
        first + crossed,
        second_gain.astype(jnp.float32),
        second_shift.astype(jnp.float32),
    )
    second = gather_rows(second_part.astype(jnp.bfloat16)).astype(second_part.dtype)
    second_low = second.astype(jnp.bfloat16)
    inner = project(second_low, inner_weight) + inner_bias.astype(jnp.float32)
    hidden = jax.nn.gelu(inner, approximate=False).astype(jnp.bfloat16)
    outer = sum_pair(project(hidden, outer_weight).astype(jnp.bfloat16)) + outer_bias.astype(
        jnp.float32
    )
    result, third_back = jax.vjp(
        normalize, second + outer, third_gain.astype(jnp.float32), third_shift.astype(jnp.float32)
    )
    output = result.astype(jnp.bfloat16)
    grad_third, grad_third_gain, grad_third_shift = third_back(cotangent.astype(jnp.float32))
    grad_outer = grad_third.astype(jnp.bfloat16)
    grad_outer_bias = column_sums(grad_outer)
    gelu_back = jax.vjp(partial(jax.nn.gelu, approximate=False), inner)[1]
    grad_inner = gelu_back(project(grad_outer, outer_weight.T))[0].astype(jnp.bfloat16)
    grad_inner_weight = project(second_low.T, grad_inner)
    grad_inner_bias = column_sums(grad_inner)
    grad_second = rows_of(grad_third) + scatter_rows(
        project(grad_inner, inner_weight.T).astype(jnp.bfloat16)
    )
    grad_second_in, grad_second_gain, grad_second_shift = second_back(grad_second)
    grad_cross_rows = grad_second_in.astype(jnp.bfloat16)
    grad_cross = gather_rows(grad_cross_rows)
    grad_cross_output_bias = column_sums(grad_cross)
    grad_cross_context = heads_of(project(grad_cross, cross_output.T).astype(jnp.bfloat16))
    cross_grad_q, cross_grad_k, cross_grad_v = attend_backward(
        cross_queries,
        cross_keys,
        cross_values,
        grad_cross_context,
        cross_totals,
        segment,
        False,
        cross_exact,
    )
    cross_grad_q = (cross_grad_q.astype(jnp.bfloat16) * scale).reshape(length, -1)
    cross_grad_k = cross_grad_k.astype(jnp.bfloat16).reshape(length, -1)
    cross_grad_v = cross_grad_v.astype(jnp.bfloat16).reshape(length, -1)
    grad_cross_query = project(first_low.T, cross_grad_q)
    grad_cross_query_bias = column_sums(cross_grad_q)
    grad_cross_key = project(memory.T, cross_grad_k)
    grad_cross_value = project(memory.T, cross_grad_v)
    grad_cross_value_bias = column_sums(cross_grad_v)
    memory_term = project(cross_grad_k, cross_key.T) + project(cross_grad_v, cross_value.T)
    grad_first = grad_second_in + scatter_rows(
        project(cross_grad_q, cross_query.T).astype(jnp.bfloat16)
    )
    grad_cross_output_t = project(grad_cross.T, cross_context)
    cross = [grad_cross_query, grad_cross_key, grad_cross_value, grad_cross_output_t]
    cross_joined = jnp.concatenate(cross, 1).astype(jnp.bfloat16)
    cross_joined, grad_first = lax.optimization_barrier((cross_joined, grad_first))
    grad_first_in, grad_first_gain, grad_first_shift = first_back(grad_first)
    grad_self_rows = grad_first_in.astype(jnp.bfloat16)
    grad_self = gather_rows(grad_self_rows)
    grad_self_output_bias = column_sums(grad_self)
    grad_self_context = heads_of(project(grad_self, self_output.T).astype(jnp.bfloat16))
    outer_size = lax.axis_size("outer")
    inner_size = lax.axis_size("inner")
    dp_size = outer_size * inner_size
    self_grad_q, self_grad_k, self_grad_v = attend_backward(
        self_queries,
        self_keys,
        self_values,
        grad_self_context,
        self_totals,
        segment,
        True,
        self_exact,
    )
    self_grad_q = (self_grad_q.astype(jnp.bfloat16) * scale).reshape(length, -1)
    self_grad_k = self_grad_k.astype(jnp.bfloat16).reshape(length, -1)
    self_grad_v = self_grad_v.astype(jnp.bfloat16).reshape(length, -1)
    grad_self_query = project(tokens.T, self_grad_q)
    grad_self_query_bias = column_sums(self_grad_q)
    grad_self_key = project(tokens.T, self_grad_k)
    grad_self_value = project(tokens.T, self_grad_v)
    grad_self_value_bias = column_sums(self_grad_v)
    tokens_term = (
        project(self_grad_q, self_query.T)
        + project(self_grad_k, self_key.T)
        + project(self_grad_v, self_value.T)
    )
    tokens_part = scatter_rows(tokens_term.astype(jnp.bfloat16))
    memory_part = scatter_rows(memory_term.astype(jnp.bfloat16))
    grad_tokens = tokens_part + grad_first_in
    grad_self_output_t = project(grad_self.T, self_context)
    grad_outer_weight_t = project(grad_outer.T, hidden)

    def split_columns(summed, pieces, flipped):
        parts = []
        offset = 0
        for position, piece in enumerate(pieces):
            width = piece.shape[1]
            part = summed[:, offset : offset + width]
            offset += width
            if position in flipped:
                part = part.T
            parts.append(part)
        return parts

    def exchange_sum(joined, extra=None):
        rows = joined.shape[0] // dp_size
        width = joined.shape[1]
        blocks = joined.reshape(dp_size, rows, width)
        if inner_size == 1 or outer_size == 1:
            if extra is not None:
                blocks = jnp.concatenate(
                    [blocks, jnp.broadcast_to(extra[None], (dp_size,) + extra.shape)], 1
                )
            received = lax.all_to_all(blocks, DP, 0, 0, tiled=True)
            return jnp.sum(received.astype(jnp.float32), 0)
        staged = blocks.reshape(outer_size, inner_size, rows, width)
        staged = jnp.swapaxes(staged, 0, 1).reshape(inner_size, outer_size * rows, width)
        if extra is not None:
            staged = jnp.concatenate(
                [staged, jnp.broadcast_to(extra[None], (inner_size,) + extra.shape)], 1
            )
        first = lax.all_to_all(staged, "inner", 0, 0, tiled=True)
        partial = jnp.sum(first.astype(jnp.float32), 0)
        middle = partial[: outer_size * rows].astype(jnp.bfloat16).reshape(
            outer_size, rows, width
        )
        if extra is not None:
            lines = extra.shape[0] // 2
            tail = partial[outer_size * rows :]
            merged = tail[:lines] + tail[lines:]
            high = merged.astype(jnp.bfloat16)
            low = (merged - high.astype(jnp.float32)).astype(jnp.bfloat16)
            pair = jnp.concatenate([high, low], 0)
            middle = jnp.concatenate(
                [middle, jnp.broadcast_to(pair[None], (outer_size,) + pair.shape)], 1
            )
        second = lax.all_to_all(middle, "outer", 0, 0, tiled=True)
        return jnp.sum(second.astype(jnp.float32), 0)

    ffn = [grad_inner_weight, grad_outer_weight_t]
    ffn_sum = lax.psum_scatter(
        jnp.concatenate(ffn, 1).astype(jnp.bfloat16), DP, scatter_dimension=0, tiled=True
    ).astype(jnp.float32)
    ffn_sums = split_columns(ffn_sum, ffn, (1,))
    cross_sums = split_columns(exchange_sum(cross_joined), cross, (3,))
    late = [grad_self_query, grad_self_key, grad_self_value, grad_self_output_t]
    late_joined = jnp.concatenate(late, 1).astype(jnp.bfloat16)
    norm_pairs = sum_pair(
        jnp.concatenate([grad_first_gain, grad_first_shift, grad_second_gain, grad_second_shift])
    )
    width = late_joined.shape[1]
    sections = norm_pairs.shape[0] // 4
    biases = [
        grad_self_query_bias,
        grad_self_value_bias,
        grad_self_output_bias,
        grad_cross_query_bias,
        grad_cross_value_bias,
        grad_cross_output_bias,
        norm_pairs[:sections],
        norm_pairs[sections : 2 * sections],
        norm_pairs[2 * sections : 3 * sections],
        norm_pairs[3 * sections :],
        grad_third_gain,
        grad_third_shift,
        grad_inner_bias,
        grad_outer_bias,
    ]
    lines = []
    current = []
    used = 0
    places = []
    for bias in biases:
        chunks = []
        for begin in range(0, bias.shape[0], width):
            chunk = bias[begin : begin + width]
            if used + chunk.shape[0] > width:
                if used < width:
                    current.append(jnp.zeros((width - used,), jnp.float32))
                lines.append(jnp.concatenate(current))
                current = []
                used = 0
            chunks.append((len(lines), used, chunk.shape[0]))
            current.append(chunk)
            used += chunk.shape[0]
        places.append(chunks)
    if used < width:
        current.append(jnp.zeros((width - used,), jnp.float32))
    lines.append(jnp.concatenate(current))
    padded = jnp.stack(lines)
    count = padded.shape[0]
    high = padded.astype(jnp.bfloat16)
    low = (padded - high.astype(jnp.float32)).astype(jnp.bfloat16)
    late_rows = late_joined.shape[0] // dp_size
    late_total = exchange_sum(late_joined, jnp.concatenate([high, low], 0))
    self_sums = split_columns(late_total[:late_rows], late, (3,))
    summed_lines = late_total[late_rows : late_rows + count] + late_total[late_rows + count :]
    smalls = []
    for chunks in places:
        smalls.append(
            jnp.concatenate(
                [summed_lines[line, begin : begin + size] for line, begin, size in chunks]
            )
        )
    return (
        output,
        grad_tokens,
        memory_part,
        self_sums[0],
        smalls[0],
        self_sums[1],
        self_sums[2],
        smalls[1],
        self_sums[3],
        smalls[2],
        cross_sums[0],
        smalls[3],
        cross_sums[1],
        cross_sums[2],
        smalls[4],
        cross_sums[3],
        smalls[5],
        smalls[6],
        smalls[7],
        smalls[8],
        smalls[9],
        smalls[10],
        smalls[11],
        ffn_sums[0],
        smalls[12],
        ffn_sums[1],
        smalls[13],
    )


def solution(mesh):
    dp_size = mesh.shape["dp"]
    inner = 4 if dp_size % 4 == 0 and dp_size > 4 else 1
    devices = np.asarray(mesh.devices).reshape(dp_size // inner, inner, mesh.shape["tensor"])
    staged = Mesh(devices, ("outer", "inner", "tensor"))
    return jax.shard_map(
        on_device,
        mesh=staged,
        in_specs=(
            P(DP, None),
            P(DP, None),
            P(DP),
            P(DP, None),
            P(None, "tensor"),
            P("tensor"),
            P(None, "tensor"),
            P(None, "tensor"),
            P("tensor"),
            P("tensor", None),
            P(),
            P(None, "tensor"),
            P("tensor"),
            P(None, "tensor"),
            P(None, "tensor"),
            P("tensor"),
            P("tensor", None),
            P(),
            P(),
            P(),
            P(),
            P(),
            P(),
            P(),
            P(None, "tensor"),
            P("tensor"),
            P("tensor", None),
            P(),
        ),
        out_specs=(
            P(DP, None),
            P(("outer", "inner", "tensor"), None),
            P(("outer", "inner", "tensor"), None),
            P(DP, "tensor"),
            P("tensor"),
            P(DP, "tensor"),
            P(DP, "tensor"),
            P("tensor"),
            P("tensor", DP),
            P(),
            P(DP, "tensor"),
            P("tensor"),
            P(DP, "tensor"),
            P(DP, "tensor"),
            P("tensor"),
            P("tensor", DP),
            P(),
            P(),
            P(),
            P(),
            P(),
            P(),
            P(),
            P(DP, "tensor"),
            P("tensor"),
            P("tensor", DP),
            P(),
        ),
        check_vma=False,
    )
```

```python
from functools import partial

import jax
import jax.numpy as jnp
from jax import lax
from jax.sharding import Mesh, PartitionSpec as P
import numpy as np

DP = ("outer", "inner")

HD = 64


EPSILON = 1e-05
NEGATIVE = -1e30


def normalize(hidden, gain, shift):
    center = hidden - jnp.mean(hidden, -1, keepdims=True)
    spread = jnp.mean(center * center, -1, keepdims=True)
    return center * lax.rsqrt(spread + EPSILON) * gain + shift


def project(data, weight):
    return jnp.dot(data, weight, preferred_element_type=jnp.float32)


def column_sums(values):
    return jnp.sum(values.astype(jnp.float32), 0)


def heads_of(matrix):
    return matrix.reshape(matrix.shape[0], -1, HD)


def allowed_pairs(query_segment, key_segment, start, causal):
    same = query_segment[:, None] == key_segment[None, :]
    if causal:
        query_place = start + jnp.arange(query_segment.shape[0], dtype=jnp.int32)
        key_place = jnp.arange(key_segment.shape[0], dtype=jnp.int32)
        same = same & (key_place[None, :] <= query_place[:, None])
    return same[None]


def attend_forward(queries, keys, values, segment, causal):
    length = queries.shape[0]
    block_rows = min(256 if causal else 512, length)
    contexts = []
    totals = []
    for index in range(length // block_rows):
        start = index * block_rows
        end = start + block_rows if causal else length
        piece = queries[start : start + block_rows]
        scores = jnp.einsum(
            "qhe,khe->hqk", piece, keys[:end], preferred_element_type=jnp.float32
        )
        scores = jnp.where(
            allowed_pairs(segment[start : start + block_rows], segment[:end], start, causal),
            scores,
            NEGATIVE,
        )
        highest = jnp.max(scores, -1, keepdims=True)
        powers = jnp.exp(scores - highest)
        summed = jnp.sum(powers, -1, keepdims=True)
        weights = (powers / summed).astype(jnp.bfloat16)
        contexts.append(
            jnp.einsum("hqk,khe->qhe", weights, values[:end], preferred_element_type=jnp.float32)
        )
        totals.append(highest + jnp.log(summed))
    return (jnp.concatenate(contexts, 0), jnp.concatenate(totals, 1))


def attend_backward(queries, keys, values, grad_context, totals, segment, causal, exact_context):
    length = queries.shape[0]
    block_rows = min(256 if causal else 512, length)
    inner = jnp.einsum(
        "qhe,qhe->hq", grad_context.astype(jnp.float32), exact_context
    )[..., None]
    grad_queries = []
    grad_keys = jnp.zeros(keys.shape, jnp.float32)
    grad_values = jnp.zeros(values.shape, jnp.float32)
    for index in range(length // block_rows):
        start = index * block_rows
        end = start + block_rows if causal else length
        piece = queries[start : start + block_rows]
        grad_piece = grad_context[start : start + block_rows]
        near_keys = keys[:end]
        scores = jnp.einsum("qhe,khe->hqk", piece, near_keys, preferred_element_type=jnp.float32)
        scores = jnp.where(
            allowed_pairs(segment[start : start + block_rows], segment[:end], start, causal),
            scores,
            NEGATIVE,
        )
        probs = jnp.exp(scores - totals[:, start : start + block_rows])
        grad_probs = jnp.einsum(
            "qhe,khe->hqk", grad_piece, values[:end], preferred_element_type=jnp.float32
        )
        row_inner = inner[:, start : start + block_rows]
        grad_scores = (probs * (grad_probs - row_inner)).astype(jnp.bfloat16)
        grad_queries.append(
            jnp.einsum("hqk,khe->qhe", grad_scores, near_keys, preferred_element_type=jnp.float32)
        )
        grad_keys = grad_keys.at[:end].add(
            jnp.einsum("hqk,qhe->khe", grad_scores, piece, preferred_element_type=jnp.float32)
        )
        grad_values = grad_values.at[:end].add(
            jnp.einsum(
                "hqk,qhe->khe",
                probs.astype(jnp.bfloat16),
                grad_piece,
                preferred_element_type=jnp.float32,
            )
        )
    return (jnp.concatenate(grad_queries, 0), grad_keys, grad_values)


def on_device(
    tokens,
    memory,
    segment,
    cotangent,
    self_query,
    self_query_bias,
    self_key,
    self_value,
    self_value_bias,
    self_output,
    self_output_bias,
    cross_query,
    cross_query_bias,
    cross_key,
    cross_value,
    cross_value_bias,
    cross_output,
    cross_output_bias,
    first_gain,
    first_shift,
    second_gain,
    second_shift,
    third_gain,
    third_shift,
    inner_weight,
    inner_bias,
    outer_weight,
    outer_bias,
):
    scale = HD ** (-0.5)
    length = tokens.shape[0]
    groups = lax.axis_size("tensor")
    member = lax.axis_index("tensor")
    half = length // groups

    def rows_of(values):
        return lax.dynamic_slice_in_dim(values, member * half, half, 0)

    def spread_out(values):
        whole = jnp.zeros((values.shape[0] * groups,), jnp.float32)
        return lax.dynamic_update_slice_in_dim(whole, values, member * values.shape[0], 0)

    def own_share(values, count):
        return lax.dynamic_slice_in_dim(values, member * count, count, 0)

    def swap(values):
        return lax.ppermute(values, "tensor", [(0, 1), (1, 0)])

    def gather_rows(values):
        if groups != 2:
            return lax.all_gather(values, "tensor", axis=0, tiled=True)
        other = swap(values)
        lead = member == 0
        return jnp.concatenate(
            [jnp.where(lead, values, other), jnp.where(lead, other, values)], 0
        )

    def scatter_rows(values):
        if groups != 2:
            return lax.psum_scatter(
                values, "tensor", scatter_dimension=0, tiled=True
            ).astype(jnp.float32)
        top = values[:half]
        bottom = values[half:]
        lead = member == 0
        keep = jnp.where(lead, top, bottom)
        send = jnp.where(lead, bottom, top)
        return keep.astype(jnp.float32) + swap(send).astype(jnp.float32)

    def sum_pair(values):
        if groups != 2:
            return lax.psum(values, "tensor").astype(jnp.float32)
        return values.astype(jnp.float32) + swap(values).astype(jnp.float32)

    queries = ((project(tokens, self_query) + self_query_bias.astype(jnp.float32)) * scale).astype(
        jnp.bfloat16
    )
    keys = project(tokens, self_key).astype(jnp.bfloat16)
    values = (project(tokens, self_value) + self_value_bias.astype(jnp.float32)).astype(
        jnp.bfloat16
    )
    self_queries = heads_of(queries)
    self_keys = heads_of(keys)
    self_values = heads_of(values)
    self_context, self_totals = attend_forward(self_queries, self_keys, self_values, segment, True)
    self_exact = self_context
    self_context = self_context.reshape(length, -1).astype(jnp.bfloat16)
    attended = scatter_rows(project(self_context, self_output)) + self_output_bias.astype(
        jnp.float32
    )
    first, first_back = jax.vjp(
        normalize,
        rows_of(tokens).astype(jnp.float32) + attended,
        first_gain.astype(jnp.float32),
        first_shift.astype(jnp.float32),
    )
    first_low = gather_rows(first.astype(jnp.bfloat16))
    queries = (
        (project(first_low, cross_query) + cross_query_bias.astype(jnp.float32)) * scale
    ).astype(jnp.bfloat16)
    keys = project(memory, cross_key).astype(jnp.bfloat16)
    values = (project(memory, cross_value) + cross_value_bias.astype(jnp.float32)).astype(
        jnp.bfloat16
    )
    cross_queries = heads_of(queries)
    cross_keys = heads_of(keys)
    cross_values = heads_of(values)
    cross_context, cross_totals = attend_forward(
        cross_queries, cross_keys, cross_values, segment, False
    )
    cross_exact = cross_context
    cross_context = cross_context.reshape(length, -1).astype(jnp.bfloat16)
    crossed = scatter_rows(
        project(cross_context, cross_output).astype(jnp.bfloat16)
    ) + cross_output_bias.astype(jnp.float32)
    second_part, second_back = jax.vjp(
        normalize,
        first + crossed,
        second_gain.astype(jnp.float32),
        second_shift.astype(jnp.float32),
    )
    second = gather_rows(second_part.astype(jnp.bfloat16)).astype(second_part.dtype)
    second_low = second.astype(jnp.bfloat16)
    inner = project(second_low, inner_weight) + inner_bias.astype(jnp.float32)
    hidden = jax.nn.gelu(inner, approximate=False).astype(jnp.bfloat16)
    outer = sum_pair(project(hidden, outer_weight).astype(jnp.bfloat16)) + outer_bias.astype(
        jnp.float32
    )
    result, third_back = jax.vjp(
        normalize, second + outer, third_gain.astype(jnp.float32), third_shift.astype(jnp.float32)
    )
    output = result.astype(jnp.bfloat16)
    grad_third, grad_third_gain, grad_third_shift = third_back(cotangent.astype(jnp.float32))
    grad_outer = grad_third.astype(jnp.bfloat16)
    grad_outer_bias = column_sums(grad_outer)
    gelu_back = jax.vjp(partial(jax.nn.gelu, approximate=False), inner)[1]
    grad_inner = gelu_back(project(grad_outer, outer_weight.T))[0].astype(jnp.bfloat16)
    grad_inner_weight = project(second_low.T, grad_inner)
    grad_inner_bias = column_sums(grad_inner)
    grad_second = rows_of(grad_third) + scatter_rows(
        project(grad_inner, inner_weight.T).astype(jnp.bfloat16)
    )
    grad_second_in, grad_second_gain, grad_second_shift = second_back(grad_second)
    grad_cross_rows = grad_second_in.astype(jnp.bfloat16)
    grad_cross = gather_rows(grad_cross_rows)
    grad_cross_output_bias = column_sums(grad_cross)
    grad_cross_context = heads_of(project(grad_cross, cross_output.T).astype(jnp.bfloat16))
    cross_grad_q, cross_grad_k, cross_grad_v = attend_backward(
        cross_queries,
        cross_keys,
        cross_values,
        grad_cross_context,
        cross_totals,
        segment,
        False,
        cross_exact,
    )
    cross_grad_q = (cross_grad_q.astype(jnp.bfloat16) * scale).reshape(length, -1)
    cross_grad_k = cross_grad_k.astype(jnp.bfloat16).reshape(length, -1)
    cross_grad_v = cross_grad_v.astype(jnp.bfloat16).reshape(length, -1)
    grad_cross_query = project(first_low.T, cross_grad_q)
    grad_cross_query_bias = column_sums(cross_grad_q)
    grad_cross_key = project(memory.T, cross_grad_k)
    grad_cross_value = project(memory.T, cross_grad_v)
    grad_cross_value_bias = column_sums(cross_grad_v)
    memory_term = project(cross_grad_k, cross_key.T) + project(cross_grad_v, cross_value.T)
    grad_first = grad_second_in + scatter_rows(
        project(cross_grad_q, cross_query.T).astype(jnp.bfloat16)
    )
    grad_cross_output_t = project(grad_cross.T, cross_context)
    cross = [grad_cross_query, grad_cross_key, grad_cross_value, grad_cross_output_t]
    cross_joined = jnp.concatenate(cross, 1).astype(jnp.bfloat16)
    cross_joined, grad_first = lax.optimization_barrier((cross_joined, grad_first))
    grad_first_in, grad_first_gain, grad_first_shift = first_back(grad_first)
    grad_self_rows = grad_first_in.astype(jnp.bfloat16)
    grad_self = gather_rows(grad_self_rows)
    grad_self_output_bias = column_sums(grad_self)
    grad_self_context = heads_of(project(grad_self, self_output.T).astype(jnp.bfloat16))
    outer_size = lax.axis_size("outer")
    inner_size = lax.axis_size("inner")
    dp_size = outer_size * inner_size
    self_grad_q, self_grad_k, self_grad_v = attend_backward(
        self_queries,
        self_keys,
        self_values,
        grad_self_context,
        self_totals,
        segment,
        True,
        self_exact,
    )
    self_grad_q = (self_grad_q.astype(jnp.bfloat16) * scale).reshape(length, -1)
    self_grad_k = self_grad_k.astype(jnp.bfloat16).reshape(length, -1)
    self_grad_v = self_grad_v.astype(jnp.bfloat16).reshape(length, -1)
    grad_self_query = project(tokens.T, self_grad_q)
    grad_self_query_bias = column_sums(self_grad_q)
    grad_self_key = project(tokens.T, self_grad_k)
    grad_self_value = project(tokens.T, self_grad_v)
    grad_self_value_bias = column_sums(self_grad_v)
    tokens_term = (
        project(self_grad_q, self_query.T)
        + project(self_grad_k, self_key.T)
        + project(self_grad_v, self_value.T)
    )
    tokens_part = scatter_rows(tokens_term.astype(jnp.bfloat16))
    memory_part = scatter_rows(memory_term.astype(jnp.bfloat16))
    grad_tokens = tokens_part + grad_first_in
    grad_self_output_t = project(grad_self.T, self_context)
    grad_outer_weight_t = project(grad_outer.T, hidden)

    def split_columns(summed, pieces, flipped):
        parts = []
        offset = 0
        for position, piece in enumerate(pieces):
            width = piece.shape[1]
            part = summed[:, offset : offset + width]
            offset += width
            if position in flipped:
                part = part.T
            parts.append(part)
        return parts

    def exchange_sum(joined, extra=None):
        rows = joined.shape[0] // dp_size
        width = joined.shape[1]
        blocks = joined.reshape(dp_size, rows, width)
        if inner_size == 1 or outer_size == 1:
            if extra is not None:
                blocks = jnp.concatenate(
                    [blocks, jnp.broadcast_to(extra[None], (dp_size,) + extra.shape)], 1
                )
            received = lax.all_to_all(blocks, DP, 0, 0, tiled=True)
            return jnp.sum(received.astype(jnp.float32), 0)
        staged = blocks.reshape(outer_size, inner_size, rows, width)
        staged = jnp.swapaxes(staged, 0, 1).reshape(inner_size, outer_size * rows, width)
        if extra is not None:
            staged = jnp.concatenate(
                [staged, jnp.broadcast_to(extra[None], (inner_size,) + extra.shape)], 1
            )
        first = lax.all_to_all(staged, "inner", 0, 0, tiled=True)
        partial = jnp.sum(first.astype(jnp.float32), 0)
        middle = partial[: outer_size * rows].astype(jnp.bfloat16).reshape(
            outer_size, rows, width
        )
        if extra is not None:
            lines = extra.shape[0] // 2
            tail = partial[outer_size * rows :]
            merged = tail[:lines] + tail[lines:]
            high = merged.astype(jnp.bfloat16)
            low = (merged - high.astype(jnp.float32)).astype(jnp.bfloat16)
            pair = jnp.concatenate([high, low], 0)
            middle = jnp.concatenate(
                [middle, jnp.broadcast_to(pair[None], (outer_size,) + pair.shape)], 1
            )
        if outer_size > 4:
            second = lax.all_to_all(middle, "outer", 0, 0, tiled=True)
            return jnp.sum(second.astype(jnp.float32), 0)
        place = lax.axis_index("outer")
        by_source = [None] * outer_size
        for shift in range(outer_size):
            piece = lax.dynamic_index_in_dim(
                middle, (place + shift) % outer_size, 0, keepdims=False
            )
            if shift:
                piece = lax.ppermute(
                    piece,
                    "outer",
                    [(peer, (peer + shift) % outer_size) for peer in range(outer_size)],
                )
            by_source[shift] = piece
        total = None
        for source in range(outer_size):
            chosen = by_source[0]
            for shift in range(1, outer_size):
                chosen = jnp.where(
                    (place - shift) % outer_size == source, by_source[shift], chosen
                )
            chosen = chosen.astype(jnp.float32)
            total = chosen if total is None else total + chosen
        return total

    ffn = [grad_inner_weight, grad_outer_weight_t]
    ffn_sum = lax.psum_scatter(
        jnp.concatenate(ffn, 1).astype(jnp.bfloat16), DP, scatter_dimension=0, tiled=True
    ).astype(jnp.float32)
    ffn_sums = split_columns(ffn_sum, ffn, (1,))
    cross_sums = split_columns(exchange_sum(cross_joined), cross, (3,))
    late = [grad_self_query, grad_self_key, grad_self_value, grad_self_output_t]
    late_joined = jnp.concatenate(late, 1).astype(jnp.bfloat16)
    norm_pairs = sum_pair(
        jnp.concatenate([grad_first_gain, grad_first_shift, grad_second_gain, grad_second_shift])
    )
    width = late_joined.shape[1]
    sections = norm_pairs.shape[0] // 4
    biases = [
        grad_self_query_bias,
        grad_self_value_bias,
        grad_self_output_bias,
        grad_cross_query_bias,
        grad_cross_value_bias,
        grad_cross_output_bias,
        norm_pairs[:sections],
        norm_pairs[sections : 2 * sections],
        norm_pairs[2 * sections : 3 * sections],
        norm_pairs[3 * sections :],
        grad_third_gain,
        grad_third_shift,
        grad_inner_bias,
        grad_outer_bias,
    ]
    lines = []
    current = []
    used = 0
    places = []
    for bias in biases:
        chunks = []
        for begin in range(0, bias.shape[0], width):
            chunk = bias[begin : begin + width]
            if used + chunk.shape[0] > width:
                if used < width:
                    current.append(jnp.zeros((width - used,), jnp.float32))
                lines.append(jnp.concatenate(current))
                current = []
                used = 0
            chunks.append((len(lines), used, chunk.shape[0]))
            current.append(chunk)
            used += chunk.shape[0]
        places.append(chunks)
    if used < width:
        current.append(jnp.zeros((width - used,), jnp.float32))
    lines.append(jnp.concatenate(current))
    padded = jnp.stack(lines)
    count = padded.shape[0]
    high = padded.astype(jnp.bfloat16)
    low = (padded - high.astype(jnp.float32)).astype(jnp.bfloat16)
    late_rows = late_joined.shape[0] // dp_size
    late_total = exchange_sum(late_joined, jnp.concatenate([high, low], 0))
    self_sums = split_columns(late_total[:late_rows], late, (3,))
    summed_lines = late_total[late_rows : late_rows + count] + late_total[late_rows + count :]
    smalls = []
    for chunks in places:
        smalls.append(
            jnp.concatenate(
                [summed_lines[line, begin : begin + size] for line, begin, size in chunks]
            )
        )
    return (
        output,
        grad_tokens,
        memory_part,
        self_sums[0],
        smalls[0],
        self_sums[1],
        self_sums[2],
        smalls[1],
        self_sums[3],
        smalls[2],
        cross_sums[0],
        smalls[3],
        cross_sums[1],
        cross_sums[2],
        smalls[4],
        cross_sums[3],
        smalls[5],
        smalls[6],
        smalls[7],
        smalls[8],
        smalls[9],
        smalls[10],
        smalls[11],
        ffn_sums[0],
        smalls[12],
        ffn_sums[1],
        smalls[13],
    )


def solution(mesh):
    dp_size = mesh.shape["dp"]
    inner = 4 if dp_size % 4 == 0 and dp_size > 4 else 1
    devices = np.asarray(mesh.devices).reshape(dp_size // inner, inner, mesh.shape["tensor"])
    staged = Mesh(devices, ("outer", "inner", "tensor"))
    return jax.shard_map(
        on_device,
        mesh=staged,
        in_specs=(
            P(DP, None),
            P(DP, None),
            P(DP),
            P(DP, None),
            P(None, "tensor"),
            P("tensor"),
            P(None, "tensor"),
            P(None, "tensor"),
            P("tensor"),
            P("tensor", None),
            P(),
            P(None, "tensor"),
            P("tensor"),
            P(None, "tensor"),
            P(None, "tensor"),
            P("tensor"),
            P("tensor", None),
            P(),
            P(),
            P(),
            P(),
            P(),
            P(),
            P(),
            P(None, "tensor"),
            P("tensor"),
            P("tensor", None),
            P(),
        ),
        out_specs=(
            P(DP, None),
            P(("outer", "inner", "tensor"), None),
            P(("outer", "inner", "tensor"), None),
            P(DP, "tensor"),
            P("tensor"),
            P(DP, "tensor"),
            P(DP, "tensor"),
            P("tensor"),
            P("tensor", DP),
            P(),
            P(DP, "tensor"),
            P("tensor"),
            P(DP, "tensor"),
            P(DP, "tensor"),
            P("tensor"),
            P("tensor", DP),
            P(),
            P(),
            P(),
            P(),
            P(),
            P(),
            P(),
            P(DP, "tensor"),
            P("tensor"),
            P("tensor", DP),
            P(),
        ),
        check_vma=False,
    )
```

```python
from functools import partial

import jax
import jax.numpy as jnp
from jax import lax
from jax.sharding import Mesh, PartitionSpec as P
import numpy as np

DP = ("outer", "inner")

HD = 64


EPSILON = 1e-05
NEGATIVE = -1e30


def normalize(hidden, gain, shift):
    center = hidden - jnp.mean(hidden, -1, keepdims=True)
    spread = jnp.mean(center * center, -1, keepdims=True)
    return center * lax.rsqrt(spread + EPSILON) * gain + shift


def project(data, weight):
    return jnp.dot(data, weight, preferred_element_type=jnp.float32)


def column_sums(values):
    return jnp.sum(values.astype(jnp.float32), 0)


def heads_of(matrix):
    return matrix.reshape(matrix.shape[0], -1, HD)


def allowed_pairs(query_segment, key_segment, start, causal):
    same = query_segment[:, None] == key_segment[None, :]
    if causal:
        query_place = start + jnp.arange(query_segment.shape[0], dtype=jnp.int32)
        key_place = jnp.arange(key_segment.shape[0], dtype=jnp.int32)
        same = same & (key_place[None, :] <= query_place[:, None])
    return same[None]


def attend_forward(queries, keys, values, segment, causal):
    length = queries.shape[0]
    block_rows = min(256 if causal else 512, length)
    contexts = []
    totals = []
    for index in range(length // block_rows):
        start = index * block_rows
        end = start + block_rows if causal else length
        piece = queries[start : start + block_rows]
        scores = jnp.einsum(
            "qhe,khe->hqk", piece, keys[:end], preferred_element_type=jnp.float32
        )
        scores = jnp.where(
            allowed_pairs(segment[start : start + block_rows], segment[:end], start, causal),
            scores,
            NEGATIVE,
        )
        highest = jnp.max(scores, -1, keepdims=True)
        powers = jnp.exp(scores - highest)
        summed = jnp.sum(powers, -1, keepdims=True)
        weights = (powers / summed).astype(jnp.bfloat16)
        contexts.append(
            jnp.einsum("hqk,khe->qhe", weights, values[:end], preferred_element_type=jnp.float32)
        )
        totals.append(highest + jnp.log(summed))
    return (jnp.concatenate(contexts, 0), jnp.concatenate(totals, 1))


def attend_backward(queries, keys, values, grad_context, totals, segment, causal, exact_context):
    length = queries.shape[0]
    block_rows = min(256 if causal else 512, length)
    inner = jnp.einsum(
        "qhe,qhe->hq", grad_context.astype(jnp.float32), exact_context
    )[..., None]
    grad_queries = []
    grad_keys = jnp.zeros(keys.shape, jnp.float32)
    grad_values = jnp.zeros(values.shape, jnp.float32)
    for index in range(length // block_rows):
        start = index * block_rows
        end = start + block_rows if causal else length
        piece = queries[start : start + block_rows]
        grad_piece = grad_context[start : start + block_rows]
        near_keys = keys[:end]
        scores = jnp.einsum("qhe,khe->hqk", piece, near_keys, preferred_element_type=jnp.float32)
        scores = jnp.where(
            allowed_pairs(segment[start : start + block_rows], segment[:end], start, causal),
            scores,
            NEGATIVE,
        )
        probs = jnp.exp(scores - totals[:, start : start + block_rows])
        grad_probs = jnp.einsum(
            "qhe,khe->hqk", grad_piece, values[:end], preferred_element_type=jnp.float32
        )
        row_inner = inner[:, start : start + block_rows]
        grad_scores = (probs * (grad_probs - row_inner)).astype(jnp.bfloat16)
        grad_queries.append(
            jnp.einsum("hqk,khe->qhe", grad_scores, near_keys, preferred_element_type=jnp.float32)
        )
        grad_keys = grad_keys.at[:end].add(
            jnp.einsum("hqk,qhe->khe", grad_scores, piece, preferred_element_type=jnp.float32)
        )
        grad_values = grad_values.at[:end].add(
            jnp.einsum(
                "hqk,qhe->khe",
                probs.astype(jnp.bfloat16),
                grad_piece,
                preferred_element_type=jnp.float32,
            )
        )
    return (jnp.concatenate(grad_queries, 0), grad_keys, grad_values)


def on_device(
    tokens,
    memory,
    segment,
    cotangent,
    self_query,
    self_query_bias,
    self_key,
    self_value,
    self_value_bias,
    self_output,
    self_output_bias,
    cross_query,
    cross_query_bias,
    cross_key,
    cross_value,
    cross_value_bias,
    cross_output,
    cross_output_bias,
    first_gain,
    first_shift,
    second_gain,
    second_shift,
    third_gain,
    third_shift,
    inner_weight,
    inner_bias,
    outer_weight,
    outer_bias,
):
    scale = HD ** (-0.5)
    length = tokens.shape[0]
    groups = lax.axis_size("tensor")
    member = lax.axis_index("tensor")
    half = length // groups

    def rows_of(values):
        return lax.dynamic_slice_in_dim(values, member * half, half, 0)

    def spread_out(values):
        whole = jnp.zeros((values.shape[0] * groups,), jnp.float32)
        return lax.dynamic_update_slice_in_dim(whole, values, member * values.shape[0], 0)

    def own_share(values, count):
        return lax.dynamic_slice_in_dim(values, member * count, count, 0)

    def swap(values):
        return lax.ppermute(values, "tensor", [(0, 1), (1, 0)])

    def gather_rows(values):
        if groups != 2:
            return lax.all_gather(values, "tensor", axis=0, tiled=True)
        other = swap(values)
        lead = member == 0
        return jnp.concatenate(
            [jnp.where(lead, values, other), jnp.where(lead, other, values)], 0
        )

    def scatter_rows(values):
        if groups != 2:
            return lax.psum_scatter(
                values, "tensor", scatter_dimension=0, tiled=True
            ).astype(jnp.float32)
        top = values[:half]
        bottom = values[half:]
        lead = member == 0
        keep = jnp.where(lead, top, bottom)
        send = jnp.where(lead, bottom, top)
        return keep.astype(jnp.float32) + swap(send).astype(jnp.float32)

    def sum_pair(values):
        if groups != 2:
            return lax.psum(values, "tensor").astype(jnp.float32)
        return values.astype(jnp.float32) + swap(values).astype(jnp.float32)

    queries = ((project(tokens, self_query) + self_query_bias.astype(jnp.float32)) * scale).astype(
        jnp.bfloat16
    )
    keys = project(tokens, self_key).astype(jnp.bfloat16)
    values = (project(tokens, self_value) + self_value_bias.astype(jnp.float32)).astype(
        jnp.bfloat16
    )
    self_queries = heads_of(queries)
    self_keys = heads_of(keys)
    self_values = heads_of(values)
    self_context, self_totals = attend_forward(self_queries, self_keys, self_values, segment, True)
    self_exact = self_context
    self_context = self_context.reshape(length, -1).astype(jnp.bfloat16)
    attended = scatter_rows(project(self_context, self_output)) + self_output_bias.astype(
        jnp.float32
    )
    first, first_back = jax.vjp(
        normalize,
        rows_of(tokens).astype(jnp.float32) + attended,
        first_gain.astype(jnp.float32),
        first_shift.astype(jnp.float32),
    )
    first_low = gather_rows(first.astype(jnp.bfloat16))
    queries = (
        (project(first_low, cross_query) + cross_query_bias.astype(jnp.float32)) * scale
    ).astype(jnp.bfloat16)
    keys = project(memory, cross_key).astype(jnp.bfloat16)
    values = (project(memory, cross_value) + cross_value_bias.astype(jnp.float32)).astype(
        jnp.bfloat16
    )
    cross_queries = heads_of(queries)
    cross_keys = heads_of(keys)
    cross_values = heads_of(values)
    cross_context, cross_totals = attend_forward(
        cross_queries, cross_keys, cross_values, segment, False
    )
    cross_exact = cross_context
    cross_context = cross_context.reshape(length, -1).astype(jnp.bfloat16)
    crossed = scatter_rows(
        project(cross_context, cross_output).astype(jnp.bfloat16)
    ) + cross_output_bias.astype(jnp.float32)
    second_part, second_back = jax.vjp(
        normalize,
        first + crossed,
        second_gain.astype(jnp.float32),
        second_shift.astype(jnp.float32),
    )
    second = gather_rows(second_part.astype(jnp.bfloat16)).astype(second_part.dtype)
    second_low = second.astype(jnp.bfloat16)
    inner = project(second_low, inner_weight) + inner_bias.astype(jnp.float32)
    hidden = jax.nn.gelu(inner, approximate=False).astype(jnp.bfloat16)
    outer = sum_pair(project(hidden, outer_weight).astype(jnp.bfloat16)) + outer_bias.astype(
        jnp.float32
    )
    result, third_back = jax.vjp(
        normalize, second + outer, third_gain.astype(jnp.float32), third_shift.astype(jnp.float32)
    )
    output = result.astype(jnp.bfloat16)
    grad_third, grad_third_gain, grad_third_shift = third_back(cotangent.astype(jnp.float32))
    grad_outer = grad_third.astype(jnp.bfloat16)
    grad_outer_bias = column_sums(grad_outer)
    gelu_back = jax.vjp(partial(jax.nn.gelu, approximate=False), inner)[1]
    grad_inner = gelu_back(project(grad_outer, outer_weight.T))[0].astype(jnp.bfloat16)
    grad_inner_weight = project(second_low.T, grad_inner)
    grad_inner_bias = column_sums(grad_inner)
    grad_second = rows_of(grad_third) + scatter_rows(
        project(grad_inner, inner_weight.T).astype(jnp.bfloat16)
    )
    grad_second_in, grad_second_gain, grad_second_shift = second_back(grad_second)
    grad_cross_rows = grad_second_in.astype(jnp.bfloat16)
    grad_cross = gather_rows(grad_cross_rows)
    grad_cross_output_bias = column_sums(grad_cross)
    grad_cross_context = heads_of(project(grad_cross, cross_output.T).astype(jnp.bfloat16))
    cross_grad_q, cross_grad_k, cross_grad_v = attend_backward(
        cross_queries,
        cross_keys,
        cross_values,
        grad_cross_context,
        cross_totals,
        segment,
        False,
        cross_exact,
    )
    cross_grad_q = (cross_grad_q.astype(jnp.bfloat16) * scale).reshape(length, -1)
    cross_grad_k = cross_grad_k.astype(jnp.bfloat16).reshape(length, -1)
    cross_grad_v = cross_grad_v.astype(jnp.bfloat16).reshape(length, -1)
    grad_cross_query = project(first_low.T, cross_grad_q)
    grad_cross_query_bias = column_sums(cross_grad_q)
    grad_cross_key = project(memory.T, cross_grad_k)
    grad_cross_value = project(memory.T, cross_grad_v)
    grad_cross_value_bias = column_sums(cross_grad_v)
    memory_term = project(cross_grad_k, cross_key.T) + project(cross_grad_v, cross_value.T)
    grad_first = grad_second_in + scatter_rows(
        project(cross_grad_q, cross_query.T).astype(jnp.bfloat16)
    )
    grad_cross_output_t = project(grad_cross.T, cross_context)
    cross = [grad_cross_query, grad_cross_key, grad_cross_value, grad_cross_output_t]
    cross_joined = jnp.concatenate(cross, 1).astype(jnp.bfloat16)
    cross_joined, grad_first = lax.optimization_barrier((cross_joined, grad_first))
    grad_first_in, grad_first_gain, grad_first_shift = first_back(grad_first)
    grad_self_rows = grad_first_in.astype(jnp.bfloat16)
    grad_self = gather_rows(grad_self_rows)
    grad_self_output_bias = column_sums(grad_self)
    grad_self_context = heads_of(project(grad_self, self_output.T).astype(jnp.bfloat16))
    outer_size = lax.axis_size("outer")
    inner_size = lax.axis_size("inner")
    dp_size = outer_size * inner_size
    self_grad_q, self_grad_k, self_grad_v = attend_backward(
        self_queries,
        self_keys,
        self_values,
        grad_self_context,
        self_totals,
        segment,
        True,
        self_exact,
    )
    self_grad_q = (self_grad_q.astype(jnp.bfloat16) * scale).reshape(length, -1)
    self_grad_k = self_grad_k.astype(jnp.bfloat16).reshape(length, -1)
    self_grad_v = self_grad_v.astype(jnp.bfloat16).reshape(length, -1)
    grad_self_query = project(tokens.T, self_grad_q)
    grad_self_query_bias = column_sums(self_grad_q)
    grad_self_key = project(tokens.T, self_grad_k)
    grad_self_value = project(tokens.T, self_grad_v)
    grad_self_value_bias = column_sums(self_grad_v)
    tokens_term = (
        project(self_grad_q, self_query.T)
        + project(self_grad_k, self_key.T)
        + project(self_grad_v, self_value.T)
    )
    tokens_part = scatter_rows(tokens_term.astype(jnp.bfloat16))
    memory_part = scatter_rows(memory_term.astype(jnp.bfloat16))
    grad_tokens = tokens_part + grad_first_in
    grad_self_output_t = project(grad_self.T, self_context)
    grad_outer_weight_t = project(grad_outer.T, hidden)

    def split_columns(summed, pieces, flipped):
        parts = []
        offset = 0
        for position, piece in enumerate(pieces):
            width = piece.shape[1]
            part = summed[:, offset : offset + width]
            offset += width
            if position in flipped:
                part = part.T
            parts.append(part)
        return parts

    def exchange_sum(joined, extra=None):
        rows = joined.shape[0] // dp_size
        width = joined.shape[1]
        blocks = joined.reshape(dp_size, rows, width)
        if inner_size == 1 or outer_size == 1:
            if extra is not None:
                blocks = jnp.concatenate(
                    [blocks, jnp.broadcast_to(extra[None], (dp_size,) + extra.shape)], 1
                )
            received = lax.all_to_all(blocks, DP, 0, 0, tiled=True)
            return jnp.sum(received.astype(jnp.float32), 0)
        staged = blocks.reshape(outer_size, inner_size, rows, width)
        staged = jnp.swapaxes(staged, 0, 1).reshape(inner_size, outer_size * rows, width)
        if extra is not None:
            staged = jnp.concatenate(
                [staged, jnp.broadcast_to(extra[None], (inner_size,) + extra.shape)], 1
            )
        if inner_size == 4:
            spot = lax.axis_index("inner")
            swapped = []
            for mask in range(inner_size):
                piece = lax.dynamic_index_in_dim(staged, spot ^ mask, 0, keepdims=False)
                if mask:
                    piece = lax.ppermute(
                        piece, "inner", [(peer, peer ^ mask) for peer in range(inner_size)]
                    )
                swapped.append(piece)
            partial = None
            for source in range(inner_size):
                chosen = swapped[0]
                for mask in range(1, inner_size):
                    chosen = jnp.where(spot ^ mask == source, swapped[mask], chosen)
                chosen = chosen.astype(jnp.float32)
                partial = chosen if partial is None else partial + chosen
        else:
            first = lax.all_to_all(staged, "inner", 0, 0, tiled=True)
            partial = jnp.sum(first.astype(jnp.float32), 0)
        middle = partial[: outer_size * rows].astype(jnp.bfloat16).reshape(
            outer_size, rows, width
        )
        if extra is not None:
            lines = extra.shape[0] // 2
            tail = partial[outer_size * rows :]
            merged = tail[:lines] + tail[lines:]
            high = merged.astype(jnp.bfloat16)
            low = (merged - high.astype(jnp.float32)).astype(jnp.bfloat16)
            pair = jnp.concatenate([high, low], 0)
            middle = jnp.concatenate(
                [middle, jnp.broadcast_to(pair[None], (outer_size,) + pair.shape)], 1
            )
        if outer_size > 4:
            second = lax.all_to_all(middle, "outer", 0, 0, tiled=True)
            return jnp.sum(second.astype(jnp.float32), 0)
        place = lax.axis_index("outer")
        by_source = [None] * outer_size
        for shift in range(outer_size):
            piece = lax.dynamic_index_in_dim(
                middle, (place + shift) % outer_size, 0, keepdims=False
            )
            if shift:
                piece = lax.ppermute(
                    piece,
                    "outer",
                    [(peer, (peer + shift) % outer_size) for peer in range(outer_size)],
                )
            by_source[shift] = piece
        total = None
        for source in range(outer_size):
            chosen = by_source[0]
            for shift in range(1, outer_size):
                chosen = jnp.where(
                    (place - shift) % outer_size == source, by_source[shift], chosen
                )
            chosen = chosen.astype(jnp.float32)
            total = chosen if total is None else total + chosen
        return total

    ffn = [grad_inner_weight, grad_outer_weight_t]
    ffn_sum = lax.psum_scatter(
        jnp.concatenate(ffn, 1).astype(jnp.bfloat16), DP, scatter_dimension=0, tiled=True
    ).astype(jnp.float32)
    ffn_sums = split_columns(ffn_sum, ffn, (1,))
    cross_sums = split_columns(exchange_sum(cross_joined), cross, (3,))
    late = [grad_self_query, grad_self_key, grad_self_value, grad_self_output_t]
    late_joined = jnp.concatenate(late, 1).astype(jnp.bfloat16)
    norm_pairs = sum_pair(
        jnp.concatenate([grad_first_gain, grad_first_shift, grad_second_gain, grad_second_shift])
    )
    width = late_joined.shape[1]
    sections = norm_pairs.shape[0] // 4
    biases = [
        grad_self_query_bias,
        grad_self_value_bias,
        grad_self_output_bias,
        grad_cross_query_bias,
        grad_cross_value_bias,
        grad_cross_output_bias,
        norm_pairs[:sections],
        norm_pairs[sections : 2 * sections],
        norm_pairs[2 * sections : 3 * sections],
        norm_pairs[3 * sections :],
        grad_third_gain,
        grad_third_shift,
        grad_inner_bias,
        grad_outer_bias,
    ]
    lines = []
    current = []
    used = 0
    places = []
    for bias in biases:
        chunks = []
        for begin in range(0, bias.shape[0], width):
            chunk = bias[begin : begin + width]
            if used + chunk.shape[0] > width:
                if used < width:
                    current.append(jnp.zeros((width - used,), jnp.float32))
                lines.append(jnp.concatenate(current))
                current = []
                used = 0
            chunks.append((len(lines), used, chunk.shape[0]))
            current.append(chunk)
            used += chunk.shape[0]
        places.append(chunks)
    if used < width:
        current.append(jnp.zeros((width - used,), jnp.float32))
    lines.append(jnp.concatenate(current))
    padded = jnp.stack(lines)
    count = padded.shape[0]
    high = padded.astype(jnp.bfloat16)
    low = (padded - high.astype(jnp.float32)).astype(jnp.bfloat16)
    late_rows = late_joined.shape[0] // dp_size
    late_total = exchange_sum(late_joined, jnp.concatenate([high, low], 0))
    self_sums = split_columns(late_total[:late_rows], late, (3,))
    summed_lines = late_total[late_rows : late_rows + count] + late_total[late_rows + count :]
    smalls = []
    for chunks in places:
        smalls.append(
            jnp.concatenate(
                [summed_lines[line, begin : begin + size] for line, begin, size in chunks]
            )
        )
    return (
        output,
        grad_tokens,
        memory_part,
        self_sums[0],
        smalls[0],
        self_sums[1],
        self_sums[2],
        smalls[1],
        self_sums[3],
        smalls[2],
        cross_sums[0],
        smalls[3],
        cross_sums[1],
        cross_sums[2],
        smalls[4],
        cross_sums[3],
        smalls[5],
        smalls[6],
        smalls[7],
        smalls[8],
        smalls[9],
        smalls[10],
        smalls[11],
        ffn_sums[0],
        smalls[12],
        ffn_sums[1],
        smalls[13],
    )


def solution(mesh):
    dp_size = mesh.shape["dp"]
    inner = 4 if dp_size % 4 == 0 and dp_size > 4 else 1
    devices = np.asarray(mesh.devices).reshape(dp_size // inner, inner, mesh.shape["tensor"])
    staged = Mesh(devices, ("outer", "inner", "tensor"))
    return jax.shard_map(
        on_device,
        mesh=staged,
        in_specs=(
            P(DP, None),
            P(DP, None),
            P(DP),
            P(DP, None),
            P(None, "tensor"),
            P("tensor"),
            P(None, "tensor"),
            P(None, "tensor"),
            P("tensor"),
            P("tensor", None),
            P(),
            P(None, "tensor"),
            P("tensor"),
            P(None, "tensor"),
            P(None, "tensor"),
            P("tensor"),
            P("tensor", None),
            P(),
            P(),
            P(),
            P(),
            P(),
            P(),
            P(),
            P(None, "tensor"),
            P("tensor"),
            P("tensor", None),
            P(),
        ),
        out_specs=(
            P(DP, None),
            P(("outer", "inner", "tensor"), None),
            P(("outer", "inner", "tensor"), None),
            P(DP, "tensor"),
            P("tensor"),
            P(DP, "tensor"),
            P(DP, "tensor"),
            P("tensor"),
            P("tensor", DP),
            P(),
            P(DP, "tensor"),
            P("tensor"),
            P(DP, "tensor"),
            P(DP, "tensor"),
            P("tensor"),
            P("tensor", DP),
            P(),
            P(),
            P(),
            P(),
            P(),
            P(),
            P(),
            P(DP, "tensor"),
            P("tensor"),
            P("tensor", DP),
            P(),
        ),
        check_vma=False,
    )
```

```python
from functools import partial

import jax
import jax.numpy as jnp
from jax import lax
from jax.sharding import Mesh, PartitionSpec as P
import numpy as np

DP = ("outer", "inner")

HD = 64


EPSILON = 1e-05
NEGATIVE = -1e30


def normalize(hidden, gain, shift):
    center = hidden - jnp.mean(hidden, -1, keepdims=True)
    spread = jnp.mean(center * center, -1, keepdims=True)
    return center * lax.rsqrt(spread + EPSILON) * gain + shift


def project(data, weight):
    return jnp.dot(data, weight, preferred_element_type=jnp.float32)


def column_sums(values):
    return jnp.sum(values.astype(jnp.float32), 0)


def heads_of(matrix):
    return matrix.reshape(matrix.shape[0], -1, HD)


def allowed_pairs(query_segment, key_segment, start, causal):
    same = query_segment[:, None] == key_segment[None, :]
    if causal:
        query_place = start + jnp.arange(query_segment.shape[0], dtype=jnp.int32)
        key_place = jnp.arange(key_segment.shape[0], dtype=jnp.int32)
        same = same & (key_place[None, :] <= query_place[:, None])
    return same[None]


def attend_forward(queries, keys, values, segment, causal):
    length = queries.shape[0]
    block_rows = min(256 if causal else 512, length)
    contexts = []
    totals = []
    for index in range(length // block_rows):
        start = index * block_rows
        end = start + block_rows if causal else length
        piece = queries[start : start + block_rows]
        scores = jnp.einsum(
            "qhe,khe->hqk", piece, keys[:end], preferred_element_type=jnp.float32
        )
        scores = jnp.where(
            allowed_pairs(segment[start : start + block_rows], segment[:end], start, causal),
            scores,
            NEGATIVE,
        )
        highest = jnp.max(scores, -1, keepdims=True)
        powers = jnp.exp(scores - highest)
        summed = jnp.sum(powers, -1, keepdims=True)
        weights = (powers / summed).astype(jnp.bfloat16)
        contexts.append(
            jnp.einsum("hqk,khe->qhe", weights, values[:end], preferred_element_type=jnp.float32)
        )
        totals.append(highest + jnp.log(summed))
    return (jnp.concatenate(contexts, 0), jnp.concatenate(totals, 1))


def attend_backward(queries, keys, values, grad_context, totals, segment, causal, exact_context):
    length = queries.shape[0]
    block_rows = min(256 if causal else 512, length)
    inner = jnp.einsum(
        "qhe,qhe->hq", grad_context.astype(jnp.float32), exact_context
    )[..., None]
    grad_queries = []
    grad_keys = jnp.zeros(keys.shape, jnp.float32)
    grad_values = jnp.zeros(values.shape, jnp.float32)
    for index in range(length // block_rows):
        start = index * block_rows
        end = start + block_rows if causal else length
        piece = queries[start : start + block_rows]
        grad_piece = grad_context[start : start + block_rows]
        near_keys = keys[:end]
        scores = jnp.einsum("qhe,khe->hqk", piece, near_keys, preferred_element_type=jnp.float32)
        scores = jnp.where(
            allowed_pairs(segment[start : start + block_rows], segment[:end], start, causal),
            scores,
            NEGATIVE,
        )
        probs = jnp.exp(scores - totals[:, start : start + block_rows])
        grad_probs = jnp.einsum(
            "qhe,khe->hqk", grad_piece, values[:end], preferred_element_type=jnp.float32
        )
        row_inner = inner[:, start : start + block_rows]
        grad_scores = (probs * (grad_probs - row_inner)).astype(jnp.bfloat16)
        grad_queries.append(
            jnp.einsum("hqk,khe->qhe", grad_scores, near_keys, preferred_element_type=jnp.float32)
        )
        grad_keys = grad_keys.at[:end].add(
            jnp.einsum("hqk,qhe->khe", grad_scores, piece, preferred_element_type=jnp.float32)
        )
        grad_values = grad_values.at[:end].add(
            jnp.einsum(
                "hqk,qhe->khe",
                probs.astype(jnp.bfloat16),
                grad_piece,
                preferred_element_type=jnp.float32,
            )
        )
    return (jnp.concatenate(grad_queries, 0), grad_keys, grad_values)


def on_device(
    tokens,
    memory,
    segment,
    cotangent,
    self_query,
    self_query_bias,
    self_key,
    self_value,
    self_value_bias,
    self_output,
    self_output_bias,
    cross_query,
    cross_query_bias,
    cross_key,
    cross_value,
    cross_value_bias,
    cross_output,
    cross_output_bias,
    first_gain,
    first_shift,
    second_gain,
    second_shift,
    third_gain,
    third_shift,
    inner_weight,
    inner_bias,
    outer_weight,
    outer_bias,
):
    scale = HD ** (-0.5)
    length = tokens.shape[0]
    groups = lax.axis_size("tensor")
    member = lax.axis_index("tensor")
    half = length // groups

    def rows_of(values):
        return lax.dynamic_slice_in_dim(values, member * half, half, 0)

    def spread_out(values):
        whole = jnp.zeros((values.shape[0] * groups,), jnp.float32)
        return lax.dynamic_update_slice_in_dim(whole, values, member * values.shape[0], 0)

    def own_share(values, count):
        return lax.dynamic_slice_in_dim(values, member * count, count, 0)

    def swap(values):
        return lax.ppermute(values, "tensor", [(0, 1), (1, 0)])

    def gather_rows(values):
        if groups != 2:
            return lax.all_gather(values, "tensor", axis=0, tiled=True)
        other = swap(values)
        lead = member == 0
        return jnp.concatenate(
            [jnp.where(lead, values, other), jnp.where(lead, other, values)], 0
        )

    def scatter_rows(values):
        if groups != 2:
            return lax.psum_scatter(
                values, "tensor", scatter_dimension=0, tiled=True
            ).astype(jnp.float32)
        top = values[:half]
        bottom = values[half:]
        lead = member == 0
        keep = jnp.where(lead, top, bottom)
        send = jnp.where(lead, bottom, top)
        return keep.astype(jnp.float32) + swap(send).astype(jnp.float32)

    def sum_pair(values):
        if groups != 2:
            return lax.psum(values, "tensor").astype(jnp.float32)
        return values.astype(jnp.float32) + swap(values).astype(jnp.float32)

    queries = ((project(tokens, self_query) + self_query_bias.astype(jnp.float32)) * scale).astype(
        jnp.bfloat16
    )
    keys = project(tokens, self_key).astype(jnp.bfloat16)
    values = (project(tokens, self_value) + self_value_bias.astype(jnp.float32)).astype(
        jnp.bfloat16
    )
    self_queries = heads_of(queries)
    self_keys = heads_of(keys)
    self_values = heads_of(values)
    self_context, self_totals = attend_forward(self_queries, self_keys, self_values, segment, True)
    self_exact = self_context
    self_context = self_context.reshape(length, -1).astype(jnp.bfloat16)
    attended = scatter_rows(project(self_context, self_output)) + self_output_bias.astype(
        jnp.float32
    )
    first, first_back = jax.vjp(
        normalize,
        rows_of(tokens).astype(jnp.float32) + attended,
        first_gain.astype(jnp.float32),
        first_shift.astype(jnp.float32),
    )
    first_low = gather_rows(first.astype(jnp.bfloat16))
    queries = (
        (project(first_low, cross_query) + cross_query_bias.astype(jnp.float32)) * scale
    ).astype(jnp.bfloat16)
    keys = project(memory, cross_key).astype(jnp.bfloat16)
    values = (project(memory, cross_value) + cross_value_bias.astype(jnp.float32)).astype(
        jnp.bfloat16
    )
    cross_queries = heads_of(queries)
    cross_keys = heads_of(keys)
    cross_values = heads_of(values)
    cross_context, cross_totals = attend_forward(
        cross_queries, cross_keys, cross_values, segment, False
    )
    cross_exact = cross_context
    cross_context = cross_context.reshape(length, -1).astype(jnp.bfloat16)
    crossed = scatter_rows(
        project(cross_context, cross_output).astype(jnp.bfloat16)
    ) + cross_output_bias.astype(jnp.float32)
    second_part, second_back = jax.vjp(
        normalize,
        first + crossed,
        second_gain.astype(jnp.float32),
        second_shift.astype(jnp.float32),
    )
    second = gather_rows(second_part.astype(jnp.bfloat16)).astype(second_part.dtype)
    second_low = second.astype(jnp.bfloat16)
    inner = project(second_low, inner_weight) + inner_bias.astype(jnp.float32)
    hidden = jax.nn.gelu(inner, approximate=False).astype(jnp.bfloat16)
    outer = sum_pair(project(hidden, outer_weight).astype(jnp.bfloat16)) + outer_bias.astype(
        jnp.float32
    )
    result, third_back = jax.vjp(
        normalize, second + outer, third_gain.astype(jnp.float32), third_shift.astype(jnp.float32)
    )
    output = result.astype(jnp.bfloat16)
    grad_third, grad_third_gain, grad_third_shift = third_back(cotangent.astype(jnp.float32))
    grad_outer = grad_third.astype(jnp.bfloat16)
    grad_outer_bias = column_sums(grad_outer)
    gelu_back = jax.vjp(partial(jax.nn.gelu, approximate=False), inner)[1]
    grad_inner = gelu_back(project(grad_outer, outer_weight.T))[0].astype(jnp.bfloat16)
    grad_inner_weight = project(second_low.T, grad_inner)
    grad_inner_bias = column_sums(grad_inner)
    grad_second = rows_of(grad_third) + scatter_rows(
        project(grad_inner, inner_weight.T).astype(jnp.bfloat16)
    )
    grad_second_in, grad_second_gain, grad_second_shift = second_back(grad_second)
    grad_cross_rows = grad_second_in.astype(jnp.bfloat16)
    grad_cross = gather_rows(grad_cross_rows)
    grad_cross_output_bias = column_sums(grad_cross)
    grad_cross_context = heads_of(project(grad_cross, cross_output.T).astype(jnp.bfloat16))
    cross_grad_q, cross_grad_k, cross_grad_v = attend_backward(
        cross_queries,
        cross_keys,
        cross_values,
        grad_cross_context,
        cross_totals,
        segment,
        False,
        cross_exact,
    )
    cross_grad_q = (cross_grad_q.astype(jnp.bfloat16) * scale).reshape(length, -1)
    cross_grad_k = cross_grad_k.astype(jnp.bfloat16).reshape(length, -1)
    cross_grad_v = cross_grad_v.astype(jnp.bfloat16).reshape(length, -1)
    grad_cross_query = project(first_low.T, cross_grad_q)
    grad_cross_query_bias = column_sums(cross_grad_q)
    grad_cross_key = project(memory.T, cross_grad_k)
    grad_cross_value = project(memory.T, cross_grad_v)
    grad_cross_value_bias = column_sums(cross_grad_v)
    memory_term = project(cross_grad_k, cross_key.T) + project(cross_grad_v, cross_value.T)
    grad_first = grad_second_in + scatter_rows(
        project(cross_grad_q, cross_query.T).astype(jnp.bfloat16)
    )
    grad_cross_output_t = project(grad_cross.T, cross_context)
    cross = [grad_cross_query, grad_cross_key, grad_cross_value, grad_cross_output_t]
    cross_joined = jnp.concatenate(cross, 1).astype(jnp.bfloat16)
    cross_joined, grad_first = lax.optimization_barrier((cross_joined, grad_first))
    grad_first_in, grad_first_gain, grad_first_shift = first_back(grad_first)
    grad_self_rows = grad_first_in.astype(jnp.bfloat16)
    grad_self = gather_rows(grad_self_rows)
    grad_self_output_bias = column_sums(grad_self)
    grad_self_context = heads_of(project(grad_self, self_output.T).astype(jnp.bfloat16))
    outer_size = lax.axis_size("outer")
    inner_size = lax.axis_size("inner")
    dp_size = outer_size * inner_size
    self_grad_q, self_grad_k, self_grad_v = attend_backward(
        self_queries,
        self_keys,
        self_values,
        grad_self_context,
        self_totals,
        segment,
        True,
        self_exact,
    )
    self_grad_q = (self_grad_q.astype(jnp.bfloat16) * scale).reshape(length, -1)
    self_grad_k = self_grad_k.astype(jnp.bfloat16).reshape(length, -1)
    self_grad_v = self_grad_v.astype(jnp.bfloat16).reshape(length, -1)
    grad_self_query = project(tokens.T, self_grad_q)
    grad_self_query_bias = column_sums(self_grad_q)
    grad_self_key = project(tokens.T, self_grad_k)
    grad_self_value = project(tokens.T, self_grad_v)
    grad_self_value_bias = column_sums(self_grad_v)
    tokens_term = (
        project(self_grad_q, self_query.T)
        + project(self_grad_k, self_key.T)
        + project(self_grad_v, self_value.T)
    )
    tokens_part = scatter_rows(tokens_term.astype(jnp.bfloat16))
    memory_part = scatter_rows(memory_term.astype(jnp.bfloat16))
    grad_tokens = tokens_part + grad_first_in
    grad_self_output_t = project(grad_self.T, self_context)
    grad_outer_weight_t = project(grad_outer.T, hidden)

    def split_columns(summed, pieces, flipped):
        parts = []
        offset = 0
        for position, piece in enumerate(pieces):
            width = piece.shape[1]
            part = summed[:, offset : offset + width]
            offset += width
            if position in flipped:
                part = part.T
            parts.append(part)
        return parts

    def exchange_sum(joined, extra=None):
        rows = joined.shape[0] // dp_size
        width = joined.shape[1]
        blocks = joined.reshape(dp_size, rows, width)
        if inner_size == 1 or outer_size == 1:
            if extra is not None:
                blocks = jnp.concatenate(
                    [blocks, jnp.broadcast_to(extra[None], (dp_size,) + extra.shape)], 1
                )
            received = lax.all_to_all(blocks, DP, 0, 0, tiled=True)
            return jnp.sum(received.astype(jnp.float32), 0)
        staged = blocks.reshape(outer_size, inner_size, rows, width)
        staged = jnp.swapaxes(staged, 0, 1).reshape(inner_size, outer_size * rows, width)
        if extra is not None:
            staged = jnp.concatenate(
                [staged, jnp.broadcast_to(extra[None], (inner_size,) + extra.shape)], 1
            )
        if inner_size == 4 and extra is not None:
            spot = lax.axis_index("inner")
            swapped = []
            for mask in range(inner_size):
                piece = lax.dynamic_index_in_dim(staged, spot ^ mask, 0, keepdims=False)
                if mask:
                    piece = lax.ppermute(
                        piece, "inner", [(peer, peer ^ mask) for peer in range(inner_size)]
                    )
                swapped.append(piece)
            partial = None
            for source in range(inner_size):
                chosen = swapped[0]
                for mask in range(1, inner_size):
                    chosen = jnp.where(spot ^ mask == source, swapped[mask], chosen)
                chosen = chosen.astype(jnp.float32)
                partial = chosen if partial is None else partial + chosen
        else:
            first = lax.all_to_all(staged, "inner", 0, 0, tiled=True)
            partial = jnp.sum(first.astype(jnp.float32), 0)
        middle = partial[: outer_size * rows].astype(jnp.bfloat16).reshape(
            outer_size, rows, width
        )
        if extra is not None:
            lines = extra.shape[0] // 2
            tail = partial[outer_size * rows :]
            merged = tail[:lines] + tail[lines:]
            high = merged.astype(jnp.bfloat16)
            low = (merged - high.astype(jnp.float32)).astype(jnp.bfloat16)
            pair = jnp.concatenate([high, low], 0)
            middle = jnp.concatenate(
                [middle, jnp.broadcast_to(pair[None], (outer_size,) + pair.shape)], 1
            )
        if outer_size > 4:
            second = lax.all_to_all(middle, "outer", 0, 0, tiled=True)
            return jnp.sum(second.astype(jnp.float32), 0)
        place = lax.axis_index("outer")
        by_source = [None] * outer_size
        for shift in range(outer_size):
            piece = lax.dynamic_index_in_dim(
                middle, (place + shift) % outer_size, 0, keepdims=False
            )
            if shift:
                piece = lax.ppermute(
                    piece,
                    "outer",
                    [(peer, (peer + shift) % outer_size) for peer in range(outer_size)],
                )
            by_source[shift] = piece
        total = None
        for source in range(outer_size):
            chosen = by_source[0]
            for shift in range(1, outer_size):
                chosen = jnp.where(
                    (place - shift) % outer_size == source, by_source[shift], chosen
                )
            chosen = chosen.astype(jnp.float32)
            total = chosen if total is None else total + chosen
        return total

    ffn = [grad_inner_weight, grad_outer_weight_t]
    ffn_sum = lax.psum_scatter(
        jnp.concatenate(ffn, 1).astype(jnp.bfloat16), DP, scatter_dimension=0, tiled=True
    ).astype(jnp.float32)
    ffn_sums = split_columns(ffn_sum, ffn, (1,))
    cross_sums = split_columns(exchange_sum(cross_joined), cross, (3,))
    late = [grad_self_query, grad_self_key, grad_self_value, grad_self_output_t]
    late_joined = jnp.concatenate(late, 1).astype(jnp.bfloat16)
    norm_pairs = sum_pair(
        jnp.concatenate([grad_first_gain, grad_first_shift, grad_second_gain, grad_second_shift])
    )
    width = late_joined.shape[1]
    sections = norm_pairs.shape[0] // 4
    biases = [
        grad_self_query_bias,
        grad_self_value_bias,
        grad_self_output_bias,
        grad_cross_query_bias,
        grad_cross_value_bias,
        grad_cross_output_bias,
        norm_pairs[:sections],
        norm_pairs[sections : 2 * sections],
        norm_pairs[2 * sections : 3 * sections],
        norm_pairs[3 * sections :],
        grad_third_gain,
        grad_third_shift,
        grad_inner_bias,
        grad_outer_bias,
    ]
    lines = []
    current = []
    used = 0
    places = []
    for bias in biases:
        chunks = []
        for begin in range(0, bias.shape[0], width):
            chunk = bias[begin : begin + width]
            if used + chunk.shape[0] > width:
                if used < width:
                    current.append(jnp.zeros((width - used,), jnp.float32))
                lines.append(jnp.concatenate(current))
                current = []
                used = 0
            chunks.append((len(lines), used, chunk.shape[0]))
            current.append(chunk)
            used += chunk.shape[0]
        places.append(chunks)
    if used < width:
        current.append(jnp.zeros((width - used,), jnp.float32))
    lines.append(jnp.concatenate(current))
    padded = jnp.stack(lines)
    count = padded.shape[0]
    high = padded.astype(jnp.bfloat16)
    low = (padded - high.astype(jnp.float32)).astype(jnp.bfloat16)
    late_rows = late_joined.shape[0] // dp_size
    late_total = exchange_sum(late_joined, jnp.concatenate([high, low], 0))
    self_sums = split_columns(late_total[:late_rows], late, (3,))
    summed_lines = late_total[late_rows : late_rows + count] + late_total[late_rows + count :]
    smalls = []
    for chunks in places:
        smalls.append(
            jnp.concatenate(
                [summed_lines[line, begin : begin + size] for line, begin, size in chunks]
            )
        )
    return (
        output,
        grad_tokens,
        memory_part,
        self_sums[0],
        smalls[0],
        self_sums[1],
        self_sums[2],
        smalls[1],
        self_sums[3],
        smalls[2],
        cross_sums[0],
        smalls[3],
        cross_sums[1],
        cross_sums[2],
        smalls[4],
        cross_sums[3],
        smalls[5],
        smalls[6],
        smalls[7],
        smalls[8],
        smalls[9],
        smalls[10],
        smalls[11],
        ffn_sums[0],
        smalls[12],
        ffn_sums[1],
        smalls[13],
    )


def solution(mesh):
    dp_size = mesh.shape["dp"]
    inner = 4 if dp_size % 4 == 0 and dp_size > 4 else 1
    devices = np.asarray(mesh.devices).reshape(dp_size // inner, inner, mesh.shape["tensor"])
    staged = Mesh(devices, ("outer", "inner", "tensor"))
    return jax.shard_map(
        on_device,
        mesh=staged,
        in_specs=(
            P(DP, None),
            P(DP, None),
            P(DP),
            P(DP, None),
            P(None, "tensor"),
            P("tensor"),
            P(None, "tensor"),
            P(None, "tensor"),
            P("tensor"),
            P("tensor", None),
            P(),
            P(None, "tensor"),
            P("tensor"),
            P(None, "tensor"),
            P(None, "tensor"),
            P("tensor"),
            P("tensor", None),
            P(),
            P(),
            P(),
            P(),
            P(),
            P(),
            P(),
            P(None, "tensor"),
            P("tensor"),
            P("tensor", None),
            P(),
        ),
        out_specs=(
            P(DP, None),
            P(("outer", "inner", "tensor"), None),
            P(("outer", "inner", "tensor"), None),
            P(DP, "tensor"),
            P("tensor"),
            P(DP, "tensor"),
            P(DP, "tensor"),
            P("tensor"),
            P("tensor", DP),
            P(),
            P(DP, "tensor"),
            P("tensor"),
            P(DP, "tensor"),
            P(DP, "tensor"),
            P("tensor"),
            P("tensor", DP),
            P(),
            P(),
            P(),
            P(),
            P(),
            P(),
            P(),
            P(DP, "tensor"),
            P("tensor"),
            P("tensor", DP),
            P(),
        ),
        check_vma=False,
    )
```

```python
from functools import partial

import jax
import jax.numpy as jnp
from jax import lax
from jax.sharding import Mesh, PartitionSpec as P
import numpy as np

DP = ("outer", "inner")

HD = 64


EPSILON = 1e-05
NEGATIVE = -1e30


def normalize(hidden, gain, shift):
    center = hidden - jnp.mean(hidden, -1, keepdims=True)
    spread = jnp.mean(center * center, -1, keepdims=True)
    return center * lax.rsqrt(spread + EPSILON) * gain + shift


def project(data, weight):
    return jnp.dot(data, weight, preferred_element_type=jnp.float32)


def column_sums(values):
    return jnp.sum(values.astype(jnp.float32), 0)


def heads_of(matrix):
    return matrix.reshape(matrix.shape[0], -1, HD)


def allowed_pairs(query_segment, key_segment, start, causal):
    same = query_segment[:, None] == key_segment[None, :]
    if causal:
        query_place = start + jnp.arange(query_segment.shape[0], dtype=jnp.int32)
        key_place = jnp.arange(key_segment.shape[0], dtype=jnp.int32)
        same = same & (key_place[None, :] <= query_place[:, None])
    return same[None]


def attend_forward(queries, keys, values, segment, causal):
    length = queries.shape[0]
    block_rows = min(256 if causal else 512, length)
    contexts = []
    totals = []
    for index in range(length // block_rows):
        start = index * block_rows
        end = start + block_rows if causal else length
        piece = queries[start : start + block_rows]
        scores = jnp.einsum(
            "qhe,khe->hqk", piece, keys[:end], preferred_element_type=jnp.float32
        )
        scores = jnp.where(
            allowed_pairs(segment[start : start + block_rows], segment[:end], start, causal),
            scores,
            NEGATIVE,
        )
        highest = jnp.max(scores, -1, keepdims=True)
        powers = jnp.exp(scores - highest)
        summed = jnp.sum(powers, -1, keepdims=True)
        weights = (powers / summed).astype(jnp.bfloat16)
        contexts.append(
            jnp.einsum("hqk,khe->qhe", weights, values[:end], preferred_element_type=jnp.float32)
        )
        totals.append(highest + jnp.log(summed))
    return (jnp.concatenate(contexts, 0), jnp.concatenate(totals, 1))


def attend_backward(queries, keys, values, grad_context, totals, segment, causal, exact_context):
    length = queries.shape[0]
    block_rows = min(256 if causal else 512, length)
    inner = jnp.einsum(
        "qhe,qhe->hq", grad_context.astype(jnp.float32), exact_context
    )[..., None]
    grad_queries = []
    grad_keys = jnp.zeros(keys.shape, jnp.float32)
    grad_values = jnp.zeros(values.shape, jnp.float32)
    for index in range(length // block_rows):
        start = index * block_rows
        end = start + block_rows if causal else length
        piece = queries[start : start + block_rows]
        grad_piece = grad_context[start : start + block_rows]
        near_keys = keys[:end]
        scores = jnp.einsum("qhe,khe->hqk", piece, near_keys, preferred_element_type=jnp.float32)
        scores = jnp.where(
            allowed_pairs(segment[start : start + block_rows], segment[:end], start, causal),
            scores,
            NEGATIVE,
        )
        probs = jnp.exp(scores - totals[:, start : start + block_rows])
        grad_probs = jnp.einsum(
            "qhe,khe->hqk", grad_piece, values[:end], preferred_element_type=jnp.float32
        )
        row_inner = inner[:, start : start + block_rows]
        grad_scores = (probs * (grad_probs - row_inner)).astype(jnp.bfloat16)
        grad_queries.append(
            jnp.einsum("hqk,khe->qhe", grad_scores, near_keys, preferred_element_type=jnp.float32)
        )
        grad_keys = grad_keys.at[:end].add(
            jnp.einsum("hqk,qhe->khe", grad_scores, piece, preferred_element_type=jnp.float32)
        )
        grad_values = grad_values.at[:end].add(
            jnp.einsum(
                "hqk,qhe->khe",
                probs.astype(jnp.bfloat16),
                grad_piece,
                preferred_element_type=jnp.float32,
            )
        )
    return (jnp.concatenate(grad_queries, 0), grad_keys, grad_values)


def on_device(
    tokens,
    memory,
    segment,
    cotangent,
    self_query,
    self_query_bias,
    self_key,
    self_value,
    self_value_bias,
    self_output,
    self_output_bias,
    cross_query,
    cross_query_bias,
    cross_key,
    cross_value,
    cross_value_bias,
    cross_output,
    cross_output_bias,
    first_gain,
    first_shift,
    second_gain,
    second_shift,
    third_gain,
    third_shift,
    inner_weight,
    inner_bias,
    outer_weight,
    outer_bias,
):
    scale = HD ** (-0.5)
    length = tokens.shape[0]
    groups = lax.axis_size("tensor")
    member = lax.axis_index("tensor")
    half = length // groups

    def rows_of(values):
        return lax.dynamic_slice_in_dim(values, member * half, half, 0)

    def spread_out(values):
        whole = jnp.zeros((values.shape[0] * groups,), jnp.float32)
        return lax.dynamic_update_slice_in_dim(whole, values, member * values.shape[0], 0)

    def own_share(values, count):
        return lax.dynamic_slice_in_dim(values, member * count, count, 0)

    def swap(values):
        return lax.ppermute(values, "tensor", [(0, 1), (1, 0)])

    def gather_rows(values):
        if groups != 2:
            return lax.all_gather(values, "tensor", axis=0, tiled=True)
        other = swap(values)
        lead = member == 0
        return jnp.concatenate(
            [jnp.where(lead, values, other), jnp.where(lead, other, values)], 0
        )

    def scatter_rows(values):
        if groups != 2:
            return lax.psum_scatter(
                values, "tensor", scatter_dimension=0, tiled=True
            ).astype(jnp.float32)
        top = values[:half]
        bottom = values[half:]
        lead = member == 0
        keep = jnp.where(lead, top, bottom)
        send = jnp.where(lead, bottom, top)
        return keep.astype(jnp.float32) + swap(send).astype(jnp.float32)

    def sum_pair(values):
        if groups != 2:
            return lax.psum(values, "tensor").astype(jnp.float32)
        return values.astype(jnp.float32) + swap(values).astype(jnp.float32)

    queries = ((project(tokens, self_query) + self_query_bias.astype(jnp.float32)) * scale).astype(
        jnp.bfloat16
    )
    keys = project(tokens, self_key).astype(jnp.bfloat16)
    values = (project(tokens, self_value) + self_value_bias.astype(jnp.float32)).astype(
        jnp.bfloat16
    )
    self_queries = heads_of(queries)
    self_keys = heads_of(keys)
    self_values = heads_of(values)
    self_context, self_totals = attend_forward(self_queries, self_keys, self_values, segment, True)
    self_exact = self_context
    self_context = self_context.reshape(length, -1).astype(jnp.bfloat16)
    attended = scatter_rows(project(self_context, self_output)) + self_output_bias.astype(
        jnp.float32
    )
    first, first_back = jax.vjp(
        normalize,
        rows_of(tokens).astype(jnp.float32) + attended,
        first_gain.astype(jnp.float32),
        first_shift.astype(jnp.float32),
    )
    first_low = gather_rows(first.astype(jnp.bfloat16))
    queries = (
        (project(first_low, cross_query) + cross_query_bias.astype(jnp.float32)) * scale
    ).astype(jnp.bfloat16)
    keys = project(memory, cross_key).astype(jnp.bfloat16)
    values = (project(memory, cross_value) + cross_value_bias.astype(jnp.float32)).astype(
        jnp.bfloat16
    )
    cross_queries = heads_of(queries)
    cross_keys = heads_of(keys)
    cross_values = heads_of(values)
    cross_context, cross_totals = attend_forward(
        cross_queries, cross_keys, cross_values, segment, False
    )
    cross_exact = cross_context
    cross_context = cross_context.reshape(length, -1).astype(jnp.bfloat16)
    crossed = scatter_rows(
        project(cross_context, cross_output).astype(jnp.bfloat16)
    ) + cross_output_bias.astype(jnp.float32)
    second_part, second_back = jax.vjp(
        normalize,
        first + crossed,
        second_gain.astype(jnp.float32),
        second_shift.astype(jnp.float32),
    )
    second = gather_rows(second_part.astype(jnp.bfloat16)).astype(second_part.dtype)
    second_low = second.astype(jnp.bfloat16)
    inner = project(second_low, inner_weight) + inner_bias.astype(jnp.float32)
    hidden = jax.nn.gelu(inner, approximate=False).astype(jnp.bfloat16)
    outer = sum_pair(project(hidden, outer_weight).astype(jnp.bfloat16)) + outer_bias.astype(
        jnp.float32
    )
    result, third_back = jax.vjp(
        normalize, second + outer, third_gain.astype(jnp.float32), third_shift.astype(jnp.float32)
    )
    output = result.astype(jnp.bfloat16)
    grad_third, grad_third_gain, grad_third_shift = third_back(cotangent.astype(jnp.float32))
    grad_outer = grad_third.astype(jnp.bfloat16)
    grad_outer_bias = column_sums(grad_outer)
    gelu_back = jax.vjp(partial(jax.nn.gelu, approximate=False), inner)[1]
    grad_inner = gelu_back(project(grad_outer, outer_weight.T))[0].astype(jnp.bfloat16)
    grad_inner_weight = project(second_low.T, grad_inner)
    grad_inner_bias = column_sums(grad_inner)
    grad_second = rows_of(grad_third) + scatter_rows(
        project(grad_inner, inner_weight.T).astype(jnp.bfloat16)
    )
    grad_second_in, grad_second_gain, grad_second_shift = second_back(grad_second)
    grad_cross_rows = grad_second_in.astype(jnp.bfloat16)
    grad_cross = gather_rows(grad_cross_rows)
    grad_cross_output_bias = column_sums(grad_cross)
    grad_cross_context = heads_of(project(grad_cross, cross_output.T).astype(jnp.bfloat16))
    cross_grad_q, cross_grad_k, cross_grad_v = attend_backward(
        cross_queries,
        cross_keys,
        cross_values,
        grad_cross_context,
        cross_totals,
        segment,
        False,
        cross_exact,
    )
    cross_grad_q = (cross_grad_q.astype(jnp.bfloat16) * scale).reshape(length, -1)
    cross_grad_k = cross_grad_k.astype(jnp.bfloat16).reshape(length, -1)
    cross_grad_v = cross_grad_v.astype(jnp.bfloat16).reshape(length, -1)
    grad_cross_query = project(first_low.T, cross_grad_q)
    grad_cross_query_bias = column_sums(cross_grad_q)
    grad_cross_key = project(memory.T, cross_grad_k)
    grad_cross_value = project(memory.T, cross_grad_v)
    grad_cross_value_bias = column_sums(cross_grad_v)
    memory_term = project(cross_grad_k, cross_key.T) + project(cross_grad_v, cross_value.T)
    grad_first = grad_second_in + scatter_rows(
        project(cross_grad_q, cross_query.T).astype(jnp.bfloat16)
    )
    grad_cross_output_t = project(grad_cross.T, cross_context)
    cross = [grad_cross_query, grad_cross_key, grad_cross_value, grad_cross_output_t]
    cross_joined = jnp.concatenate(cross, 1).astype(jnp.bfloat16)
    cross_joined, grad_first = lax.optimization_barrier((cross_joined, grad_first))
    grad_first_in, grad_first_gain, grad_first_shift = first_back(grad_first)
    grad_self_rows = grad_first_in.astype(jnp.bfloat16)
    grad_self = gather_rows(grad_self_rows)
    grad_self_output_bias = column_sums(grad_self)
    grad_self_context = heads_of(project(grad_self, self_output.T).astype(jnp.bfloat16))
    outer_size = lax.axis_size("outer")
    inner_size = lax.axis_size("inner")
    dp_size = outer_size * inner_size
    self_grad_q, self_grad_k, self_grad_v = attend_backward(
        self_queries,
        self_keys,
        self_values,
        grad_self_context,
        self_totals,
        segment,
        True,
        self_exact,
    )
    self_grad_q = (self_grad_q.astype(jnp.bfloat16) * scale).reshape(length, -1)
    self_grad_k = self_grad_k.astype(jnp.bfloat16).reshape(length, -1)
    self_grad_v = self_grad_v.astype(jnp.bfloat16).reshape(length, -1)
    grad_self_query = project(tokens.T, self_grad_q)
    grad_self_query_bias = column_sums(self_grad_q)
    grad_self_key = project(tokens.T, self_grad_k)
    grad_self_value = project(tokens.T, self_grad_v)
    grad_self_value_bias = column_sums(self_grad_v)
    tokens_term = (
        project(self_grad_q, self_query.T)
        + project(self_grad_k, self_key.T)
        + project(self_grad_v, self_value.T)
    )
    tokens_part = scatter_rows(tokens_term.astype(jnp.bfloat16))
    memory_part = scatter_rows(memory_term.astype(jnp.bfloat16))
    grad_tokens = tokens_part + grad_first_in
    grad_self_output_t = project(grad_self.T, self_context)
    grad_outer_weight_t = project(grad_outer.T, hidden)

    def split_columns(summed, pieces, flipped):
        parts = []
        offset = 0
        for position, piece in enumerate(pieces):
            width = piece.shape[1]
            part = summed[:, offset : offset + width]
            offset += width
            if position in flipped:
                part = part.T
            parts.append(part)
        return parts

    def exchange_sum(joined, extra=None):
        rows = joined.shape[0] // dp_size
        width = joined.shape[1]
        blocks = joined.reshape(dp_size, rows, width)
        if inner_size == 1 or outer_size == 1:
            if extra is not None:
                blocks = jnp.concatenate(
                    [blocks, jnp.broadcast_to(extra[None], (dp_size,) + extra.shape)], 1
                )
            received = lax.all_to_all(blocks, DP, 0, 0, tiled=True)
            return jnp.sum(received.astype(jnp.float32), 0)
        staged = blocks.reshape(outer_size, inner_size, rows, width)
        staged = jnp.swapaxes(staged, 0, 1).reshape(inner_size, outer_size * rows, width)
        if extra is not None:
            staged = jnp.concatenate(
                [staged, jnp.broadcast_to(extra[None], (inner_size,) + extra.shape)], 1
            )
        first = lax.all_to_all(staged, "inner", 0, 0, tiled=True)
        partial = jnp.sum(first.astype(jnp.float32), 0)
        middle = partial[: outer_size * rows].astype(jnp.bfloat16).reshape(
            outer_size, rows, width
        )
        if extra is not None:
            lines = extra.shape[0] // 2
            tail = partial[outer_size * rows :]
            merged = tail[:lines] + tail[lines:]
            high = merged.astype(jnp.bfloat16)
            low = (merged - high.astype(jnp.float32)).astype(jnp.bfloat16)
            pair = jnp.concatenate([high, low], 0)
            middle = jnp.concatenate(
                [middle, jnp.broadcast_to(pair[None], (outer_size,) + pair.shape)], 1
            )
        if outer_size > 4 or extra is not None:
            second = lax.all_to_all(middle, "outer", 0, 0, tiled=True)
            return jnp.sum(second.astype(jnp.float32), 0)
        place = lax.axis_index("outer")
        by_source = [None] * outer_size
        for shift in range(outer_size):
            piece = lax.dynamic_index_in_dim(
                middle, (place + shift) % outer_size, 0, keepdims=False
            )
            if shift:
                piece = lax.ppermute(
                    piece,
                    "outer",
                    [(peer, (peer + shift) % outer_size) for peer in range(outer_size)],
                )
            by_source[shift] = piece
        total = None
        for source in range(outer_size):
            chosen = by_source[0]
            for shift in range(1, outer_size):
                chosen = jnp.where(
                    (place - shift) % outer_size == source, by_source[shift], chosen
                )
            chosen = chosen.astype(jnp.float32)
            total = chosen if total is None else total + chosen
        return total

    ffn = [grad_inner_weight, grad_outer_weight_t]
    ffn_sum = lax.psum_scatter(
        jnp.concatenate(ffn, 1).astype(jnp.bfloat16), DP, scatter_dimension=0, tiled=True
    ).astype(jnp.float32)
    ffn_sums = split_columns(ffn_sum, ffn, (1,))
    cross_sums = split_columns(exchange_sum(cross_joined), cross, (3,))
    late = [grad_self_query, grad_self_key, grad_self_value, grad_self_output_t]
    late_joined = jnp.concatenate(late, 1).astype(jnp.bfloat16)
    norm_pairs = sum_pair(
        jnp.concatenate([grad_first_gain, grad_first_shift, grad_second_gain, grad_second_shift])
    )
    width = late_joined.shape[1]
    sections = norm_pairs.shape[0] // 4
    biases = [
        grad_self_query_bias,
        grad_self_value_bias,
        grad_self_output_bias,
        grad_cross_query_bias,
        grad_cross_value_bias,
        grad_cross_output_bias,
        norm_pairs[:sections],
        norm_pairs[sections : 2 * sections],
        norm_pairs[2 * sections : 3 * sections],
        norm_pairs[3 * sections :],
        grad_third_gain,
        grad_third_shift,
        grad_inner_bias,
        grad_outer_bias,
    ]
    lines = []
    current = []
    used = 0
    places = []
    for bias in biases:
        chunks = []
        for begin in range(0, bias.shape[0], width):
            chunk = bias[begin : begin + width]
            if used + chunk.shape[0] > width:
                if used < width:
                    current.append(jnp.zeros((width - used,), jnp.float32))
                lines.append(jnp.concatenate(current))
                current = []
                used = 0
            chunks.append((len(lines), used, chunk.shape[0]))
            current.append(chunk)
            used += chunk.shape[0]
        places.append(chunks)
    if used < width:
        current.append(jnp.zeros((width - used,), jnp.float32))
    lines.append(jnp.concatenate(current))
    padded = jnp.stack(lines)
    count = padded.shape[0]
    high = padded.astype(jnp.bfloat16)
    low = (padded - high.astype(jnp.float32)).astype(jnp.bfloat16)
    late_rows = late_joined.shape[0] // dp_size
    late_total = exchange_sum(late_joined, jnp.concatenate([high, low], 0))
    self_sums = split_columns(late_total[:late_rows], late, (3,))
    summed_lines = late_total[late_rows : late_rows + count] + late_total[late_rows + count :]
    smalls = []
    for chunks in places:
        smalls.append(
            jnp.concatenate(
                [summed_lines[line, begin : begin + size] for line, begin, size in chunks]
            )
        )
    return (
        output,
        grad_tokens,
        memory_part,
        self_sums[0],
        smalls[0],
        self_sums[1],
        self_sums[2],
        smalls[1],
        self_sums[3],
        smalls[2],
        cross_sums[0],
        smalls[3],
        cross_sums[1],
        cross_sums[2],
        smalls[4],
        cross_sums[3],
        smalls[5],
        smalls[6],
        smalls[7],
        smalls[8],
        smalls[9],
        smalls[10],
        smalls[11],
        ffn_sums[0],
        smalls[12],
        ffn_sums[1],
        smalls[13],
    )


def solution(mesh):
    dp_size = mesh.shape["dp"]
    inner = 4 if dp_size % 4 == 0 and dp_size > 4 else 1
    devices = np.asarray(mesh.devices).reshape(dp_size // inner, inner, mesh.shape["tensor"])
    staged = Mesh(devices, ("outer", "inner", "tensor"))
    return jax.shard_map(
        on_device,
        mesh=staged,
        in_specs=(
            P(DP, None),
            P(DP, None),
            P(DP),
            P(DP, None),
            P(None, "tensor"),
            P("tensor"),
            P(None, "tensor"),
            P(None, "tensor"),
            P("tensor"),
            P("tensor", None),
            P(),
            P(None, "tensor"),
            P("tensor"),
            P(None, "tensor"),
            P(None, "tensor"),
            P("tensor"),
            P("tensor", None),
            P(),
            P(),
            P(),
            P(),
            P(),
            P(),
            P(),
            P(None, "tensor"),
            P("tensor"),
            P("tensor", None),
            P(),
        ),
        out_specs=(
            P(DP, None),
            P(("outer", "inner", "tensor"), None),
            P(("outer", "inner", "tensor"), None),
            P(DP, "tensor"),
            P("tensor"),
            P(DP, "tensor"),
            P(DP, "tensor"),
            P("tensor"),
            P("tensor", DP),
            P(),
            P(DP, "tensor"),
            P("tensor"),
            P(DP, "tensor"),
            P(DP, "tensor"),
            P("tensor"),
            P("tensor", DP),
            P(),
            P(),
            P(),
            P(),
            P(),
            P(),
            P(),
            P(DP, "tensor"),
            P("tensor"),
            P("tensor", DP),
            P(),
        ),
        check_vma=False,
    )
```

```python
from functools import partial

import jax
import jax.numpy as jnp
from jax import lax
from jax.sharding import Mesh, PartitionSpec as P
import numpy as np

DP = ("outer", "inner")

HD = 64


EPSILON = 1e-05
NEGATIVE = -1e30


def normalize(hidden, gain, shift):
    center = hidden - jnp.mean(hidden, -1, keepdims=True)
    spread = jnp.mean(center * center, -1, keepdims=True)
    return center * lax.rsqrt(spread + EPSILON) * gain + shift


def project(data, weight):
    return jnp.dot(data, weight, preferred_element_type=jnp.float32)


def column_sums(values):
    return jnp.sum(values.astype(jnp.float32), 0)


def heads_of(matrix):
    return matrix.reshape(matrix.shape[0], -1, HD)


def allowed_pairs(query_segment, key_segment, start, causal):
    same = query_segment[:, None] == key_segment[None, :]
    if causal:
        query_place = start + jnp.arange(query_segment.shape[0], dtype=jnp.int32)
        key_place = jnp.arange(key_segment.shape[0], dtype=jnp.int32)
        same = same & (key_place[None, :] <= query_place[:, None])
    return same[None]


def attend_forward(queries, keys, values, segment, causal):
    length = queries.shape[0]
    block_rows = min(512, length)
    contexts = []
    totals = []
    for index in range(length // block_rows):
        start = index * block_rows
        end = start + block_rows if causal else length
        piece = queries[start : start + block_rows]
        scores = jnp.einsum(
            "qhe,khe->hqk", piece, keys[:end], preferred_element_type=jnp.float32
        )
        scores = jnp.where(
            allowed_pairs(segment[start : start + block_rows], segment[:end], start, causal),
            scores,
            NEGATIVE,
        )
        highest = jnp.max(scores, -1, keepdims=True)
        powers = jnp.exp(scores - highest)
        summed = jnp.sum(powers, -1, keepdims=True)
        weights = (powers / summed).astype(jnp.bfloat16)
        contexts.append(
            jnp.einsum("hqk,khe->qhe", weights, values[:end], preferred_element_type=jnp.float32)
        )
        totals.append(highest + jnp.log(summed))
    return (jnp.concatenate(contexts, 0), jnp.concatenate(totals, 1))


def attend_backward(queries, keys, values, grad_context, totals, segment, causal, exact_context):
    length = queries.shape[0]
    block_rows = min(256 if causal else 512, length)
    inner = jnp.einsum(
        "qhe,qhe->hq", grad_context.astype(jnp.float32), exact_context
    )[..., None]
    grad_queries = []
    grad_keys = jnp.zeros(keys.shape, jnp.float32)
    grad_values = jnp.zeros(values.shape, jnp.float32)
    for index in range(length // block_rows):
        start = index * block_rows
        end = start + block_rows if causal else length
        piece = queries[start : start + block_rows]
        grad_piece = grad_context[start : start + block_rows]
        near_keys = keys[:end]
        scores = jnp.einsum("qhe,khe->hqk", piece, near_keys, preferred_element_type=jnp.float32)
        scores = jnp.where(
            allowed_pairs(segment[start : start + block_rows], segment[:end], start, causal),
            scores,
            NEGATIVE,
        )
        probs = jnp.exp(scores - totals[:, start : start + block_rows])
        grad_probs = jnp.einsum(
            "qhe,khe->hqk", grad_piece, values[:end], preferred_element_type=jnp.float32
        )
        row_inner = inner[:, start : start + block_rows]
        grad_scores = (probs * (grad_probs - row_inner)).astype(jnp.bfloat16)
        grad_queries.append(
            jnp.einsum("hqk,khe->qhe", grad_scores, near_keys, preferred_element_type=jnp.float32)
        )
        grad_keys = grad_keys.at[:end].add(
            jnp.einsum("hqk,qhe->khe", grad_scores, piece, preferred_element_type=jnp.float32)
        )
        grad_values = grad_values.at[:end].add(
            jnp.einsum(
                "hqk,qhe->khe",
                probs.astype(jnp.bfloat16),
                grad_piece,
                preferred_element_type=jnp.float32,
            )
        )
    return (jnp.concatenate(grad_queries, 0), grad_keys, grad_values)


def on_device(
    tokens,
    memory,
    segment,
    cotangent,
    self_query,
    self_query_bias,
    self_key,
    self_value,
    self_value_bias,
    self_output,
    self_output_bias,
    cross_query,
    cross_query_bias,
    cross_key,
    cross_value,
    cross_value_bias,
    cross_output,
    cross_output_bias,
    first_gain,
    first_shift,
    second_gain,
    second_shift,
    third_gain,
    third_shift,
    inner_weight,
    inner_bias,
    outer_weight,
    outer_bias,
):
    scale = HD ** (-0.5)
    length = tokens.shape[0]
    groups = lax.axis_size("tensor")
    member = lax.axis_index("tensor")
    half = length // groups

    def rows_of(values):
        return lax.dynamic_slice_in_dim(values, member * half, half, 0)

    def spread_out(values):
        whole = jnp.zeros((values.shape[0] * groups,), jnp.float32)
        return lax.dynamic_update_slice_in_dim(whole, values, member * values.shape[0], 0)

    def own_share(values, count):
        return lax.dynamic_slice_in_dim(values, member * count, count, 0)

    def swap(values):
        return lax.ppermute(values, "tensor", [(0, 1), (1, 0)])

    def gather_rows(values):
        if groups != 2:
            return lax.all_gather(values, "tensor", axis=0, tiled=True)
        other = swap(values)
        lead = member == 0
        return jnp.concatenate(
            [jnp.where(lead, values, other), jnp.where(lead, other, values)], 0
        )

    def scatter_rows(values):
        if groups != 2:
            return lax.psum_scatter(
                values, "tensor", scatter_dimension=0, tiled=True
            ).astype(jnp.float32)
        top = values[:half]
        bottom = values[half:]
        lead = member == 0
        keep = jnp.where(lead, top, bottom)
        send = jnp.where(lead, bottom, top)
        return keep.astype(jnp.float32) + swap(send).astype(jnp.float32)

    def sum_pair(values):
        if groups != 2:
            return lax.psum(values, "tensor").astype(jnp.float32)
        return values.astype(jnp.float32) + swap(values).astype(jnp.float32)

    queries = ((project(tokens, self_query) + self_query_bias.astype(jnp.float32)) * scale).astype(
        jnp.bfloat16
    )
    keys = project(tokens, self_key).astype(jnp.bfloat16)
    values = (project(tokens, self_value) + self_value_bias.astype(jnp.float32)).astype(
        jnp.bfloat16
    )
    self_queries = heads_of(queries)
    self_keys = heads_of(keys)
    self_values = heads_of(values)
    self_context, self_totals = attend_forward(self_queries, self_keys, self_values, segment, True)
    self_exact = self_context
    self_context = self_context.reshape(length, -1).astype(jnp.bfloat16)
    attended = scatter_rows(project(self_context, self_output)) + self_output_bias.astype(
        jnp.float32
    )
    first, first_back = jax.vjp(
        normalize,
        rows_of(tokens).astype(jnp.float32) + attended,
        first_gain.astype(jnp.float32),
        first_shift.astype(jnp.float32),
    )
    first_low = gather_rows(first.astype(jnp.bfloat16))
    queries = (
        (project(first_low, cross_query) + cross_query_bias.astype(jnp.float32)) * scale
    ).astype(jnp.bfloat16)
    keys = project(memory, cross_key).astype(jnp.bfloat16)
    values = (project(memory, cross_value) + cross_value_bias.astype(jnp.float32)).astype(
        jnp.bfloat16
    )
    cross_queries = heads_of(queries)
    cross_keys = heads_of(keys)
    cross_values = heads_of(values)
    cross_context, cross_totals = attend_forward(
        cross_queries, cross_keys, cross_values, segment, False
    )
    cross_exact = cross_context
    cross_context = cross_context.reshape(length, -1).astype(jnp.bfloat16)
    crossed = scatter_rows(
        project(cross_context, cross_output).astype(jnp.bfloat16)
    ) + cross_output_bias.astype(jnp.float32)
    second_part, second_back = jax.vjp(
        normalize,
        first + crossed,
        second_gain.astype(jnp.float32),
        second_shift.astype(jnp.float32),
    )
    second = gather_rows(second_part.astype(jnp.bfloat16)).astype(second_part.dtype)
    second_low = second.astype(jnp.bfloat16)
    inner = project(second_low, inner_weight) + inner_bias.astype(jnp.float32)
    hidden = jax.nn.gelu(inner, approximate=False).astype(jnp.bfloat16)
    outer = sum_pair(project(hidden, outer_weight).astype(jnp.bfloat16)) + outer_bias.astype(
        jnp.float32
    )
    result, third_back = jax.vjp(
        normalize, second + outer, third_gain.astype(jnp.float32), third_shift.astype(jnp.float32)
    )
    output = result.astype(jnp.bfloat16)
    grad_third, grad_third_gain, grad_third_shift = third_back(cotangent.astype(jnp.float32))
    grad_outer = grad_third.astype(jnp.bfloat16)
    grad_outer_bias = column_sums(grad_outer)
    gelu_back = jax.vjp(partial(jax.nn.gelu, approximate=False), inner)[1]
    grad_inner = gelu_back(project(grad_outer, outer_weight.T))[0].astype(jnp.bfloat16)
    grad_inner_weight = project(second_low.T, grad_inner)
    grad_inner_bias = column_sums(grad_inner)
    grad_second = rows_of(grad_third) + scatter_rows(
        project(grad_inner, inner_weight.T).astype(jnp.bfloat16)
    )
    grad_second_in, grad_second_gain, grad_second_shift = second_back(grad_second)
    grad_cross_rows = grad_second_in.astype(jnp.bfloat16)
    grad_cross = gather_rows(grad_cross_rows)
    grad_cross_output_bias = column_sums(grad_cross)
    grad_cross_context = heads_of(project(grad_cross, cross_output.T).astype(jnp.bfloat16))
    cross_grad_q, cross_grad_k, cross_grad_v = attend_backward(
        cross_queries,
        cross_keys,
        cross_values,
        grad_cross_context,
        cross_totals,
        segment,
        False,
        cross_exact,
    )
    cross_grad_q = (cross_grad_q.astype(jnp.bfloat16) * scale).reshape(length, -1)
    cross_grad_k = cross_grad_k.astype(jnp.bfloat16).reshape(length, -1)
    cross_grad_v = cross_grad_v.astype(jnp.bfloat16).reshape(length, -1)
    grad_cross_query = project(first_low.T, cross_grad_q)
    grad_cross_query_bias = column_sums(cross_grad_q)
    grad_cross_key = project(memory.T, cross_grad_k)
    grad_cross_value = project(memory.T, cross_grad_v)
    grad_cross_value_bias = column_sums(cross_grad_v)
    memory_term = project(cross_grad_k, cross_key.T) + project(cross_grad_v, cross_value.T)
    grad_first = grad_second_in + scatter_rows(
        project(cross_grad_q, cross_query.T).astype(jnp.bfloat16)
    )
    grad_cross_output_t = project(grad_cross.T, cross_context)
    cross = [grad_cross_query, grad_cross_key, grad_cross_value, grad_cross_output_t]
    cross_joined = jnp.concatenate(cross, 1).astype(jnp.bfloat16)
    cross_joined, grad_first = lax.optimization_barrier((cross_joined, grad_first))
    grad_first_in, grad_first_gain, grad_first_shift = first_back(grad_first)
    grad_self_rows = grad_first_in.astype(jnp.bfloat16)
    grad_self = gather_rows(grad_self_rows)
    grad_self_output_bias = column_sums(grad_self)
    grad_self_context = heads_of(project(grad_self, self_output.T).astype(jnp.bfloat16))
    outer_size = lax.axis_size("outer")
    inner_size = lax.axis_size("inner")
    dp_size = outer_size * inner_size
    self_grad_q, self_grad_k, self_grad_v = attend_backward(
        self_queries,
        self_keys,
        self_values,
        grad_self_context,
        self_totals,
        segment,
        True,
        self_exact,
    )
    self_grad_q = (self_grad_q.astype(jnp.bfloat16) * scale).reshape(length, -1)
    self_grad_k = self_grad_k.astype(jnp.bfloat16).reshape(length, -1)
    self_grad_v = self_grad_v.astype(jnp.bfloat16).reshape(length, -1)
    grad_self_query = project(tokens.T, self_grad_q)
    grad_self_query_bias = column_sums(self_grad_q)
    grad_self_key = project(tokens.T, self_grad_k)
    grad_self_value = project(tokens.T, self_grad_v)
    grad_self_value_bias = column_sums(self_grad_v)
    tokens_term = (
        project(self_grad_q, self_query.T)
        + project(self_grad_k, self_key.T)
        + project(self_grad_v, self_value.T)
    )
    tokens_part = scatter_rows(tokens_term.astype(jnp.bfloat16))
    memory_part = scatter_rows(memory_term.astype(jnp.bfloat16))
    grad_tokens = tokens_part + grad_first_in
    grad_self_output_t = project(grad_self.T, self_context)
    grad_outer_weight_t = project(grad_outer.T, hidden)

    def split_columns(summed, pieces, flipped):
        parts = []
        offset = 0
        for position, piece in enumerate(pieces):
            width = piece.shape[1]
            part = summed[:, offset : offset + width]
            offset += width
            if position in flipped:
                part = part.T
            parts.append(part)
        return parts

    def exchange_sum(joined, extra=None):
        rows = joined.shape[0] // dp_size
        width = joined.shape[1]
        blocks = joined.reshape(dp_size, rows, width)
        if inner_size == 1 or outer_size == 1:
            if extra is not None:
                blocks = jnp.concatenate(
                    [blocks, jnp.broadcast_to(extra[None], (dp_size,) + extra.shape)], 1
                )
            received = lax.all_to_all(blocks, DP, 0, 0, tiled=True)
            return jnp.sum(received.astype(jnp.float32), 0)
        staged = blocks.reshape(outer_size, inner_size, rows, width)
        staged = jnp.swapaxes(staged, 0, 1).reshape(inner_size, outer_size * rows, width)
        if extra is not None:
            staged = jnp.concatenate(
                [staged, jnp.broadcast_to(extra[None], (inner_size,) + extra.shape)], 1
            )
        first = lax.all_to_all(staged, "inner", 0, 0, tiled=True)
        partial = jnp.sum(first.astype(jnp.float32), 0)
        middle = partial[: outer_size * rows].astype(jnp.bfloat16).reshape(
            outer_size, rows, width
        )
        if extra is not None:
            lines = extra.shape[0] // 2
            tail = partial[outer_size * rows :]
            merged = tail[:lines] + tail[lines:]
            high = merged.astype(jnp.bfloat16)
            low = (merged - high.astype(jnp.float32)).astype(jnp.bfloat16)
            pair = jnp.concatenate([high, low], 0)
            middle = jnp.concatenate(
                [middle, jnp.broadcast_to(pair[None], (outer_size,) + pair.shape)], 1
            )
        if outer_size > 4:
            second = lax.all_to_all(middle, "outer", 0, 0, tiled=True)
            return jnp.sum(second.astype(jnp.float32), 0)
        place = lax.axis_index("outer")
        by_source = [None] * outer_size
        for shift in range(outer_size):
            piece = lax.dynamic_index_in_dim(
                middle, (place + shift) % outer_size, 0, keepdims=False
            )
            if shift:
                piece = lax.ppermute(
                    piece,
                    "outer",
                    [(peer, (peer + shift) % outer_size) for peer in range(outer_size)],
                )
            by_source[shift] = piece
        total = None
        for source in range(outer_size):
            chosen = by_source[0]
            for shift in range(1, outer_size):
                chosen = jnp.where(
                    (place - shift) % outer_size == source, by_source[shift], chosen
                )
            chosen = chosen.astype(jnp.float32)
            total = chosen if total is None else total + chosen
        return total

    ffn = [grad_inner_weight, grad_outer_weight_t]
    ffn_sum = lax.psum_scatter(
        jnp.concatenate(ffn, 1).astype(jnp.bfloat16), DP, scatter_dimension=0, tiled=True
    ).astype(jnp.float32)
    ffn_sums = split_columns(ffn_sum, ffn, (1,))
    cross_sums = split_columns(exchange_sum(cross_joined), cross, (3,))
    late = [grad_self_query, grad_self_key, grad_self_value, grad_self_output_t]
    late_joined = jnp.concatenate(late, 1).astype(jnp.bfloat16)
    norm_pairs = sum_pair(
        jnp.concatenate([grad_first_gain, grad_first_shift, grad_second_gain, grad_second_shift])
    )
    width = late_joined.shape[1]
    sections = norm_pairs.shape[0] // 4
    biases = [
        grad_self_query_bias,
        grad_self_value_bias,
        grad_self_output_bias,
        grad_cross_query_bias,
        grad_cross_value_bias,
        grad_cross_output_bias,
        norm_pairs[:sections],
        norm_pairs[sections : 2 * sections],
        norm_pairs[2 * sections : 3 * sections],
        norm_pairs[3 * sections :],
        grad_third_gain,
        grad_third_shift,
        grad_inner_bias,
        grad_outer_bias,
    ]
    lines = []
    current = []
    used = 0
    places = []
    for bias in biases:
        chunks = []
        for begin in range(0, bias.shape[0], width):
            chunk = bias[begin : begin + width]
            if used + chunk.shape[0] > width:
                if used < width:
                    current.append(jnp.zeros((width - used,), jnp.float32))
                lines.append(jnp.concatenate(current))
                current = []
                used = 0
            chunks.append((len(lines), used, chunk.shape[0]))
            current.append(chunk)
            used += chunk.shape[0]
        places.append(chunks)
    if used < width:
        current.append(jnp.zeros((width - used,), jnp.float32))
    lines.append(jnp.concatenate(current))
    padded = jnp.stack(lines)
    count = padded.shape[0]
    high = padded.astype(jnp.bfloat16)
    low = (padded - high.astype(jnp.float32)).astype(jnp.bfloat16)
    late_rows = late_joined.shape[0] // dp_size
    late_total = exchange_sum(late_joined, jnp.concatenate([high, low], 0))
    self_sums = split_columns(late_total[:late_rows], late, (3,))
    summed_lines = late_total[late_rows : late_rows + count] + late_total[late_rows + count :]
    smalls = []
    for chunks in places:
        smalls.append(
            jnp.concatenate(
                [summed_lines[line, begin : begin + size] for line, begin, size in chunks]
            )
        )
    return (
        output,
        grad_tokens,
        memory_part,
        self_sums[0],
        smalls[0],
        self_sums[1],
        self_sums[2],
        smalls[1],
        self_sums[3],
        smalls[2],
        cross_sums[0],
        smalls[3],
        cross_sums[1],
        cross_sums[2],
        smalls[4],
        cross_sums[3],
        smalls[5],
        smalls[6],
        smalls[7],
        smalls[8],
        smalls[9],
        smalls[10],
        smalls[11],
        ffn_sums[0],
        smalls[12],
        ffn_sums[1],
        smalls[13],
    )


def solution(mesh):
    dp_size = mesh.shape["dp"]
    inner = 4 if dp_size % 4 == 0 and dp_size > 4 else 1
    devices = np.asarray(mesh.devices).reshape(dp_size // inner, inner, mesh.shape["tensor"])
    staged = Mesh(devices, ("outer", "inner", "tensor"))
    return jax.shard_map(
        on_device,
        mesh=staged,
        in_specs=(
            P(DP, None),
            P(DP, None),
            P(DP),
            P(DP, None),
            P(None, "tensor"),
            P("tensor"),
            P(None, "tensor"),
            P(None, "tensor"),
            P("tensor"),
            P("tensor", None),
            P(),
            P(None, "tensor"),
            P("tensor"),
            P(None, "tensor"),
            P(None, "tensor"),
            P("tensor"),
            P("tensor", None),
            P(),
            P(),
            P(),
            P(),
            P(),
            P(),
            P(),
            P(None, "tensor"),
            P("tensor"),
            P("tensor", None),
            P(),
        ),
        out_specs=(
            P(DP, None),
            P(("outer", "inner", "tensor"), None),
            P(("outer", "inner", "tensor"), None),
            P(DP, "tensor"),
            P("tensor"),
            P(DP, "tensor"),
            P(DP, "tensor"),
            P("tensor"),
            P("tensor", DP),
            P(),
            P(DP, "tensor"),
            P("tensor"),
            P(DP, "tensor"),
            P(DP, "tensor"),
            P("tensor"),
            P("tensor", DP),
            P(),
            P(),
            P(),
            P(),
            P(),
            P(),
            P(),
            P(DP, "tensor"),
            P("tensor"),
            P("tensor", DP),
            P(),
        ),
        check_vma=False,
    )
```
